32 devices in a mesh: cfg: 2 (over x), seq: 8 (over z, y), dp: 2 (over core).
Axes of the slice: x: 2, y: 2, z: 4, core: 2. Of those that a mesh axis runs over, the one named last changes fastest.
Arguments:
- teacher_query: bfloat16 [2, 2, 2, 1024, 2048], P('cfg', None, 'dp', 'seq'), may hold values from -6 to 6
- teacher_key: bfloat16 [2, 2, 2, 1024, 2048], P('cfg', None, 'dp', 'seq'), may hold values from -6 to 6
- teacher_value: bfloat16 [2, 2, 2, 1024, 2048], P('cfg', None, 'dp', 'seq'), may hold values from -6 to 6
- hidden: bfloat16 [2, 2, 1024, 3072], P('cfg', 'dp', 'seq'), may hold values from -6 to 6
- adapter_down_weight: bfloat16 [3, 3072, 128], replicated, may hold values from -0.109375 to 0.109375
- adapter_up_weight: bfloat16 [3, 128, 2048], replicated, may hold values from -0.5 to 0.5
- guidance_index: int32 [2, 2], P(None, 'dp'), may hold values from 0 to 7
- timestep_index: int32 [2, 2], P(None, 'dp'), may hold values from 0 to 999
Outputs:
- student_out: bfloat16 [2, 2, 1024, 2048], P('cfg', 'dp', 'seq')
- grad_down: float32 [3, 3072, 128], P(None, ('cfg', 'seq', 'dp'))
- grad_up: float32 [3, 128, 2048], P(None, ('cfg', 'dp'), 'seq')
The draws below stay inside these ranges and needn't reach their ends.
All inputs are finite; a program needn't handle non-finite values.
Results may differ from the reference program's by a relative error of at most 0.02.
The reference program's roundings to bfloat16 on the way count: a program that leaves them out, or rounds other values in their place, can miss the bound.
Values may be sent and summed in bfloat16 or wider, within the bound.
A program may use at most 128 MiB of HBM per device.

```python
import math
import jax
import jax.numpy as jnp
from jax import lax

MODEL_WIDTH = 3072
HEADS = 16
HDIM = 128
ADAPTER_RANK = 128
GUIDES = 8
TSTEPS = 1000
ALL_HEADS_WIDTH = 2048
TOKENS = 1024
N_DP = 2


def field_shape():
    return (2, 2, N_DP, TOKENS, HEADS * HDIM)


def draw_teacher_query(key, part):
    field = 2.7 * jax.random.truncated_normal(jax.random.fold_in(key, 11), -2.2, 2.2, field_shape(), jnp.float32)
    return field.astype(jnp.bfloat16)


def draw_teacher_key(key, part):
    field = 2.7 * jax.random.truncated_normal(jax.random.fold_in(key, 23), -2.2, 2.2, field_shape(), jnp.float32)
    return field.astype(jnp.bfloat16)


def place_ends(entries, own_key, least, largest):
    longest = entries.shape.index(max(entries.shape))
    spots = []
    for shift in (0, 1):
        where = [jax.random.randint(jax.random.fold_in(own_key, axis), (), 0, length) for axis, length in enumerate(entries.shape)]
        where[longest] = (where[longest] + shift) % entries.shape[longest]
        spots.append(tuple(where))
    return entries.at[spots[0]].set(least).at[spots[1]].set(largest)


def with_spikes(values, own_key, source, target, parts, factor):
    owner, partner = [(jnp.arange(values.shape[dim]) // (values.shape[dim] // parts)).reshape([-1 if axis == dim else 1 for axis in range(values.ndim)]) for dim in (source, target)]
    chosen = jax.random.permutation(own_key, parts)[partner]
    strong = (owner == chosen) | (owner == (partner + parts // 2) % parts)
    return jnp.where(strong, factor * values, values)


def block_scale(rng, shape, split, low, high):
    gain = 1.0
    for dim, blocks in split:
        draws = jax.random.uniform(jax.random.fold_in(jax.random.fold_in(rng, 6), dim), (blocks,), jnp.float32, low / len(split), high / len(split))
        gain = gain * jnp.repeat(jnp.exp(draws), shape[dim] // blocks).reshape((-1,) + (1,) * (len(shape) - 1 - dim))
    return gain


def noise(rng, shape, width, most, shards=(), held_as=jnp.bfloat16):
    result = jax.random.normal(rng, shape, jnp.float32) * width
    if len(shards) > 0:
        result = block_scale(rng, shape, shards, -0.22, 0.18) * result
    return jnp.clip(result, min=-most, max=most).astype(held_as)


def noise_with(own_key, shape, spread, bound, cuts, heavy, dtype=jnp.bfloat16):
    values = spread * jax.random.normal(own_key, shape, jnp.float32)
    if cuts:
        values = values * block_scale(own_key, shape, cuts, -0.22, 0.18)
    return jnp.clip(with_spikes(values, jax.random.fold_in(own_key, 3), *heavy), -bound, bound).astype(dtype)


def setup_inputs(seed: int = 0) -> dict:
    streams_of = jax.random.split(jax.random.key(seed), 9)
    return {
        "teacher_query": draw_teacher_query(jax.random.fold_in(streams_of[8], 71), 0),
        "teacher_key": draw_teacher_key(jax.random.fold_in(streams_of[8], 71), 0),
        "teacher_value": noise(streams_of[2], (2, 2, N_DP, TOKENS, ALL_HEADS_WIDTH), 1.0, 6.0, ((0, 2), (2, 2), (3, 8))),
        "hidden": noise_with(streams_of[3], (2, N_DP, TOKENS, MODEL_WIDTH), 1.0, 6.0, ((0, 2), (1, 2), (2, 8)), (2, 3, 8, 2.0)),
        "adapter_down_weight": noise(streams_of[4], (3, MODEL_WIDTH, ADAPTER_RANK), MODEL_WIDTH ** -0.5, 0.109375),
        "adapter_up_weight": noise(streams_of[5], (3, ADAPTER_RANK, ALL_HEADS_WIDTH), ADAPTER_RANK ** -0.5, 0.5),
        "guidance_index": place_ends(jax.random.randint(streams_of[6], (2, N_DP), 0, GUIDES), jax.random.fold_in(streams_of[6], 1), 0, GUIDES - 1).astype(jnp.int32),
        "timestep_index": place_ends(jax.random.randint(streams_of[7], (2, N_DP), 0, TSTEPS), jax.random.fold_in(streams_of[7], 1), 0, TSTEPS - 1).astype(jnp.int32),
    }


def head_probs(query_head, key_head):
    scores = jnp.dot(query_head, key_head.T, preferred_element_type=jnp.float32) * HDIM ** (-0.5)
    highest = lax.optimization_barrier(jnp.max(scores, axis=-1, keepdims=True))
    raised = jnp.exp(scores - highest)
    return raised / lax.optimization_barrier(jnp.sum(raised, axis=-1, keepdims=True))

def to_heads(array):
    return array.reshape(array.shape[0], HEADS, HDIM).transpose(1, 0, 2)

def from_heads(array):
    return array.transpose(1, 0, 2).reshape(array.shape[1], HEADS * HDIM)

def attend(queries, keys, values):

    def per_head(triple):
        query_head, key_head, value_head = triple
        weights = head_probs(query_head, key_head).astype(jnp.bfloat16)
        return jnp.dot(weights, value_head, preferred_element_type=jnp.float32)
    return from_heads(lax.map(per_head, (to_heads(queries), to_heads(keys), to_heads(values))))

def attend_back(queries, keys, values, upstream):
    factor = HDIM ** (-0.5)

    def per_head(group):
        query_head, key_head, value_head, upstream_head = group
        probability = head_probs(query_head, key_head)
        weights = probability.astype(jnp.bfloat16)
        value_grad = jnp.dot(weights.T, upstream_head, preferred_element_type=jnp.float32)
        prob_grad = jnp.dot(upstream_head, value_head.T, preferred_element_type=jnp.float32)
        center = lax.optimization_barrier(jnp.sum(probability * prob_grad, axis=-1, keepdims=True))
        score_grad = (probability * (prob_grad - center)).astype(jnp.bfloat16)
        query_grad = jnp.dot(score_grad, key_head, preferred_element_type=jnp.float32) * factor
        key_grad = jnp.dot(score_grad.T, query_head, preferred_element_type=jnp.float32) * factor
        return (query_grad.astype(jnp.bfloat16), key_grad.astype(jnp.bfloat16), value_grad.astype(jnp.bfloat16))
    results = lax.map(per_head, (to_heads(queries), to_heads(keys), to_heads(values), to_heads(upstream)))
    return tuple((from_heads(stack_member) for stack_member in results))

def flatten(array):
    return array.reshape(-1, TOKENS, ALL_HEADS_WIDTH)

def reference(teacher_query, teacher_key, teacher_value, hidden, adapter_down_weight, adapter_up_weight, guidance_index, timestep_index):
    teacher_out = lax.map(lambda triple: attend(*triple).astype(jnp.bfloat16), (flatten(teacher_query), flatten(teacher_key), flatten(teacher_value)))
    teacher_out = teacher_out.reshape(2, 2, N_DP, TOKENS, ALL_HEADS_WIDTH).astype(jnp.float32)
    guide_scale = 1.0 + 0.5 * guidance_index.astype(jnp.float32)
    time_frac = (timestep_index.astype(jnp.float32) + 0.5) / TSTEPS
    target = teacher_out[1] + guide_scale[:, :, None, None] * (teacher_out[0] - teacher_out[1])
    rank_index = jnp.arange(1, ADAPTER_RANK + 1).astype(jnp.float32)
    feature_modulation = 1.0 + 0.5 * jnp.cos(math.pi * rank_index * time_frac[:, :, None] + 0.25 * rank_index * guide_scale[:, :, None])
    hidden_full_width = hidden.astype(jnp.float32)
    rank_projected = (jnp.einsum('eyog,mgf->meyof', hidden_full_width, adapter_down_weight.astype(jnp.float32)) * feature_modulation[None, :, :, None, :]).astype(jnp.bfloat16)
    up_full_width = adapter_up_weight.astype(jnp.float32)
    frozen = (teacher_query[0], teacher_key[0], teacher_value[0])
    student = []
    for stack_member in range(3):
        adapted_output = jnp.einsum('citr,rh->cith', rank_projected[stack_member].astype(jnp.float32), up_full_width[stack_member])
        student.append(flatten((frozen[stack_member].astype(jnp.float32) + adapted_output).astype(jnp.bfloat16)))
    student = tuple(student)
    student_flat = lax.map(lambda triple: attend(*triple).astype(jnp.bfloat16), student)
    student_out = student_flat.reshape(2, N_DP, TOKENS, ALL_HEADS_WIDTH)
    upstream = ((student_out.astype(jnp.float32) - target) * (1.0 / math.sqrt(2 * N_DP * TOKENS))).astype(jnp.bfloat16)
    grads = lax.map(lambda group: attend_back(*group), student + (flatten(upstream),))
    gradient_stack = jnp.stack(grads).astype(jnp.float32).reshape(3, 2, N_DP, TOKENS, ALL_HEADS_WIDTH)
    grad_up = jnp.einsum('kcitr,kcith->krh', rank_projected.astype(jnp.float32), gradient_stack)
    rank_backward = jnp.einsum('kcith,krh->kcitr', gradient_stack, up_full_width)
    low_grad = (rank_backward * feature_modulation[None, :, :, None, :]).astype(jnp.bfloat16)
    grad_down = jnp.einsum('citd,kcitr->kdr', hidden_full_width, low_grad.astype(jnp.float32))
    return (student_out, grad_down, grad_up)
```

```python
import functools
import math

import jax
import jax.numpy as jnp
from jax import lax
from jax.experimental import pallas as pl
from jax.experimental.pallas import tpu as pltpu
from jax.sharding import PartitionSpec as P

HDIM = 128
ADAPTER_RANK = 128
TSTEPS = 1000
FACTOR = HDIM ** (-0.5)
FACTOR_BASE2 = FACTOR * math.log2(math.e)
VMEM_LIMIT = 60 * 1024 * 1024
BLOCK = 256
MESH = pl.DeviceIdType.MESH

NT = (((1,), (1,)), ((), ()))
TN = (((0,), (0,)), ((), ()))


def dot_f32(left, right):
    return jnp.dot(left, right, preferred_element_type=jnp.float32)


def dot_nt(left, right):
    return lax.dot_general(left, right, NT, preferred_element_type=jnp.float32)


def dot_tn(left, right):
    return lax.dot_general(left, right, TN, preferred_element_type=jnp.float32)


def inner_size(count):
    return max(size for size in range(1, count + 1) if count % size == 0 and size * size <= count)


def aligned(index, size):
    return pl.ds(pl.multiple_of(index * size, size), size)


def probs_by_key(key_head, query_block):
    scores = dot_nt(key_head, query_block)
    highest = jnp.max(scores, axis=0, keepdims=True)
    raised = jnp.exp2((scores - highest) * FACTOR_BASE2)
    return raised * (1.0 / jnp.sum(raised, axis=0, keepdims=True))


def step_kernel(
    sizes,
    out_scale,
    weight_ref,
    query_ref,
    key_ref,
    value_ref,
    hidden_ref,
    hidden_cols_ref,
    down_ref,
    up_ref,
    modulation_ref,
    tokens_ref,
    grad_down_ref,
    grad_up_ref,
    heads,
    hidden_own,
    hidden_all,
    down_own,
    up_own,
    ranks,
    weighted,
    weighted_in,
    target,
    s_query,
    s_key,
    s_value,
    key_t,
    value_t,
    grad_query,
    grad_key,
    grad_value,
    back_sum,
    back,
    back_in,
    student,
    up_parts,
    up_in,
    low,
    low_all,
    down_out,
    down_in,
    field_send,
    field_recv,
    pass_send,
    pass_recv,
    rank_send,
    rank_recv,
    fan_send,
    fan_recv,
    swap_send,
    swap_recv,
    out_send,
    out_recv,
    cols_send,
    cols_recv,
    up_send,
    up_recv,
    back_send,
    back_recv,
    low_send,
    low_recv,
    down_send,
    down_recv,
    local_sem,
):
    count, inner, dp_count = sizes
    outer = count // inner
    groups = 2 * inner * dp_count
    up_groups = 2 * dp_count
    fields = (query_ref, key_ref, value_ref)
    tok_here = query_ref.shape[1]
    length = tok_here * count
    columns = student.shape[1]
    heads_here = columns // HDIM
    step_rows = min(BLOCK, length)
    blocks = length // step_rows

    me = lax.axis_index("seq")
    cfg = lax.axis_index("cfg")
    dp = lax.axis_index("dp")
    other = 1 - cfg
    far = me // inner
    near = lax.rem(me, inner)
    group = (cfg * inner + near) * dp_count + dp
    up_group = cfg * dp_count + dp
    own_rows = aligned(me, tok_here)
    order = (other, cfg)

    def head_columns(head):
        return slice(head * HDIM, (head + 1) * HDIM)

    def seq_peer(step):
        return lax.rem(me + step, count)

    def group_device(step):
        peer = lax.rem(group + step, groups)
        rest = peer // dp_count
        return {
            "cfg": rest // inner,
            "seq": far * inner + lax.rem(rest, inner),
            "dp": lax.rem(peer, dp_count),
        }

    def remote(src, dst, send, recv, device):
        return pltpu.make_async_remote_copy(
            src_ref=src,
            dst_ref=dst,
            send_sem=send,
            recv_sem=recv,
            device_id=device,
            device_id_type=MESH,
        )

    loads = [
        pltpu.make_async_copy(hidden_ref, hidden_own, local_sem.at[0]),
        pltpu.make_async_copy(down_ref, down_own, local_sem.at[1]),
        pltpu.make_async_copy(
            up_ref.at[:, :, aligned(me, columns)], up_own, local_sem.at[2]
        ),
        pltpu.make_async_copy(hidden_cols_ref.at[group], hidden_all.at[group], local_sem.at[3]),
    ] + [
        pltpu.make_async_copy(
            fields[member].at[:, :, aligned(me, columns)],
            heads.at[member, 0:2, own_rows, :],
            local_sem.at[4 + member],
        )
        for member in range(3)
    ]
    for load in loads:
        load.start()

    barrier = pltpu.get_barrier_semaphore()
    for step in range(1, count):
        pl.semaphore_signal(
            barrier, inc=1, device_id={"seq": seq_peer(step)}, device_id_type=MESH
        )
    for step in range(1, groups):
        pl.semaphore_signal(barrier, inc=1, device_id=group_device(step), device_id_type=MESH)
    pl.semaphore_wait(barrier, count + groups - 2)

    def field_copy(phase, head, member, step):
        peer = seq_peer(step)
        half = order[phase]
        start = pl.multiple_of(peer * columns, columns) + head * HDIM
        return remote(
            fields[member].at[half, :, pl.ds(start, HDIM)],
            heads.at[member, half, own_rows, head_columns(head)],
            field_send.at[phase, head, member, step],
            field_recv.at[phase, head, member, step],
            {"seq": peer},
        )

    def start_fields(phase, head):
        for member in (1, 2, 0):
            for step in range(1, count):
                field_copy(phase, head, member, step).start()

    def wait_fields(phase, head):
        for member in (1, 2, 0):
            for step in range(1, count):
                field_copy(phase, head, member, step).wait_recv()

    def pass_copy(head, member):
        return remote(
            heads.at[member, 1, :, head_columns(head)],
            heads.at[member, 2, :, head_columns(head)],
            pass_send.at[head, member],
            pass_recv.at[head, member],
            {"cfg": other},
        )

    def rank_copy(step):
        return remote(
            ranks.at[far, near],
            ranks.at[far, near],
            rank_send.at[step],
            rank_recv.at[step],
            {"seq": lax.rem(far + step, outer) * inner + near},
        )

    def fan_copy(step):
        return remote(
            ranks.at[:, near],
            ranks.at[:, near],
            fan_send.at[step],
            fan_recv.at[step],
            {"seq": far * inner + lax.rem(near + step, inner)},
        )

    def swap_copy(head):
        return remote(
            weighted.at[head],
            weighted_in.at[head],
            swap_send.at[head],
            swap_recv.at[head],
            {"cfg": other},
        )

    def out_copy(head, step):
        peer = seq_peer(step)
        start = pl.multiple_of(me * columns, columns) + head * HDIM
        return remote(
            student.at[aligned(peer, tok_here), head_columns(head)],
            tokens_ref.at[:, pl.ds(start, HDIM)],
            out_send.at[head, step],
            out_recv.at[head, step],
            {"seq": peer},
        )

    def cols_copy(step):
        return remote(
            hidden_cols_ref.at[lax.rem(group + step, groups)],
            hidden_all.at[group],
            cols_send.at[step],
            cols_recv.at[step],
            group_device(step),
        )

    def up_copy(step):
        peer = lax.rem(up_group + step, up_groups)
        return remote(
            up_parts.at[peer],
            up_in.at[step],
            up_send.at[step],
            up_recv.at[step],
            {"cfg": peer // dp_count, "dp": lax.rem(peer, dp_count)},
        )

    def back_copy(step):
        peer = seq_peer(step)
        return remote(
            back.at[aligned(peer, tok_here), :],
            back_in.at[step],
            back_send.at[step],
            back_recv.at[step],
            {"seq": peer},
        )

    def low_copy(step):
        return remote(
            low, low_all.at[group], low_send.at[step], low_recv.at[step], group_device(step)
        )

    def down_copy(step):
        peer = lax.rem(far + step, outer)
        return remote(
            down_out.at[peer],
            down_in.at[step],
            down_send.at[step],
            down_recv.at[step],
            {"seq": peer * inner + near},
        )

    phases = [(phase, head) for phase in range(2) for head in range(heads_here)]
    start_fields(*phases[0])

    loads[0].wait()
    loads[1].wait()
    for member in range(3):
        projected = dot_f32(hidden_own[...], down_own[member]) * modulation_ref[...]
        ranks[far, near, :, head_columns(member)] = projected.astype(jnp.bfloat16)
    for step in range(1, outer):
        rank_copy(step).start()
    start_fields(*phases[1])
    for step in range(1, outer):
        rank_copy(step).wait_recv()
    for step in range(1, inner):
        fan_copy(step).start()
    for step in range(1, groups):
        cols_copy(step).start()
    for phase, head in phases[2:]:
        start_fields(phase, head)
    for load in loads[2:]:
        load.wait()

    def teacher(half, head, store):
        lanes = head_columns(head)
        value_t[...] = heads[2, half, :, lanes].T

        def one_block(step, _):
            rows = aligned(step, step_rows)
            weights = probs_by_key(heads[1, half, :, lanes], heads[0, half, rows, lanes])
            attended = dot_f32(value_t[...], weights.astype(jnp.bfloat16)).T
            store(rows, attended.astype(jnp.bfloat16).astype(jnp.float32))
            return 0

        lax.fori_loop(0, blocks, one_block, 0)

    for head in range(heads_here):
        wait_fields(0, head)

        @pl.when(cfg == 0)
        def _():
            for member in range(3):
                pass_copy(head, member).start()

        def store_other(rows, attended):
            weighted[head, rows, :] = (weight_ref[1] * attended).astype(jnp.bfloat16)

        teacher(other, head, store_other)
        swap_copy(head).start()

    for step in range(1, inner):
        fan_copy(step).wait_recv()

    for head in range(heads_here):
        lanes = head_columns(head)
        wait_fields(1, head)

        def store_own(rows, attended):
            target[rows, :] = weight_ref[0] * attended

        teacher(cfg, head, store_own)

        @pl.when(cfg == 1)
        def _():
            for member in range(3):
                pass_copy(head, member).wait_recv()

        for member, projected in enumerate((s_query, s_key, s_value)):
            low_rank = ranks[:, :, :, head_columns(member)].reshape(length, ADAPTER_RANK)
            frozen = heads[member, 2 * cfg, :, lanes].astype(jnp.float32)
            projected[...] = (frozen + dot_f32(low_rank, up_own[member, :, lanes])).astype(
                jnp.bfloat16
            )
        key_t[...] = s_key[...].T
        value_t[...] = s_value[...].T
        grad_key[...] = jnp.zeros_like(grad_key)
        grad_value[...] = jnp.zeros_like(grad_value)
        swap_copy(head).wait_recv()

        def one_block(step, _):
            rows = aligned(step, step_rows)
            query_block = s_query[rows, :]
            probability = probs_by_key(s_key[...], query_block)
            weights = probability.astype(jnp.bfloat16)
            attended = dot_f32(value_t[...], weights).T.astype(jnp.bfloat16)
            student[rows, lanes] = attended
            aim = target[rows, :] + weighted_in[head, rows, :].astype(jnp.float32)
            upstream = ((attended.astype(jnp.float32) - aim) * out_scale).astype(jnp.bfloat16)
            grad_value[...] += dot_f32(weights, upstream)
            prob_grad = dot_nt(s_value[...], upstream)
            center = jnp.sum(probability * prob_grad, axis=0, keepdims=True)
            score_grad = (probability * (prob_grad - center)).astype(jnp.bfloat16)
            grad_key[...] += dot_f32(score_grad, query_block)
            grad_query[rows, :] = (dot_f32(key_t[...], score_grad).T * FACTOR).astype(
                jnp.bfloat16
            )
            return 0

        lax.fori_loop(0, blocks, one_block, 0)
        for step in range(1, count):
            out_copy(head, step).start()

        gradients = (
            grad_query[...],
            (grad_key[...] * FACTOR).astype(jnp.bfloat16),
            grad_value[...].astype(jnp.bfloat16),
        )
        for member, gradient in enumerate(gradients):
            part = dot_nt(gradient, up_own[member, :, lanes])
            if head > 0:
                part = part + back_sum[:, head_columns(member)]
            if head < heads_here - 1:
                back_sum[:, head_columns(member)] = part
            else:
                back[:, head_columns(member)] = part.astype(jnp.bfloat16)
        if head == heads_here - 1:
            for step in range(1, count):
                back_copy(step).start()
        for member, gradient in enumerate(gradients):
            low_rank = ranks[:, :, :, head_columns(member)].reshape(length, ADAPTER_RANK)
            part = dot_tn(low_rank, gradient).astype(jnp.bfloat16)
            up_parts[:, member, :, lanes] = part.reshape(up_groups, -1, HDIM)

    for step in range(1, up_groups):
        up_copy(step).start()
    own_store = pltpu.make_async_copy(
        student.at[own_rows, :], tokens_ref.at[:, aligned(me, columns)], local_sem.at[7]
    )
    own_store.start()

    total = back[own_rows, :].astype(jnp.float32)
    for step in range(1, count):
        back_copy(step).wait_recv()
        total = total + back_in[step].astype(jnp.float32)
    scale = jnp.concatenate([modulation_ref[...]] * 3, axis=1)
    low_grad = (total * scale).astype(jnp.bfloat16)
    low[...] = low_grad
    low_all[group] = low_grad
    for step in range(1, groups):
        low_copy(step).start()

    up_total = up_parts[up_group].astype(jnp.float32)
    for step in range(1, up_groups):
        up_copy(step).wait_recv()
        up_total = up_total + up_in[step].astype(jnp.float32)
    grad_up_ref[...] = up_total

    for step in range(1, groups):
        cols_copy(step).wait_recv()
        low_copy(step).wait_recv()
    gathered_cols = hidden_all[...].reshape(groups * tok_here, -1)
    gathered_low = low_all[...].reshape(groups * tok_here, -1)
    down_rows = gathered_cols.shape[1] // outer
    partial = dot_tn(gathered_cols, gathered_low).astype(jnp.bfloat16)
    for peer in range(outer):
        down_out[peer] = partial[peer * down_rows : (peer + 1) * down_rows, :]
    for step in range(1, outer):
        down_copy(step).start()
    down_total = down_out[far].astype(jnp.float32)
    for step in range(1, outer):
        down_copy(step).wait_recv()
        down_total = down_total + down_in[step].astype(jnp.float32)
    for member in range(3):
        grad_down_ref[member] = down_total[:, head_columns(member)]

    own_store.wait()
    for phase, head in phases:
        for member in range(3):
            for step in range(1, count):
                field_copy(phase, head, member, step).wait_send()
    for head in range(heads_here):
        swap_copy(head).wait_send()

        @pl.when(cfg == 0)
        def _():
            for member in range(3):
                pass_copy(head, member).wait_send()

        for step in range(1, count):
            out_copy(head, step).wait()
    for step in range(1, outer):
        rank_copy(step).wait_send()
        down_copy(step).wait_send()
    for step in range(1, inner):
        fan_copy(step).wait_send()
    for step in range(1, groups):
        cols_copy(step).wait_send()
        low_copy(step).wait_send()
    for step in range(1, up_groups):
        up_copy(step).wait_send()
    for step in range(1, count):
        back_copy(step).wait_send()


def run_step(sizes, weights, fields, hidden, hidden_cols, down, up, modulation):
    count, inner, dp_count = sizes
    outer = count // inner
    groups, tok_here, group_cols = hidden_cols.shape
    up_groups = 2 * dp_count
    width = fields[0].shape[2]
    model_width = hidden.shape[1]
    length, columns = tok_here * count, width // count
    heads_here = columns // HDIM
    rank_cols = 3 * ADAPTER_RANK
    down_rows = group_cols // outer
    up_rows = ADAPTER_RANK // up_groups
    any_spec = pl.BlockSpec(memory_space=pl.ANY)
    vmem_spec = pl.BlockSpec(memory_space=pltpu.VMEM)

    def bf16(*shape):
        return pltpu.VMEM(shape, jnp.bfloat16)

    def f32(*shape):
        return pltpu.VMEM(shape, jnp.float32)

    def sems(*shape):
        return [pltpu.SemaphoreType.DMA(shape)] * 2

    total_rows = 2 * dp_count * length
    return pl.pallas_call(
        functools.partial(step_kernel, sizes, 1.0 / math.sqrt(total_rows)),
        out_shape=(
            jax.ShapeDtypeStruct((tok_here, width), jnp.bfloat16),
            jax.ShapeDtypeStruct((3, down_rows, ADAPTER_RANK), jnp.float32),
            jax.ShapeDtypeStruct((3, up_rows, columns), jnp.float32),
        ),
        in_specs=[pl.BlockSpec(memory_space=pltpu.SMEM)] + [any_spec] * 7 + [vmem_spec],
        out_specs=(any_spec, vmem_spec, vmem_spec),
        scratch_shapes=[
            bf16(3, 3, length, columns),
            bf16(tok_here, model_width),
            bf16(groups, tok_here, group_cols),
            bf16(3, model_width, ADAPTER_RANK),
            bf16(3, ADAPTER_RANK, columns),
            bf16(outer, inner, tok_here, rank_cols),
            bf16(heads_here, length, HDIM),
            bf16(heads_here, length, HDIM),
            f32(length, HDIM),
            bf16(length, HDIM),
            bf16(length, HDIM),
            bf16(length, HDIM),
            bf16(HDIM, length),
            bf16(HDIM, length),
            bf16(length, HDIM),
            f32(length, HDIM),
            f32(length, HDIM),
            f32(length, rank_cols),
            bf16(length, rank_cols),
            bf16(count, tok_here, rank_cols),
            bf16(length, columns),
            bf16(up_groups, 3, up_rows, columns),
            bf16(up_groups, 3, up_rows, columns),
            bf16(tok_here, rank_cols),
            bf16(groups, tok_here, rank_cols),
            bf16(outer, down_rows, rank_cols),
            bf16(outer, down_rows, rank_cols),
            *sems(2, heads_here, 3, count),
            *sems(heads_here, 3),
            *sems(outer),
            *sems(inner),
            *sems(heads_here),
            *sems(heads_here, count),
            *sems(groups),
            *sems(up_groups),
            *sems(count),
            *sems(groups),
            *sems(outer),
            pltpu.SemaphoreType.DMA((8,)),
        ],
        compiler_params=pltpu.CompilerParams(
            collective_id=0, has_side_effects=True, vmem_limit_bytes=VMEM_LIMIT
        ),
        name="step",
    )(weights, *fields, hidden, hidden_cols, down, up, modulation)


def body(
    teacher_query,
    teacher_key,
    teacher_value,
    hidden,
    adapter_down_weight,
    adapter_up_weight,
    guidance_index,
    timestep_index,
):
    cfg_index = lax.axis_index("cfg")
    seq_count = lax.axis_size("seq")
    dp_count = lax.axis_size("dp")
    inner = inner_size(seq_count)
    outer = seq_count // inner
    tok_here, model_width = hidden.shape[2:]
    groups = 2 * inner * dp_count

    guide_scale = 1.0 + 0.5 * guidance_index[:, 0].astype(jnp.float32)
    time_frac = (timestep_index[:, 0].astype(jnp.float32) + 0.5) / TSTEPS
    own_scale = lax.dynamic_index_in_dim(guide_scale, cfg_index, 0, keepdims=False)
    own_time = lax.dynamic_index_in_dim(time_frac, cfg_index, 0, keepdims=False)
    weighting = jnp.where(cfg_index == 0, guide_scale, 1.0 - guide_scale)
    weights = jnp.where(cfg_index == 0, weighting, weighting[::-1])
    rank_index = jnp.arange(1, ADAPTER_RANK + 1).astype(jnp.float32)
    modulation = 1.0 + 0.5 * jnp.cos(
        math.pi * rank_index * own_time + 0.25 * rank_index * own_scale
    )

    own_hidden = hidden[0, 0]
    hidden_cols = own_hidden.reshape(tok_here, 2, outer, inner, dp_count, -1)
    hidden_cols = hidden_cols.transpose(1, 3, 4, 0, 2, 5).reshape(groups, tok_here, -1)
    student_tokens, grad_down, grad_up = run_step(
        (seq_count, inner, dp_count),
        weights,
        (teacher_query[0, :, 0], teacher_key[0, :, 0], teacher_value[0, :, 0]),
        own_hidden,
        hidden_cols,
        adapter_down_weight,
        adapter_up_weight,
        modulation[None],
    )
    return (student_tokens[None, None], grad_down, grad_up)


def solution(mesh):
    placed = (
        P("cfg", None, "dp", "seq", None),
        P("cfg", None, "dp", "seq", None),
        P("cfg", None, "dp", "seq", None),
        P("cfg", "dp", "seq", None),
        P(),
        P(),
        P(None, "dp"),
        P(None, "dp"),
    )
    return jax.shard_map(
        body,
        mesh=mesh,
        in_specs=placed,
        out_specs=(
            P("cfg", "dp", "seq", None),
            P(None, ("cfg", "seq", "dp"), None),
            P(None, ("cfg", "dp"), "seq"),
        ),
        check_vma=False,
    )
```

```python
import functools
import math

import jax
import jax.numpy as jnp
from jax import lax
from jax.experimental import pallas as pl
from jax.experimental.pallas import tpu as pltpu
from jax.sharding import PartitionSpec as P

HDIM = 128
ADAPTER_RANK = 128
TSTEPS = 1000
FACTOR = HDIM ** (-0.5)
FACTOR_BASE2 = FACTOR * math.log2(math.e)
VMEM_LIMIT = 60 * 1024 * 1024
BLOCK = 512
MESH = pl.DeviceIdType.MESH

NT = (((1,), (1,)), ((), ()))
TN = (((0,), (0,)), ((), ()))


def dot_f32(left, right):
    return jnp.dot(left, right, preferred_element_type=jnp.float32)


def dot_nt(left, right):
    return lax.dot_general(left, right, NT, preferred_element_type=jnp.float32)


def dot_tn(left, right):
    return lax.dot_general(left, right, TN, preferred_element_type=jnp.float32)


def inner_size(count):
    return max(size for size in range(1, count + 1) if count % size == 0 and size * size <= count)


def aligned(index, size):
    return pl.ds(pl.multiple_of(index * size, size), size)


def probs_by_key(key_head, query_block):
    scores = dot_nt(key_head, query_block)
    highest = jnp.max(scores, axis=0, keepdims=True)
    raised = jnp.exp2((scores - highest) * FACTOR_BASE2)
    return raised * (1.0 / jnp.sum(raised, axis=0, keepdims=True))


def step_kernel(
    sizes,
    out_scale,
    guide_ref,
    time_ref,
    query_ref,
    key_ref,
    value_ref,
    hidden_ref,
    down_ref,
    up_ref,
    tokens_ref,
    grad_down_ref,
    grad_up_ref,
    heads,
    hidden_own,
    hidden_cols,
    hidden_all,
    down_own,
    up_own,
    ranks,
    weighted,
    weighted_in,
    target,
    s_query,
    s_key,
    s_value,
    key_t,
    value_t,
    grad_query,
    grad_key,
    grad_value,
    back_sum,
    back,
    near_in,
    far_out,
    far_in,
    student,
    up_parts,
    up_in,
    low,
    low_all,
    down_out,
    down_in,
    field_send,
    field_recv,
    pass_send,
    pass_recv,
    rank_send,
    rank_recv,
    fan_send,
    fan_recv,
    swap_send,
    swap_recv,
    out_send,
    out_recv,
    cols_send,
    cols_recv,
    up_send,
    up_recv,
    near_send,
    near_recv,
    far_send,
    far_recv,
    low_send,
    low_recv,
    share_send,
    share_recv,
    down_send,
    down_recv,
    local_sem,
):
    count, inner, dp_count = sizes
    outer = count // inner
    pairs = 2 * inner
    groups = pairs * dp_count
    up_groups = 2 * dp_count
    fields = (query_ref, key_ref, value_ref)
    tok_here = query_ref.shape[1]
    length = tok_here * count
    columns = student.shape[1]
    heads_here = columns // HDIM
    step_rows = min(BLOCK, length)
    blocks = length // step_rows

    me = lax.axis_index("seq")
    cfg = lax.axis_index("cfg")
    dp = lax.axis_index("dp")
    other = 1 - cfg
    far = me // inner
    near = lax.rem(me, inner)
    pair = cfg * inner + near
    group = dp * pairs + pair
    up_group = cfg * dp_count + dp
    own_rows = aligned(me, tok_here)
    order = (other, cfg)

    def head_columns(head):
        return slice(head * HDIM, (head + 1) * HDIM)

    def seq_peer(step):
        return lax.rem(me + step, count)

    def device_of(pair_index):
        return {"cfg": pair_index // inner, "seq": far * inner + lax.rem(pair_index, inner)}

    def group_device(step):
        peer = lax.rem(group + step, groups)
        return {**device_of(lax.rem(peer, pairs)), "dp": peer // pairs}

    def remote(src, dst, send, recv, device):
        return pltpu.make_async_remote_copy(
            src_ref=src,
            dst_ref=dst,
            send_sem=send,
            recv_sem=recv,
            device_id=device,
            device_id_type=MESH,
        )

    loads = [
        pltpu.make_async_copy(hidden_ref, hidden_own, local_sem.at[0]),
        pltpu.make_async_copy(down_ref, down_own, local_sem.at[1]),
        pltpu.make_async_copy(
            up_ref.at[:, :, aligned(me, columns)], up_own, local_sem.at[2]
        ),
    ] + [
        pltpu.make_async_copy(
            fields[member].at[:, :, aligned(me, columns)],
            heads.at[member, 0:2, own_rows, :],
            local_sem.at[3 + member],
        )
        for member in range(3)
    ]
    for load in loads:
        load.start()

    barrier = pltpu.get_barrier_semaphore()
    for step in range(1, count):
        pl.semaphore_signal(
            barrier, inc=1, device_id={"seq": seq_peer(step)}, device_id_type=MESH
        )
    for step in range(1, groups):
        pl.semaphore_signal(barrier, inc=1, device_id=group_device(step), device_id_type=MESH)
    pl.semaphore_wait(barrier, count + groups - 2)

    def field_copy(phase, head, member, step):
        peer = seq_peer(step)
        half = order[phase]
        start = pl.multiple_of(peer * columns, columns) + head * HDIM
        return remote(
            fields[member].at[half, :, pl.ds(start, HDIM)],
            heads.at[member, half, own_rows, head_columns(head)],
            field_send.at[phase, head, member, step],
            field_recv.at[phase, head, member, step],
            {"seq": peer},
        )

    def start_fields(phase, head):
        for member in (1, 2, 0):
            for step in range(1, count):
                field_copy(phase, head, member, step).start()

    def wait_fields(phase, head):
        for member in (1, 2, 0):
            for step in range(1, count):
                field_copy(phase, head, member, step).wait_recv()

    def pass_copy(head, member):
        return remote(
            heads.at[member, 1, :, head_columns(head)],
            heads.at[member, 2, :, head_columns(head)],
            pass_send.at[head, member],
            pass_recv.at[head, member],
            {"cfg": other},
        )

    def rank_copy(step):
        return remote(
            ranks.at[far, near],
            ranks.at[far, near],
            rank_send.at[step],
            rank_recv.at[step],
            {"seq": lax.rem(far + step, outer) * inner + near},
        )

    def fan_copy(step):
        return remote(
            ranks.at[:, near],
            ranks.at[:, near],
            fan_send.at[step],
            fan_recv.at[step],
            {"seq": far * inner + lax.rem(near + step, inner)},
        )

    def swap_copy(head):
        return remote(
            weighted.at[head],
            weighted_in.at[head],
            swap_send.at[head],
            swap_recv.at[head],
            {"cfg": other},
        )

    def out_copy(head, step):
        peer = seq_peer(step)
        start = pl.multiple_of(me * columns, columns) + head * HDIM
        return remote(
            student.at[aligned(peer, tok_here), head_columns(head)],
            tokens_ref.at[:, pl.ds(start, HDIM)],
            out_send.at[head, step],
            out_recv.at[head, step],
            {"seq": peer},
        )

    def cols_copy(step):
        return remote(
            hidden_cols.at[lax.rem(group + step, groups)],
            hidden_all.at[group],
            cols_send.at[step],
            cols_recv.at[step],
            group_device(step),
        )

    def up_copy(step):
        peer = lax.rem(up_group + step, up_groups)
        return remote(
            up_parts.at[peer],
            up_in.at[step],
            up_send.at[step],
            up_recv.at[step],
            {"cfg": peer // dp_count, "dp": lax.rem(peer, dp_count)},
        )

    def near_copy(far_step, step):
        peer = lax.rem(near + step, inner)
        row = lax.rem(far + far_step, outer)
        return remote(
            back.at[aligned(row * inner + peer, tok_here), :],
            near_in.at[far_step, step],
            near_send.at[far_step, step],
            near_recv.at[far_step, step],
            {"seq": far * inner + peer},
        )

    def far_copy(step):
        return remote(
            far_out.at[step],
            far_in.at[step],
            far_send.at[step],
            far_recv.at[step],
            {"seq": lax.rem(far + step, outer) * inner + near},
        )

    def low_copy(step):
        return remote(
            low,
            low_all.at[group],
            low_send.at[step],
            low_recv.at[step],
            device_of(lax.rem(pair + step, pairs)),
        )

    def share_copy(pair_step, step):
        source = lax.rem(pair - pair_step + pairs, pairs)
        slot = low_all.at[dp * pairs + source]
        return remote(
            low if pair_step == 0 else slot,
            slot,
            share_send.at[pair_step, step],
            share_recv.at[pair_step, step],
            {"dp": lax.rem(dp + step, dp_count)},
        )

    def down_copy(step):
        peer = lax.rem(far + step, outer)
        return remote(
            down_out.at[peer],
            down_in.at[step],
            down_send.at[step],
            down_recv.at[step],
            {"seq": peer * inner + near},
        )

    def guide_scale(half):
        return 1.0 + 0.5 * guide_ref[half].astype(jnp.float32)

    def weighting(half):
        scale = guide_scale(half)
        return jnp.where(cfg == 0, scale, 1.0 - scale)

    rank_index = (lax.broadcasted_iota(jnp.int32, (1, ADAPTER_RANK), 1) + 1).astype(jnp.float32)
    time_frac = (time_ref[cfg].astype(jnp.float32) + 0.5) / TSTEPS
    modulation = 1.0 + 0.5 * jnp.cos(
        math.pi * rank_index * time_frac + 0.25 * rank_index * guide_scale(cfg)
    )

    phases = [(phase, head) for phase in range(2) for head in range(heads_here)]
    start_fields(*phases[0])

    loads[0].wait()
    loads[1].wait()
    for member in range(3):
        projected = dot_f32(hidden_own[...], down_own[member]) * modulation
        ranks[far, near, :, head_columns(member)] = projected.astype(jnp.bfloat16)
    for step in range(1, outer):
        rank_copy(step).start()
    start_fields(*phases[1])
    rows_here = hidden_cols.shape[2] // outer
    for block in range(outer * groups):
        target_dp = block % dp_count
        target_near = block // dp_count % inner
        target_far = block // dp_count // inner % outer
        target_pair = block // (dp_count * count) * inner + target_near
        hidden_cols[
            target_dp * pairs + target_pair, :, target_far * rows_here : (target_far + 1) * rows_here
        ] = hidden_own[:, block * rows_here : (block + 1) * rows_here]
    hidden_all[group] = hidden_cols[group]
    for step in range(1, outer):
        rank_copy(step).wait_recv()
    for step in range(1, inner):
        fan_copy(step).start()
    for step in range(1, groups):
        cols_copy(step).start()
    for phase, head in phases[2:]:
        start_fields(phase, head)
    for load in loads[2:]:
        load.wait()

    far_order = sorted(range(outer), key=lambda step: (step == 0, abs(2 * step - outer)))

    def run_blocks(one_block):
        unroll = 2 if blocks % 2 == 0 else 1

        def some(step, _):
            for offset in range(unroll):
                one_block(step * unroll + offset)
            return 0

        lax.fori_loop(0, blocks // unroll, some, 0)

    def teacher(half, head, store):
        lanes = head_columns(head)
        value_t[...] = heads[2, half, :, lanes].T

        def one_block(step):
            rows = aligned(step, step_rows)
            weights = probs_by_key(heads[1, half, :, lanes], heads[0, half, rows, lanes])
            attended = dot_f32(value_t[...], weights.astype(jnp.bfloat16)).T
            store(rows, attended.astype(jnp.bfloat16).astype(jnp.float32))

        run_blocks(one_block)

    for head in range(heads_here):
        wait_fields(0, head)

        @pl.when(cfg == 0)
        def _():
            for member in range(3):
                pass_copy(head, member).start()

        def store_other(rows, attended):
            weighted[head, rows, :] = (weighting(other) * attended).astype(jnp.bfloat16)

        teacher(other, head, store_other)
        swap_copy(head).start()

    for step in range(1, inner):
        fan_copy(step).wait_recv()

    for head in range(heads_here):
        lanes = head_columns(head)
        wait_fields(1, head)

        def store_own(rows, attended):
            target[rows, :] = weighting(cfg) * attended

        teacher(cfg, head, store_own)

        @pl.when(cfg == 1)
        def _():
            for member in range(3):
                pass_copy(head, member).wait_recv()

        for member, projected in enumerate((s_query, s_key, s_value)):
            low_rank = ranks[:, :, :, head_columns(member)].reshape(length, ADAPTER_RANK)
            frozen = heads[member, 2 * cfg, :, lanes].astype(jnp.float32)
            projected[...] = (frozen + dot_f32(low_rank, up_own[member, :, lanes])).astype(
                jnp.bfloat16
            )
        key_t[...] = s_key[...].T
        value_t[...] = s_value[...].T
        grad_key[...] = jnp.zeros_like(grad_key)
        grad_value[...] = jnp.zeros_like(grad_value)
        swap_copy(head).wait_recv()

        def one_block(step):
            rows = aligned(step, step_rows)
            query_block = s_query[rows, :]
            probability = probs_by_key(s_key[...], query_block)
            weights = probability.astype(jnp.bfloat16)
            attended = dot_f32(value_t[...], weights).T.astype(jnp.bfloat16)
            student[rows, lanes] = attended
            aim = target[rows, :] + weighted_in[head, rows, :].astype(jnp.float32)
            upstream = ((attended.astype(jnp.float32) - aim) * out_scale).astype(jnp.bfloat16)
            grad_value[...] += dot_f32(weights, upstream)
            prob_grad = dot_nt(s_value[...], upstream)
            center = jnp.sum(probability * prob_grad, axis=0, keepdims=True)
            score_grad = (probability * (prob_grad - center)).astype(jnp.bfloat16)
            grad_key[...] += dot_f32(score_grad, query_block)
            grad_query[rows, :] = (dot_f32(key_t[...], score_grad).T * FACTOR).astype(
                jnp.bfloat16
            )

        run_blocks(one_block)
        if head < heads_here - 1:
            for step in range(1, count):
                out_copy(head, step).start()

        gradients = (
            grad_query[...],
            (grad_key[...] * FACTOR).astype(jnp.bfloat16),
            grad_value[...].astype(jnp.bfloat16),
        )
        for member, gradient in enumerate(gradients):
            part = dot_nt(gradient, up_own[member, :, lanes])
            if head > 0:
                part = part + back_sum[:, head_columns(member)]
            if head < heads_here - 1:
                back_sum[:, head_columns(member)] = part
            else:
                back[:, head_columns(member)] = part.astype(jnp.bfloat16)
        if head == heads_here - 1:
            for far_step in far_order:
                for step in range(1, inner):
                    near_copy(far_step, step).start()
        for member, gradient in enumerate(gradients):
            low_rank = ranks[:, :, :, head_columns(member)].reshape(length, ADAPTER_RANK)
            part = dot_tn(low_rank, gradient).astype(jnp.bfloat16)
            up_parts[:, member, :, lanes] = part.reshape(up_groups, -1, HDIM)

    for far_step in far_order:
        row = lax.rem(far + far_step, outer)
        part = back[aligned(row * inner + near, tok_here), :].astype(jnp.float32)
        for step in range(1, inner):
            near_copy(far_step, step).wait_recv()
            part = part + near_in[far_step, step].astype(jnp.float32)
        if far_step > 0:
            far_out[far_step] = part.astype(jnp.bfloat16)
            far_copy(far_step).start()
        else:
            total = part
    for step in range(1, count):
        out_copy(heads_here - 1, step).start()
    for step in range(1, up_groups):
        up_copy(step).start()
    own_store = pltpu.make_async_copy(
        student.at[own_rows, :], tokens_ref.at[:, aligned(me, columns)], local_sem.at[6]
    )
    own_store.start()

    for step in range(1, outer):
        far_copy(step).wait_recv()
        total = total + far_in[step].astype(jnp.float32)
    scale = jnp.concatenate([modulation] * 3, axis=1)
    low_grad = (total * scale).astype(jnp.bfloat16)
    low[...] = low_grad
    low_all[group] = low_grad
    for step in range(1, pairs):
        low_copy(step).start()
    for step in range(1, dp_count):
        share_copy(0, step).start()
    for pair_step in range(1, pairs):
        low_copy(pair_step).wait_recv()
        for step in range(1, dp_count):
            share_copy(pair_step, step).start()

    up_total = up_parts[up_group].astype(jnp.float32)
    for step in range(1, up_groups):
        up_copy(step).wait_recv()
        up_total = up_total + up_in[step].astype(jnp.float32)
    grad_up_ref[...] = up_total

    for step in range(1, groups):
        cols_copy(step).wait_recv()
    for pair_step in range(pairs):
        for step in range(1, dp_count):
            share_copy(pair_step, step).wait_recv()
    gathered_cols = hidden_all[...].reshape(groups * tok_here, -1)
    gathered_low = low_all[...].reshape(groups * tok_here, -1)
    down_rows = gathered_cols.shape[1] // outer
    partial = dot_tn(gathered_cols, gathered_low).astype(jnp.bfloat16)
    for peer in range(outer):
        down_out[peer] = partial[peer * down_rows : (peer + 1) * down_rows, :]
    for step in range(1, outer):
        down_copy(step).start()
    down_total = down_out[far].astype(jnp.float32)
    for step in range(1, outer):
        down_copy(step).wait_recv()
        down_total = down_total + down_in[step].astype(jnp.float32)
    for member in range(3):
        grad_down_ref[member] = down_total[:, head_columns(member)]

    own_store.wait()
    for phase, head in phases:
        for member in range(3):
            for step in range(1, count):
                field_copy(phase, head, member, step).wait_send()
    for head in range(heads_here):
        swap_copy(head).wait_send()

        @pl.when(cfg == 0)
        def _():
            for member in range(3):
                pass_copy(head, member).wait_send()

        for step in range(1, count):
            out_copy(head, step).wait()
    for step in range(1, outer):
        rank_copy(step).wait_send()
        down_copy(step).wait_send()
    for step in range(1, inner):
        fan_copy(step).wait_send()
    for step in range(1, groups):
        cols_copy(step).wait_send()
    for pair_step in range(pairs):
        if pair_step > 0:
            low_copy(pair_step).wait_send()
        for step in range(1, dp_count):
            share_copy(pair_step, step).wait_send()
    for step in range(1, up_groups):
        up_copy(step).wait_send()
    for far_step in range(outer):
        if far_step > 0:
            far_copy(far_step).wait_send()
        for step in range(1, inner):
            near_copy(far_step, step).wait_send()


def run_step(sizes, guide, time_index, fields, hidden, down, up):
    count, inner, dp_count = sizes
    outer = count // inner
    pairs = 2 * inner
    groups = pairs * dp_count
    up_groups = 2 * dp_count
    tok_here, width = fields[0].shape[1:]
    model_width = hidden.shape[1]
    length, columns = tok_here * count, width // count
    heads_here = columns // HDIM
    rank_cols = 3 * ADAPTER_RANK
    group_cols = model_width // groups
    down_rows = group_cols // outer
    up_rows = ADAPTER_RANK // up_groups
    any_spec = pl.BlockSpec(memory_space=pl.ANY)
    vmem_spec = pl.BlockSpec(memory_space=pltpu.VMEM)
    smem_spec = pl.BlockSpec(memory_space=pltpu.SMEM)

    def bf16(*shape):
        return pltpu.VMEM(shape, jnp.bfloat16)

    def f32(*shape):
        return pltpu.VMEM(shape, jnp.float32)

    def sems(*shape):
        return [pltpu.SemaphoreType.DMA(shape)] * 2

    total_rows = 2 * dp_count * length
    return pl.pallas_call(
        functools.partial(step_kernel, sizes, 1.0 / math.sqrt(total_rows)),
        out_shape=(
            jax.ShapeDtypeStruct((tok_here, width), jnp.bfloat16),
            jax.ShapeDtypeStruct((3, down_rows, ADAPTER_RANK), jnp.float32),
            jax.ShapeDtypeStruct((3, up_rows, columns), jnp.float32),
        ),
        in_specs=[smem_spec] * 2 + [any_spec] * 6,
        out_specs=(any_spec, vmem_spec, vmem_spec),
        scratch_shapes=[
            bf16(3, 3, length, columns),
            bf16(tok_here, model_width),
            bf16(groups, tok_here, group_cols),
            bf16(groups, tok_here, group_cols),
            bf16(3, model_width, ADAPTER_RANK),
            bf16(3, ADAPTER_RANK, columns),
            bf16(outer, inner, tok_here, rank_cols),
            bf16(heads_here, length, HDIM),
            bf16(heads_here, length, HDIM),
            f32(length, HDIM),
            bf16(length, HDIM),
            bf16(length, HDIM),
            bf16(length, HDIM),
            bf16(HDIM, length),
            bf16(HDIM, length),
            bf16(length, HDIM),
            f32(length, HDIM),
            f32(length, HDIM),
            f32(length, rank_cols),
            bf16(length, rank_cols),
            bf16(outer, inner, tok_here, rank_cols),
            bf16(outer, tok_here, rank_cols),
            bf16(outer, tok_here, rank_cols),
            bf16(length, columns),
            bf16(up_groups, 3, up_rows, columns),
            bf16(up_groups, 3, up_rows, columns),
            bf16(tok_here, rank_cols),
            bf16(groups, tok_here, rank_cols),
            bf16(outer, down_rows, rank_cols),
            bf16(outer, down_rows, rank_cols),
            *sems(2, heads_here, 3, count),
            *sems(heads_here, 3),
            *sems(outer),
            *sems(inner),
            *sems(heads_here),
            *sems(heads_here, count),
            *sems(groups),
            *sems(up_groups),
            *sems(outer, inner),
            *sems(outer),
            *sems(pairs),
            *sems(pairs, dp_count),
            *sems(outer),
            pltpu.SemaphoreType.DMA((7,)),
        ],
        compiler_params=pltpu.CompilerParams(
            collective_id=0, has_side_effects=True, vmem_limit_bytes=VMEM_LIMIT
        ),
        name="step",
    )(guide, time_index, *fields, hidden, down, up)


def emit_kernel(*refs):
    half = len(refs) // 2
    sems = refs[-1]
    copies = [
        pltpu.make_async_copy(refs[item], refs[half + item], sems.at[item])
        for item in range(half)
    ]
    for copy in copies:
        copy.start()
    for copy in copies:
        copy.wait()


def emit(arrays):
    return pl.pallas_call(
        emit_kernel,
        out_shape=tuple(jax.ShapeDtypeStruct(array.shape, array.dtype) for array in arrays),
        in_specs=[pl.BlockSpec(memory_space=pltpu.VMEM)] * len(arrays),
        out_specs=(pl.BlockSpec(memory_space=pl.ANY),) * len(arrays),
        scratch_shapes=[pltpu.SemaphoreType.DMA((len(arrays),))],
        compiler_params=pltpu.CompilerParams(vmem_limit_bytes=4 * 1024 * 1024),
        name="emit",
    )(*arrays)


def body(
    teacher_query,
    teacher_key,
    teacher_value,
    hidden,
    adapter_down_weight,
    adapter_up_weight,
    guidance_index,
    timestep_index,
):
    seq_count = lax.axis_size("seq")
    outputs = run_step(
        (seq_count, inner_size(seq_count), lax.axis_size("dp")),
        guidance_index[:, 0],
        timestep_index[:, 0],
        (teacher_query[0, :, 0], teacher_key[0, :, 0], teacher_value[0, :, 0]),
        hidden[0, 0],
        adapter_down_weight,
        adapter_up_weight,
    )
    student_tokens, grad_down, grad_up = emit(outputs)
    return (student_tokens[None, None], grad_down, grad_up)


def solution(mesh):
    placed = (
        P("cfg", None, "dp", "seq", None),
        P("cfg", None, "dp", "seq", None),
        P("cfg", None, "dp", "seq", None),
        P("cfg", "dp", "seq", None),
        P(),
        P(),
        P(None, "dp"),
        P(None, "dp"),
    )
    return jax.shard_map(
        body,
        mesh=mesh,
        in_specs=placed,
        out_specs=(
            P("cfg", "dp", "seq", None),
            P(None, ("cfg", "seq", "dp"), None),
            P(None, ("cfg", "dp"), "seq"),
        ),
        check_vma=False,
    )
```

```python
import functools
import math

import jax
import jax.numpy as jnp
from jax import lax
from jax.experimental import pallas as pl
from jax.experimental.pallas import tpu as pltpu
from jax.sharding import PartitionSpec as P

HDIM = 128
ADAPTER_RANK = 128
TSTEPS = 1000
FACTOR = HDIM ** (-0.5)
FACTOR_BASE2 = FACTOR * math.log2(math.e)
VMEM_LIMIT = 60 * 1024 * 1024
BLOCK = 512
MESH = pl.DeviceIdType.MESH

NT = (((1,), (1,)), ((), ()))
TN = (((0,), (0,)), ((), ()))


def dot_f32(left, right):
    return jnp.dot(left, right, preferred_element_type=jnp.float32)


def dot_nt(left, right):
    return lax.dot_general(left, right, NT, preferred_element_type=jnp.float32)


def dot_tn(left, right):
    return lax.dot_general(left, right, TN, preferred_element_type=jnp.float32)


def inner_size(count):
    return max(size for size in range(1, count + 1) if count % size == 0 and size * size <= count)


def aligned(index, size):
    return pl.ds(pl.multiple_of(index * size, size), size)


def probs_by_key(key_head, query_block):
    scores = dot_nt(key_head, query_block)
    highest = jnp.max(scores, axis=0, keepdims=True)
    raised = jnp.exp2((scores - highest) * FACTOR_BASE2)
    return raised * (1.0 / jnp.sum(raised, axis=0, keepdims=True))


def step_kernel(
    sizes,
    out_scale,
    guide_ref,
    time_ref,
    query_ref,
    key_ref,
    value_ref,
    hidden_ref,
    down_ref,
    up_ref,
    tokens_ref,
    grad_down_ref,
    grad_up_ref,
    heads,
    hidden_own,
    hidden_cols,
    hidden_all,
    hidden_t,
    down_own,
    up_own,
    ranks,
    weighted,
    weighted_in,
    target,
    s_query,
    s_key,
    s_value,
    key_t,
    value_t,
    grad_query,
    grad_key,
    grad_value,
    back_sum,
    back,
    near_in,
    far_out,
    far_in,
    student,
    up_parts,
    up_in,
    low,
    low_all,
    down_out,
    down_in,
    field_send,
    field_recv,
    pass_send,
    pass_recv,
    rank_send,
    rank_recv,
    fan_send,
    fan_recv,
    swap_send,
    swap_recv,
    out_send,
    out_recv,
    cols_send,
    cols_recv,
    up_send,
    up_recv,
    near_send,
    near_recv,
    far_send,
    far_recv,
    low_send,
    low_recv,
    share_send,
    share_recv,
    down_send,
    down_recv,
    local_sem,
):
    count, inner, dp_count = sizes
    outer = count // inner
    pairs = 2 * inner
    groups = pairs * dp_count
    up_groups = 2 * dp_count
    fields = (query_ref, key_ref, value_ref)
    tok_here = query_ref.shape[1]
    length = tok_here * count
    columns = student.shape[1]
    heads_here = columns // HDIM
    step_rows = min(BLOCK, length)
    blocks = length // step_rows

    me = lax.axis_index("seq")
    cfg = lax.axis_index("cfg")
    dp = lax.axis_index("dp")
    other = 1 - cfg
    far = me // inner
    near = lax.rem(me, inner)
    pair = cfg * inner + near
    group = dp * pairs + pair
    up_group = cfg * dp_count + dp
    own_rows = aligned(me, tok_here)
    order = (other, cfg)

    def head_columns(head):
        return slice(head * HDIM, (head + 1) * HDIM)

    def seq_peer(step):
        return lax.rem(me + step, count)

    def device_of(pair_index):
        return {"cfg": pair_index // inner, "seq": far * inner + lax.rem(pair_index, inner)}

    def group_device(step):
        peer = lax.rem(group + step, groups)
        return {**device_of(lax.rem(peer, pairs)), "dp": peer // pairs}

    def remote(src, dst, send, recv, device):
        return pltpu.make_async_remote_copy(
            src_ref=src,
            dst_ref=dst,
            send_sem=send,
            recv_sem=recv,
            device_id=device,
            device_id_type=MESH,
        )

    loads = [
        pltpu.make_async_copy(hidden_ref, hidden_own, local_sem.at[0]),
        pltpu.make_async_copy(down_ref, down_own, local_sem.at[1]),
        pltpu.make_async_copy(
            up_ref.at[:, :, aligned(me, columns)], up_own, local_sem.at[2]
        ),
    ] + [
        pltpu.make_async_copy(
            fields[member].at[:, :, aligned(me, columns)],
            heads.at[member, 0:2, own_rows, :],
            local_sem.at[3 + member],
        )
        for member in range(3)
    ]
    for load in loads:
        load.start()

    barrier = pltpu.get_barrier_semaphore()
    for step in range(1, count):
        pl.semaphore_signal(
            barrier, inc=1, device_id={"seq": seq_peer(step)}, device_id_type=MESH
        )
    for step in range(1, groups):
        pl.semaphore_signal(barrier, inc=1, device_id=group_device(step), device_id_type=MESH)
    def field_copy(phase, head, member, step):
        peer = seq_peer(step)
        half = order[phase]
        start = pl.multiple_of(peer * columns, columns) + head * HDIM
        return remote(
            fields[member].at[half, :, pl.ds(start, HDIM)],
            heads.at[member, half, own_rows, head_columns(head)],
            field_send.at[phase, head, member, step],
            field_recv.at[phase, head, member, step],
            {"seq": peer},
        )

    def start_fields(phase, head, member):
        for step in range(1, count):
            field_copy(phase, head, member, step).start()

    def wait_fields(phase, head):
        for member in (1, 2, 0):
            for step in range(1, count):
                field_copy(phase, head, member, step).wait_recv()

    def pass_copy(head, member):
        return remote(
            heads.at[member, 1, :, head_columns(head)],
            heads.at[member, 2, :, head_columns(head)],
            pass_send.at[head, member],
            pass_recv.at[head, member],
            {"cfg": other},
        )

    def rank_copy(way, hop):
        toward, back_by = (1, outer - hop) if way == 0 else (outer - 1, hop)
        block = ranks.at[lax.rem(far + back_by, outer), near]
        return remote(
            block,
            block,
            rank_send.at[way, hop],
            rank_recv.at[way, hop],
            {"seq": lax.rem(far + toward, outer) * inner + near},
        )

    def ranks_leave(way, hop):
        if way == 0:
            return jnp.logical_and(far >= hop, far < outer - 1)
        return jnp.logical_and(far < outer - hop, far > 0)

    def ranks_come(way, hop):
        return far > hop if way == 0 else far < outer - 1 - hop

    def rank_step(hop, action, test):
        for way in range(2):

            @pl.when(test(way, hop))
            def _():
                getattr(rank_copy(way, hop), action)()

    def fan_copy(step):
        return remote(
            ranks.at[:, near],
            ranks.at[:, near],
            fan_send.at[step],
            fan_recv.at[step],
            {"seq": far * inner + lax.rem(near + step, inner)},
        )

    def swap_copy(head):
        return remote(
            weighted.at[head],
            weighted_in.at[head],
            swap_send.at[head],
            swap_recv.at[head],
            {"cfg": other},
        )

    def out_copy(head, step):
        peer = seq_peer(step)
        start = pl.multiple_of(me * columns, columns) + head * HDIM
        return remote(
            student.at[aligned(peer, tok_here), head_columns(head)],
            tokens_ref.at[:, pl.ds(start, HDIM)],
            out_send.at[head, step],
            out_recv.at[head, step],
            {"seq": peer},
        )

    def cols_copy(step):
        return remote(
            hidden_cols.at[lax.rem(group + step, groups)],
            hidden_all.at[group],
            cols_send.at[step],
            cols_recv.at[step],
            group_device(step),
        )

    def up_copy(step):
        peer = lax.rem(up_group + step, up_groups)
        return remote(
            up_parts.at[peer],
            up_in.at[step],
            up_send.at[step],
            up_recv.at[step],
            {"cfg": peer // dp_count, "dp": lax.rem(peer, dp_count)},
        )

    def near_copy(member, far_step, step):
        peer = lax.rem(near + step, inner)
        row = lax.rem(far + far_step, outer)
        return remote(
            back.at[aligned(row * inner + peer, tok_here), head_columns(member)],
            near_in.at[far_step, step, :, head_columns(member)],
            near_send.at[member, far_step, step],
            near_recv.at[member, far_step, step],
            {"seq": far * inner + peer},
        )

    def far_copy(member, step):
        return remote(
            far_out.at[step, :, head_columns(member)],
            far_in.at[step, :, head_columns(member)],
            far_send.at[member, step],
            far_recv.at[member, step],
            {"seq": lax.rem(far + step, outer) * inner + near},
        )

    def low_copy(member, step):
        return remote(
            low.at[:, head_columns(member)],
            low_all.at[group, :, head_columns(member)],
            low_send.at[member, step],
            low_recv.at[member, step],
            device_of(lax.rem(pair + step, pairs)),
        )

    def share_copy(member, pair_step, step):
        source = lax.rem(pair - pair_step + pairs, pairs)
        lanes = head_columns(member)
        slot = low_all.at[dp * pairs + source, :, lanes]
        return remote(
            low.at[:, lanes] if pair_step == 0 else slot,
            slot,
            share_send.at[member, pair_step, step],
            share_recv.at[member, pair_step, step],
            {"dp": lax.rem(dp + step, dp_count)},
        )

    def down_copy(member, step):
        peer = lax.rem(far + step, outer)
        return remote(
            down_out.at[peer, :, head_columns(member)],
            down_in.at[step, :, head_columns(member)],
            down_send.at[member, step],
            down_recv.at[member, step],
            {"seq": peer * inner + near},
        )

    def guide_scale(half):
        return 1.0 + 0.5 * guide_ref[half].astype(jnp.float32)

    def weighting(half):
        scale = guide_scale(half)
        return jnp.where(cfg == 0, scale, 1.0 - scale)

    rank_index = (lax.broadcasted_iota(jnp.int32, (1, ADAPTER_RANK), 1) + 1).astype(jnp.float32)
    time_frac = (time_ref[cfg].astype(jnp.float32) + 0.5) / TSTEPS
    modulation = 1.0 + 0.5 * jnp.cos(
        math.pi * rank_index * time_frac + 0.25 * rank_index * guide_scale(cfg)
    )

    phases = [(phase, head) for phase in range(2) for head in range(heads_here)]
    loads[0].wait()
    loads[1].wait()
    for member in range(3):
        projected = dot_f32(hidden_own[...], down_own[member]) * modulation
        ranks[far, near, :, head_columns(member)] = projected.astype(jnp.bfloat16)
    pl.semaphore_wait(barrier, count + groups - 2)

    sends = [(phase, head, member) for phase, head in phases for member in (1, 2, 0)]
    sent = 0
    for hop in range(outer - 1):
        if hop > 0:
            rank_step(hop - 1, "wait_recv", ranks_come)
        rank_step(hop, "start", ranks_leave)
        start_fields(*sends[sent])
        sent += 1
    for turn in sends[sent : 2 * sent]:
        start_fields(*turn)
    rank_step(outer - 2, "wait_recv", ranks_come)
    for step in range(1, inner):
        fan_copy(step).start()
    for turn in sends[2 * sent :]:
        start_fields(*turn)
    rows_here = hidden_cols.shape[2] // outer
    for block in range(outer * groups):
        target_dp = block % dp_count
        target_near = block // dp_count % inner
        target_far = block // dp_count // inner % outer
        target_pair = block // (dp_count * count) * inner + target_near
        hidden_cols[
            target_dp * pairs + target_pair, :, target_far * rows_here : (target_far + 1) * rows_here
        ] = hidden_own[:, block * rows_here : (block + 1) * rows_here]
    hidden_all[group] = hidden_cols[group]
    for step in range(1, groups):
        cols_copy(step).start()
    for load in loads[2:]:
        load.wait()

    far_order = sorted(range(outer), key=lambda step: (step == 0, abs(2 * step - outer)))

    def run_blocks(one_block):
        unroll = 2 if blocks % 2 == 0 else 1

        def some(step, _):
            for offset in range(unroll):
                one_block(step * unroll + offset)
            return 0

        lax.fori_loop(0, blocks // unroll, some, 0)

    def teacher(half, head, store):
        lanes = head_columns(head)
        value_t[...] = heads[2, half, :, lanes].T

        def one_block(step):
            rows = aligned(step, step_rows)
            weights = probs_by_key(heads[1, half, :, lanes], heads[0, half, rows, lanes])
            attended = dot_f32(value_t[...], weights.astype(jnp.bfloat16)).T
            store(rows, attended.astype(jnp.bfloat16).astype(jnp.float32))

        run_blocks(one_block)

    for head in range(heads_here):
        wait_fields(0, head)

        @pl.when(cfg == 0)
        def _():
            for member in range(3):
                pass_copy(head, member).start()

        def store_other(rows, attended):
            weighted[head, rows, :] = (weighting(other) * attended).astype(jnp.bfloat16)

        teacher(other, head, store_other)
        swap_copy(head).start()

    for step in range(1, inner):
        fan_copy(step).wait_recv()

    for head in range(heads_here):
        lanes = head_columns(head)
        wait_fields(1, head)

        def store_own(rows, attended):
            target[rows, :] = weighting(cfg) * attended

        teacher(cfg, head, store_own)

        @pl.when(cfg == 1)
        def _():
            for member in range(3):
                pass_copy(head, member).wait_recv()

        for member, projected in enumerate((s_query, s_key, s_value)):
            low_rank = ranks[:, :, :, head_columns(member)].reshape(length, ADAPTER_RANK)
            frozen = heads[member, 2 * cfg, :, lanes].astype(jnp.float32)
            projected[...] = (frozen + dot_f32(low_rank, up_own[member, :, lanes])).astype(
                jnp.bfloat16
            )
        key_t[...] = s_key[...].T
        value_t[...] = s_value[...].T
        grad_key[...] = jnp.zeros_like(grad_key)
        grad_value[...] = jnp.zeros_like(grad_value)
        swap_copy(head).wait_recv()

        def one_block(step):
            rows = aligned(step, step_rows)
            query_block = s_query[rows, :]
            probability = probs_by_key(s_key[...], query_block)
            weights = probability.astype(jnp.bfloat16)
            attended = dot_f32(value_t[...], weights).T.astype(jnp.bfloat16)
            student[rows, lanes] = attended
            aim = target[rows, :] + weighted_in[head, rows, :].astype(jnp.float32)
            upstream = ((attended.astype(jnp.float32) - aim) * out_scale).astype(jnp.bfloat16)
            grad_value[...] += dot_f32(weights, upstream)
            prob_grad = dot_nt(s_value[...], upstream)
            center = jnp.sum(probability * prob_grad, axis=0, keepdims=True)
            score_grad = (probability * (prob_grad - center)).astype(jnp.bfloat16)
            grad_key[...] += dot_f32(score_grad, query_block)
            grad_query[rows, :] = (dot_f32(key_t[...], score_grad).T * FACTOR).astype(
                jnp.bfloat16
            )

        run_blocks(one_block)
        if head < heads_here - 1:
            for step in range(1, count):
                out_copy(head, step).start()

        gradients = (
            grad_query[...],
            (grad_key[...] * FACTOR).astype(jnp.bfloat16),
            grad_value[...].astype(jnp.bfloat16),
        )
        for member, gradient in enumerate(gradients):
            part = dot_nt(gradient, up_own[member, :, lanes])
            if head > 0:
                part = part + back_sum[:, head_columns(member)]
            if head < heads_here - 1:
                back_sum[:, head_columns(member)] = part
            else:
                back[:, head_columns(member)] = part.astype(jnp.bfloat16)
                for far_step in far_order:
                    for step in range(1, inner):
                        near_copy(member, far_step, step).start()
        if head == heads_here - 1:
            for step in range(1, count):
                out_copy(head, step).start()
        for member, gradient in enumerate(gradients):
            low_rank = ranks[:, :, :, head_columns(member)].reshape(length, ADAPTER_RANK)
            part = dot_tn(low_rank, gradient).astype(jnp.bfloat16)
            up_parts[:, member, :, lanes] = part.reshape(up_groups, -1, HDIM)

    for step in range(1, up_groups):
        up_copy(step).start()
    own_store = pltpu.make_async_copy(
        student.at[own_rows, :], tokens_ref.at[:, aligned(me, columns)], local_sem.at[6]
    )
    own_store.start()
    for step in range(1, groups):
        cols_copy(step).wait_recv()
    gathered_cols = hidden_all[...].reshape(groups * tok_here, -1)
    hidden_t[...] = gathered_cols.T
    down_rows = gathered_cols.shape[1] // outer

    def reduce_near(member):
        lanes = head_columns(member)
        for far_step in far_order:
            row = lax.rem(far + far_step, outer)
            part = back[aligned(row * inner + near, tok_here), lanes].astype(jnp.float32)
            for step in range(1, inner):
                near_copy(member, far_step, step).wait_recv()
                part = part + near_in[far_step, step, :, lanes].astype(jnp.float32)
            if far_step > 0:
                far_out[far_step, :, lanes] = part.astype(jnp.bfloat16)
                far_copy(member, far_step).start()
        return part

    def reduce_far(member, total):
        lanes = head_columns(member)
        for step in range(1, outer):
            far_copy(member, step).wait_recv()
            total = total + far_in[step, :, lanes].astype(jnp.float32)
        low_grad = (total * modulation).astype(jnp.bfloat16)
        low[:, lanes] = low_grad
        low_all[group, :, lanes] = low_grad
        for step in range(1, pairs):
            low_copy(member, step).start()
        for step in range(1, dp_count):
            share_copy(member, 0, step).start()

    def spread(member):
        for pair_step in range(1, pairs):
            low_copy(member, pair_step).wait_recv()
            for step in range(1, dp_count):
                share_copy(member, pair_step, step).start()

    def contract(member):
        lanes = head_columns(member)
        for pair_step in range(pairs):
            for step in range(1, dp_count):
                share_copy(member, pair_step, step).wait_recv()
        gathered_low = low_all[:, :, lanes].reshape(groups * tok_here, ADAPTER_RANK)
        partial = dot_f32(hidden_t[...], gathered_low).astype(jnp.bfloat16)
        for peer in range(outer):
            down_out[peer, :, lanes] = partial[peer * down_rows : (peer + 1) * down_rows, :]
        for step in range(1, outer):
            down_copy(member, step).start()

    totals = {}
    for turn in range(6):
        if turn < 3:
            totals[turn] = reduce_near(turn)
        if 1 <= turn < 4:
            reduce_far(turn - 1, totals[turn - 1])
        if 2 <= turn < 5:
            spread(turn - 2)
        if turn >= 3:
            contract(turn - 3)

    up_total = up_parts[up_group].astype(jnp.float32)
    for step in range(1, up_groups):
        up_copy(step).wait_recv()
        up_total = up_total + up_in[step].astype(jnp.float32)
    grad_up_ref[...] = up_total

    for member in range(3):
        lanes = head_columns(member)
        down_total = down_out[far, :, lanes].astype(jnp.float32)
        for step in range(1, outer):
            down_copy(member, step).wait_recv()
            down_total = down_total + down_in[step, :, lanes].astype(jnp.float32)
        grad_down_ref[member] = down_total

    own_store.wait()
    for phase, head in phases:
        for member in range(3):
            for step in range(1, count):
                field_copy(phase, head, member, step).wait_send()
    for head in range(heads_here):
        swap_copy(head).wait_send()

        @pl.when(cfg == 0)
        def _():
            for member in range(3):
                pass_copy(head, member).wait_send()

        for step in range(1, count):
            out_copy(head, step).wait()
    for hop in range(outer - 1):
        rank_step(hop, "wait_send", ranks_leave)
    for step in range(1, inner):
        fan_copy(step).wait_send()
    for step in range(1, groups):
        cols_copy(step).wait_send()
    for step in range(1, up_groups):
        up_copy(step).wait_send()
    for member in range(3):
        for pair_step in range(pairs):
            if pair_step > 0:
                low_copy(member, pair_step).wait_send()
            for step in range(1, dp_count):
                share_copy(member, pair_step, step).wait_send()
        for far_step in range(outer):
            if far_step > 0:
                far_copy(member, far_step).wait_send()
                down_copy(member, far_step).wait_send()
            for step in range(1, inner):
                near_copy(member, far_step, step).wait_send()


def run_step(sizes, guide, time_index, fields, hidden, down, up):
    count, inner, dp_count = sizes
    outer = count // inner
    pairs = 2 * inner
    groups = pairs * dp_count
    up_groups = 2 * dp_count
    tok_here, width = fields[0].shape[1:]
    model_width = hidden.shape[1]
    length, columns = tok_here * count, width // count
    heads_here = columns // HDIM
    rank_cols = 3 * ADAPTER_RANK
    group_cols = model_width // groups
    down_rows = group_cols // outer
    up_rows = ADAPTER_RANK // up_groups
    any_spec = pl.BlockSpec(memory_space=pl.ANY)
    vmem_spec = pl.BlockSpec(memory_space=pltpu.VMEM)
    smem_spec = pl.BlockSpec(memory_space=pltpu.SMEM)

    def bf16(*shape):
        return pltpu.VMEM(shape, jnp.bfloat16)

    def f32(*shape):
        return pltpu.VMEM(shape, jnp.float32)

    def sems(*shape):
        return [pltpu.SemaphoreType.DMA(shape)] * 2

    total_rows = 2 * dp_count * length
    return pl.pallas_call(
        functools.partial(step_kernel, sizes, 1.0 / math.sqrt(total_rows)),
        out_shape=(
            jax.ShapeDtypeStruct((tok_here, width), jnp.bfloat16),
            jax.ShapeDtypeStruct((3, down_rows, ADAPTER_RANK), jnp.float32),
            jax.ShapeDtypeStruct((3, up_rows, columns), jnp.float32),
        ),
        in_specs=[smem_spec] * 2 + [any_spec] * 6,
        out_specs=(any_spec, vmem_spec, vmem_spec),
        scratch_shapes=[
            bf16(3, 3, length, columns),
            bf16(tok_here, model_width),
            bf16(groups, tok_here, group_cols),
            bf16(groups, tok_here, group_cols),
            bf16(group_cols, groups * tok_here),
            bf16(3, model_width, ADAPTER_RANK),
            bf16(3, ADAPTER_RANK, columns),
            bf16(outer, inner, tok_here, rank_cols),
            bf16(heads_here, length, HDIM),
            bf16(heads_here, length, HDIM),
            f32(length, HDIM),
            bf16(length, HDIM),
            bf16(length, HDIM),
            bf16(length, HDIM),
            bf16(HDIM, length),
            bf16(HDIM, length),
            bf16(length, HDIM),
            f32(length, HDIM),
            f32(length, HDIM),
            f32(length, rank_cols),
            bf16(length, rank_cols),
            bf16(outer, inner, tok_here, rank_cols),
            bf16(outer, tok_here, rank_cols),
            bf16(outer, tok_here, rank_cols),
            bf16(length, columns),
            bf16(up_groups, 3, up_rows, columns),
            bf16(up_groups, 3, up_rows, columns),
            bf16(tok_here, rank_cols),
            bf16(groups, tok_here, rank_cols),
            bf16(outer, down_rows, rank_cols),
            bf16(outer, down_rows, rank_cols),
            *sems(2, heads_here, 3, count),
            *sems(heads_here, 3),
            *sems(2, outer),
            *sems(inner),
            *sems(heads_here),
            *sems(heads_here, count),
            *sems(groups),
            *sems(up_groups),
            *sems(3, outer, inner),
            *sems(3, outer),
            *sems(3, pairs),
            *sems(3, pairs, dp_count),
            *sems(3, outer),
            pltpu.SemaphoreType.DMA((7,)),
        ],
        compiler_params=pltpu.CompilerParams(
            collective_id=0, has_side_effects=True, vmem_limit_bytes=VMEM_LIMIT
        ),
        name="step",
    )(guide, time_index, *fields, hidden, down, up)


def emit_kernel(*refs):
    count = (len(refs) - 2) // 3
    held = refs[2 * count : 3 * count]
    load_sem, store_sem = refs[3 * count :]
    loads = [
        pltpu.make_async_copy(refs[item], held[item], load_sem.at[item]) for item in range(count)
    ]
    stores = [
        pltpu.make_async_copy(held[item], refs[count + item], store_sem.at[item])
        for item in range(count)
    ]
    for load in loads:
        load.start()
    for load, store in zip(loads, stores):
        load.wait()
        store.start()
    for store in stores:
        store.wait()


def emit(arrays):
    any_specs = (pl.BlockSpec(memory_space=pl.ANY),) * len(arrays)
    return pl.pallas_call(
        emit_kernel,
        out_shape=tuple(jax.ShapeDtypeStruct(array.shape, array.dtype) for array in arrays),
        in_specs=any_specs,
        out_specs=any_specs,
        scratch_shapes=[pltpu.VMEM(array.shape, array.dtype) for array in arrays]
        + [pltpu.SemaphoreType.DMA((len(arrays),))] * 2,
        compiler_params=pltpu.CompilerParams(vmem_limit_bytes=VMEM_LIMIT),
        name="emit",
    )(*arrays)


def body(
    teacher_query,
    teacher_key,
    teacher_value,
    hidden,
    adapter_down_weight,
    adapter_up_weight,
    guidance_index,
    timestep_index,
):
    seq_count = lax.axis_size("seq")
    outputs = run_step(
        (seq_count, inner_size(seq_count), lax.axis_size("dp")),
        guidance_index[:, 0],
        timestep_index[:, 0],
        (teacher_query[0, :, 0], teacher_key[0, :, 0], teacher_value[0, :, 0]),
        hidden[0, 0],
        adapter_down_weight,
        adapter_up_weight,
    )
    student_tokens, grad_down, grad_up = emit(outputs)
    return (student_tokens[None, None], grad_down, grad_up)


def solution(mesh):
    placed = (
        P("cfg", None, "dp", "seq", None),
        P("cfg", None, "dp", "seq", None),
        P("cfg", None, "dp", "seq", None),
        P("cfg", "dp", "seq", None),
        P(),
        P(),
        P(None, "dp"),
        P(None, "dp"),
    )
    return jax.shard_map(
        body,
        mesh=mesh,
        in_specs=placed,
        out_specs=(
            P("cfg", "dp", "seq", None),
            P(None, ("cfg", "seq", "dp"), None),
            P(None, ("cfg", "dp"), "seq"),
        ),
        check_vma=False,
    )
```

```python
import functools
import math

import jax
import jax.numpy as jnp
from jax import lax
from jax.experimental import pallas as pl
from jax.experimental.pallas import tpu as pltpu
from jax.sharding import PartitionSpec as P

HDIM = 128
ADAPTER_RANK = 128
TSTEPS = 1000
FACTOR = HDIM ** (-0.5)
FACTOR_BASE2 = FACTOR * math.log2(math.e)
VMEM_LIMIT = 60 * 1024 * 1024
BLOCK = 512
MESH = pl.DeviceIdType.MESH

NT = (((1,), (1,)), ((), ()))
TN = (((0,), (0,)), ((), ()))


def dot_f32(left, right):
    return jnp.dot(left, right, preferred_element_type=jnp.float32)


def dot_nt(left, right):
    return lax.dot_general(left, right, NT, preferred_element_type=jnp.float32)


def dot_tn(left, right):
    return lax.dot_general(left, right, TN, preferred_element_type=jnp.float32)


def inner_size(count, dp_count):
    return max(
        size
        for size in range(1, count + 1)
        if count % size == 0 and dp_count % size == 0 and size * size <= count
    )


def aligned(index, size):
    return pl.ds(pl.multiple_of(index * size, size), size)


def probs_by_key(key_head, query_block):
    scores = dot_nt(key_head, query_block)
    highest = jnp.max(scores, axis=0, keepdims=True)
    raised = jnp.exp2((scores - highest) * FACTOR_BASE2)
    return raised * (1.0 / jnp.sum(raised, axis=0, keepdims=True))


def step_kernel(
    sizes,
    out_scale,
    guide_ref,
    time_ref,
    query_ref,
    key_ref,
    value_ref,
    hidden_ref,
    down_ref,
    up_ref,
    tokens_ref,
    grad_down_ref,
    grad_up_ref,
    heads,
    hidden_own,
    hidden_cols,
    hidden_all,
    hidden_t,
    down_own,
    up_own,
    rank_line,
    ranks,
    facts,
    work_facts,
    weighted,
    weighted_in,
    target,
    s_query,
    s_key,
    s_value,
    key_t,
    value_t,
    grad_query,
    grad_key,
    grad_value,
    back_sum,
    back,
    near_in,
    far_out,
    far_in,
    student,
    up_parts,
    up_in,
    low,
    low_all,
    down_out,
    down_in,
    field_send,
    field_recv,
    pass_send,
    pass_recv,
    rank_send,
    rank_recv,
    fan_send,
    fan_recv,
    swap_send,
    swap_recv,
    out_send,
    out_recv,
    cols_send,
    cols_recv,
    up_send,
    up_recv,
    near_send,
    near_recv,
    far_send,
    far_recv,
    low_send,
    low_recv,
    share_send,
    share_recv,
    down_send,
    down_recv,
    facts_send,
    facts_recv,
    local_sem,
):
    count, inner, dp_count = sizes
    outer = count // inner
    pairs = 2 * inner
    groups = pairs * dp_count
    up_groups = 2 * dp_count
    fields = (query_ref, key_ref, value_ref)
    tok_here = query_ref.shape[1]
    length = tok_here * count
    columns = student.shape[1]
    heads_here = columns // HDIM
    step_rows = min(BLOCK, length)
    blocks = length // step_rows

    me = lax.axis_index("seq")
    cfg = lax.axis_index("cfg")
    dp = lax.axis_index("dp")
    other = 1 - cfg
    far = me // inner
    near = lax.rem(me, inner)
    part = lax.rem(dp, inner)
    bundle = dp // inner
    bundles = dp_count // inner
    diagonal = near == part
    off_diagonal = near != part
    pair = cfg * inner + near
    group = dp * pairs + pair
    work_block = far * inner + part
    own_rows = aligned(me, tok_here)
    grid_steps = [(far_step, near_step) for far_step in range(outer) for near_step in range(inner)]
    up_steps = [
        (cfg_step, bundle_step, near_step)
        for cfg_step in range(2)
        for bundle_step in range(bundles)
        for near_step in range(inner)
    ]
    order = (other, cfg)

    def head_columns(head):
        return slice(head * HDIM, (head + 1) * HDIM)

    def when_remote(steps, action):
        if any(steps):
            action()
        else:
            pl.when(off_diagonal)(action)

    def low_slot(pair_index, dp_index):
        return (
            dp_index // inner * inner + lax.rem(pair_index, inner)
        ) * pairs + pair_index // inner * inner + lax.rem(dp_index, inner)

    def device_of(pair_index):
        return {"cfg": pair_index // inner, "seq": far * inner + lax.rem(pair_index, inner)}

    def group_device(step):
        peer = lax.rem(group + step, groups)
        return {**device_of(lax.rem(peer, pairs)), "dp": peer // pairs}

    def remote(src, dst, send, recv, device):
        return pltpu.make_async_remote_copy(
            src_ref=src,
            dst_ref=dst,
            send_sem=send,
            recv_sem=recv,
            device_id=device,
            device_id_type=MESH,
        )

    loads = [
        pltpu.make_async_copy(hidden_ref, hidden_own, local_sem.at[0]),
        pltpu.make_async_copy(down_ref, down_own, local_sem.at[1]),
        pltpu.make_async_copy(
            up_ref.at[:, :, aligned(work_block, columns)], up_own, local_sem.at[2]
        ),
    ]
    own_loads = [
        pltpu.make_async_copy(
            fields[member].at[:, :, aligned(me, columns)],
            heads.at[member, 0:2, own_rows, :],
            local_sem.at[3 + member],
        )
        for member in range(3)
    ]
    for load in loads:
        load.start()

    @pl.when(diagonal)
    def _():
        for load in own_loads:
            load.start()

    barrier = pltpu.get_barrier_semaphore()
    for step in range(1, count * inner):
        peer_near = lax.rem(near + step // inner % inner, inner)
        peer_part = lax.rem(part + step % inner, inner)
        pl.semaphore_signal(
            barrier,
            inc=1,
            device_id={
                "seq": lax.rem(far + step // (inner * inner), outer) * inner + peer_near,
                "dp": bundle * inner + peer_part,
            },
            device_id_type=MESH,
        )
    for step in range(1, groups):
        pl.semaphore_signal(barrier, inc=1, device_id=group_device(step), device_id_type=MESH)

    def field_copy(phase, head, member, steps):
        peer_far = lax.rem(far + steps[0], outer)
        peer_part = lax.rem(near + steps[1], inner)
        half = order[phase]
        start = pl.multiple_of((peer_far * inner + peer_part) * columns, columns) + head * HDIM
        return remote(
            fields[member].at[half, :, pl.ds(start, HDIM)],
            heads.at[member, half, own_rows, head_columns(head)],
            field_send.at[phase, head, member, *steps],
            field_recv.at[phase, head, member, *steps],
            {"seq": peer_far * inner + part, "dp": bundle * inner + peer_part},
        )

    def each_field(phase, head, member, action):
        for steps in grid_steps:
            when_remote(steps, getattr(field_copy(phase, head, member, steps), action))

    def pass_copy(head, member):
        return remote(
            heads.at[member, 1, :, head_columns(head)],
            heads.at[member, 2, :, head_columns(head)],
            pass_send.at[head, member],
            pass_recv.at[head, member],
            {"cfg": other},
        )

    def rank_copy(way, hop):
        toward, back_by = (1, outer - hop) if way == 0 else (outer - 1, hop)
        block = rank_line.at[lax.rem(far + back_by, outer)]
        return remote(
            block,
            block,
            rank_send.at[way, hop],
            rank_recv.at[way, hop],
            {"seq": lax.rem(far + toward, outer) * inner + near},
        )

    def ranks_leave(way, hop):
        if way == 0:
            return jnp.logical_and(far >= hop, far < outer - 1)
        return jnp.logical_and(far < outer - hop, far > 0)

    def ranks_come(way, hop):
        return far > hop if way == 0 else far < outer - 1 - hop

    def rank_step(hop, action, test):
        for way in range(2):

            @pl.when(test(way, hop))
            def _():
                getattr(rank_copy(way, hop), action)()

    def fan_copy(step):
        peer_part = lax.rem(near + step, inner)
        return remote(
            rank_line,
            ranks.at[:, near],
            fan_send.at[step],
            fan_recv.at[step],
            {"seq": far * inner + part, "dp": bundle * inner + peer_part},
        )

    def facts_copy(step):
        return remote(
            facts,
            work_facts,
            facts_send.at[step],
            facts_recv.at[0],
            {"dp": bundle * inner + lax.rem(part + step, inner)},
        )

    def swap_copy(head):
        return remote(
            weighted.at[head],
            weighted_in.at[head],
            swap_send.at[head],
            swap_recv.at[head],
            {"cfg": other},
        )

    def out_copy(head, steps):
        peer = lax.rem(far + steps[0], outer) * inner + lax.rem(part + steps[1], inner)
        start = pl.multiple_of(work_block * columns, columns) + head * HDIM
        return remote(
            student.at[aligned(peer, tok_here), head_columns(head)],
            tokens_ref.at[:, pl.ds(start, HDIM)],
            out_send.at[head, *steps],
            out_recv.at[head, *steps],
            {"seq": peer, "dp": bundle * inner + near},
        )

    def each_out(head, action):
        for steps in grid_steps:
            when_remote(steps, getattr(out_copy(head, steps), action))

    def cols_copy(step):
        return remote(
            hidden_cols.at[lax.rem(group + step, groups)],
            hidden_all.at[group],
            cols_send.at[step],
            cols_recv.at[step],
            group_device(step),
        )

    def up_copy(steps):
        peer_cfg = lax.rem(cfg + steps[0], 2)
        peer_dp = lax.rem(bundle + steps[1], bundles) * inner + lax.rem(near + steps[2], inner)
        return remote(
            up_parts.at[peer_cfg * dp_count + peer_dp],
            up_in.at[steps],
            up_send.at[steps],
            up_recv.at[steps],
            {"cfg": peer_cfg, "seq": work_block, "dp": peer_dp},
        )

    def each_up(action):
        for steps in up_steps:
            when_remote(steps, getattr(up_copy(steps), action))

    def near_copy(member, far_step, step):
        peer = lax.rem(part + step, inner)
        row = lax.rem(far + far_step, outer)
        return remote(
            back.at[aligned(row * inner + peer, tok_here), head_columns(member)],
            near_in.at[far_step, step, :, head_columns(member)],
            near_send.at[member, far_step, step],
            near_recv.at[member, far_step, step],
            {"dp": bundle * inner + peer},
        )

    def far_copy(member, step):
        return remote(
            far_out.at[step, :, head_columns(member)],
            far_in.at[step, :, head_columns(member)],
            far_send.at[member, step],
            far_recv.at[member, step],
            {"seq": lax.rem(far + step, outer) * inner + near},
        )

    def low_copy(member, step):
        return remote(
            low.at[:, head_columns(member)],
            low_all.at[low_slot(pair, dp), :, head_columns(member)],
            low_send.at[member, step],
            low_recv.at[member, step],
            device_of(lax.rem(pair + step, pairs)),
        )

    def share_copy(member, pair_step, step):
        source = lax.rem(pair - pair_step + pairs, pairs)
        lanes = head_columns(member)
        slot = low_all.at[low_slot(source, dp), :, lanes]
        return remote(
            low.at[:, lanes] if pair_step == 0 else slot,
            slot,
            share_send.at[member, pair_step, step],
            share_recv.at[member, pair_step, step],
            {"dp": lax.rem(dp + step, dp_count)},
        )

    def down_copy(member, step):
        peer = lax.rem(far + step, outer)
        return remote(
            down_out.at[peer, :, head_columns(member)],
            down_in.at[step, :, head_columns(member)],
            down_send.at[member, step],
            down_recv.at[member, step],
            {"seq": peer * inner + near},
        )

    def guide_scale(half):
        return 1.0 + 0.5 * guide_ref[half].astype(jnp.float32)

    rank_index = (lax.broadcasted_iota(jnp.int32, (1, ADAPTER_RANK), 1) + 1).astype(jnp.float32)
    time_frac = (time_ref[cfg].astype(jnp.float32) + 0.5) / TSTEPS
    modulation = 1.0 + 0.5 * jnp.cos(
        math.pi * rank_index * time_frac + 0.25 * rank_index * guide_scale(cfg)
    )

    facts[0] = modulation
    for half in range(2):
        facts[1 + half] = jnp.full((1, ADAPTER_RANK), guide_scale(half), jnp.float32)

    def weighting(half):
        scale = work_facts[1 + half]
        return jnp.where(cfg == 0, scale, 1.0 - scale)

    phases = [(phase, head) for phase in range(2) for head in range(heads_here)]
    sends = [(phase, head, member) for phase, head in phases for member in (1, 2, 0)]
    pl.semaphore_wait(barrier, count * inner + groups - 2)
    each_field(*sends[0], "start")

    @pl.when(diagonal)
    def _():
        work_facts[...] = facts[...]
        for step in range(1, inner):
            facts_copy(step).start()

    loads[0].wait()
    loads[1].wait()
    for member in range(3):
        projected = dot_f32(hidden_own[...], down_own[member]) * modulation
        rank_line[far, :, head_columns(member)] = projected.astype(jnp.bfloat16)
    for hop in range(outer - 1):
        rank_step(hop, "start", ranks_leave)
        each_field(*sends[1 + hop], "start")
        rank_step(hop, "wait_recv", ranks_come)
    for step in range(inner):
        when_remote((step,), fan_copy(step).start)
    for turn in sends[outer:]:
        each_field(*turn, "start")

    @pl.when(diagonal)
    def _():
        ranks[:, near] = rank_line[...]

    @pl.when(off_diagonal)
    def _():
        facts_copy(inner - 1).wait_recv()

    rows_here = hidden_cols.shape[2] // outer
    for block in range(outer * groups):
        target_dp = block % dp_count
        target_near = block // dp_count % inner
        target_far = block // dp_count // inner % outer
        target_pair = block // (dp_count * count) * inner + target_near
        hidden_cols[
            target_dp * pairs + target_pair, :, target_far * rows_here : (target_far + 1) * rows_here
        ] = hidden_own[:, block * rows_here : (block + 1) * rows_here]
    hidden_all[group] = hidden_cols[group]
    for step in range(1, groups):
        cols_copy(step).start()
    loads[2].wait()

    @pl.when(diagonal)
    def _():
        for load in own_loads:
            load.wait()

    far_order = sorted(range(outer), key=lambda step: (step == 0, abs(2 * step - outer)))

    def run_blocks(one_block):
        unroll = 2 if blocks % 2 == 0 else 1

        def some(step, _):
            for offset in range(unroll):
                one_block(step * unroll + offset)
            return 0

        lax.fori_loop(0, blocks // unroll, some, 0)

    def teacher(half, head, store):
        lanes = head_columns(head)
        value_t[...] = heads[2, half, :, lanes].T

        def one_block(step):
            rows = aligned(step, step_rows)
            weights = probs_by_key(heads[1, half, :, lanes], heads[0, half, rows, lanes])
            attended = dot_f32(value_t[...], weights.astype(jnp.bfloat16)).T
            store(rows, attended.astype(jnp.bfloat16).astype(jnp.float32))

        run_blocks(one_block)

    for head in range(heads_here):
        for member in (1, 2, 0):
            each_field(0, head, member, "wait_recv")
            pl.when(cfg == 0)(pass_copy(head, member).start)

        def store_other(rows, attended):
            weighted[head, rows, :] = (weighting(other) * attended).astype(jnp.bfloat16)

        teacher(other, head, store_other)
        swap_copy(head).start()

    for step in range(inner):
        when_remote((step,), fan_copy(step).wait_recv)

    for head in range(heads_here):
        lanes = head_columns(head)
        for member in (1, 2, 0):
            each_field(1, head, member, "wait_recv")

        def store_own(rows, attended):
            target[rows, :] = weighting(cfg) * attended

        teacher(cfg, head, store_own)

        @pl.when(cfg == 1)
        def _():
            for member in range(3):
                pass_copy(head, member).wait_recv()

        for member, projected in enumerate((s_query, s_key, s_value)):
            low_rank = ranks[:, :, :, head_columns(member)].reshape(length, ADAPTER_RANK)
            frozen = heads[member, 2 * cfg, :, lanes].astype(jnp.float32)
            projected[...] = (frozen + dot_f32(low_rank, up_own[member, :, lanes])).astype(
                jnp.bfloat16
            )
        key_t[...] = s_key[...].T
        value_t[...] = s_value[...].T
        grad_key[...] = jnp.zeros_like(grad_key)
        grad_value[...] = jnp.zeros_like(grad_value)
        swap_copy(head).wait_recv()

        def one_block(step):
            rows = aligned(step, step_rows)
            query_block = s_query[rows, :]
            probability = probs_by_key(s_key[...], query_block)
            weights = probability.astype(jnp.bfloat16)
            attended = dot_f32(value_t[...], weights).T.astype(jnp.bfloat16)
            student[rows, lanes] = attended
            aim = target[rows, :] + weighted_in[head, rows, :].astype(jnp.float32)
            upstream = ((attended.astype(jnp.float32) - aim) * out_scale).astype(jnp.bfloat16)
            grad_value[...] += dot_f32(weights, upstream)
            prob_grad = dot_nt(s_value[...], upstream)
            center = jnp.sum(probability * prob_grad, axis=0, keepdims=True)
            score_grad = (probability * (prob_grad - center)).astype(jnp.bfloat16)
            grad_key[...] += dot_f32(score_grad, query_block)
            grad_query[rows, :] = (dot_f32(key_t[...], score_grad).T * FACTOR).astype(
                jnp.bfloat16
            )

        run_blocks(one_block)
        if head < heads_here - 1:
            each_out(head, "start")

        gradients = (
            grad_query[...],
            (grad_key[...] * FACTOR).astype(jnp.bfloat16),
            grad_value[...].astype(jnp.bfloat16),
        )
        for member, gradient in enumerate(gradients):
            piece = dot_nt(gradient, up_own[member, :, lanes])
            if head > 0:
                piece = piece + back_sum[:, head_columns(member)]
            if head < heads_here - 1:
                back_sum[:, head_columns(member)] = piece
            else:
                back[:, head_columns(member)] = piece.astype(jnp.bfloat16)
                for far_step in far_order:
                    for step in range(1, inner):
                        near_copy(member, far_step, step).start()
        if head == heads_here - 1:
            each_out(head, "start")
        for member, gradient in enumerate(gradients):
            low_rank = ranks[:, :, :, head_columns(member)].reshape(length, ADAPTER_RANK)
            piece = dot_tn(low_rank, gradient).astype(jnp.bfloat16)
            up_parts[:, member, :, lanes] = piece.reshape(up_groups, -1, HDIM)

    each_up("start")
    own_store = pltpu.make_async_copy(
        student.at[own_rows, :], tokens_ref.at[:, aligned(me, columns)], local_sem.at[6]
    )

    @pl.when(diagonal)
    def _():
        own_store.start()
        up_in[0, 0, 0] = up_parts[cfg * dp_count + dp]

    for step in range(1, groups):
        cols_copy(step).wait_recv()
    gathered_cols = hidden_all[...].reshape(groups * tok_here, -1)
    hidden_t[...] = gathered_cols.T
    down_rows = gathered_cols.shape[1] // outer

    def reduce_near(member):
        lanes = head_columns(member)
        for far_step in far_order:
            row = lax.rem(far + far_step, outer)
            total = back[aligned(row * inner + part, tok_here), lanes].astype(jnp.float32)
            for step in range(1, inner):
                near_copy(member, far_step, step).wait_recv()
                total = total + near_in[far_step, step, :, lanes].astype(jnp.float32)
            if far_step > 0:
                far_out[far_step, :, lanes] = total.astype(jnp.bfloat16)
                far_copy(member, far_step).start()
        return total

    def reduce_far(member, total):
        lanes = head_columns(member)
        for step in range(1, outer):
            far_copy(member, step).wait_recv()
            total = total + far_in[step, :, lanes].astype(jnp.float32)
        low_grad = (total * work_facts[0]).astype(jnp.bfloat16)
        low[:, lanes] = low_grad
        low_all[low_slot(pair, dp), :, lanes] = low_grad
        for step in range(1, pairs):
            low_copy(member, step).start()
        for step in range(1, dp_count):
            share_copy(member, 0, step).start()

    def spread(member):
        for pair_step in range(1, pairs):
            low_copy(member, pair_step).wait_recv()
            for step in range(1, dp_count):
                share_copy(member, pair_step, step).start()

    def contract(member):
        lanes = head_columns(member)
        for pair_step in range(pairs):
            for step in range(1, dp_count):
                share_copy(member, pair_step, step).wait_recv()
        gathered_low = low_all[:, :, lanes].reshape(groups * tok_here, ADAPTER_RANK)
        partial = dot_f32(hidden_t[...], gathered_low).astype(jnp.bfloat16)
        for peer in range(outer):
            down_out[peer, :, lanes] = partial[peer * down_rows : (peer + 1) * down_rows, :]
        for step in range(1, outer):
            down_copy(member, step).start()

    totals = {}
    for turn in range(6):
        if turn < 3:
            totals[turn] = reduce_near(turn)
        if 1 <= turn < 4:
            reduce_far(turn - 1, totals[turn - 1])
        if 2 <= turn < 5:
            spread(turn - 2)
        if turn >= 3:
            contract(turn - 3)

    each_up("wait_recv")
    up_total = up_in[up_steps[0]].astype(jnp.float32)
    for steps in up_steps[1:]:
        up_total = up_total + up_in[steps].astype(jnp.float32)
    grad_up_ref[...] = up_total

    for member in range(3):
        lanes = head_columns(member)
        down_total = down_out[far, :, lanes].astype(jnp.float32)
        for step in range(1, outer):
            down_copy(member, step).wait_recv()
            down_total = down_total + down_in[step, :, lanes].astype(jnp.float32)
        grad_down_ref[member] = down_total

    @pl.when(diagonal)
    def _():
        own_store.wait()
        for step in range(1, inner):
            facts_copy(step).wait_send()

    for turn in sends:
        each_field(*turn, "wait_send")
    for head in range(heads_here):
        swap_copy(head).wait_send()

        @pl.when(cfg == 0)
        def _():
            for member in range(3):
                pass_copy(head, member).wait_send()

        each_out(head, "wait")
    for hop in range(outer - 1):
        rank_step(hop, "wait_send", ranks_leave)
    for step in range(inner):
        when_remote((step,), fan_copy(step).wait_send)
    for step in range(1, groups):
        cols_copy(step).wait_send()
    each_up("wait_send")
    for member in range(3):
        for pair_step in range(pairs):
            if pair_step > 0:
                low_copy(member, pair_step).wait_send()
            for step in range(1, dp_count):
                share_copy(member, pair_step, step).wait_send()
        for far_step in range(outer):
            if far_step > 0:
                far_copy(member, far_step).wait_send()
                down_copy(member, far_step).wait_send()
            for step in range(1, inner):
                near_copy(member, far_step, step).wait_send()


def run_step(sizes, guide, time_index, fields, hidden, down, up):
    count, inner, dp_count = sizes
    outer = count // inner
    pairs = 2 * inner
    groups = pairs * dp_count
    up_groups = 2 * dp_count
    tok_here, width = fields[0].shape[1:]
    model_width = hidden.shape[1]
    length, columns = tok_here * count, width // count
    heads_here = columns // HDIM
    rank_cols = 3 * ADAPTER_RANK
    group_cols = model_width // groups
    down_rows = group_cols // outer
    up_rows = ADAPTER_RANK // up_groups
    any_spec = pl.BlockSpec(memory_space=pl.ANY)
    vmem_spec = pl.BlockSpec(memory_space=pltpu.VMEM)
    smem_spec = pl.BlockSpec(memory_space=pltpu.SMEM)

    def bf16(*shape):
        return pltpu.VMEM(shape, jnp.bfloat16)

    def f32(*shape):
        return pltpu.VMEM(shape, jnp.float32)

    def sems(*shape):
        return [pltpu.SemaphoreType.DMA(shape)] * 2

    total_rows = 2 * dp_count * length
    return pl.pallas_call(
        functools.partial(step_kernel, sizes, 1.0 / math.sqrt(total_rows)),
        out_shape=(
            jax.ShapeDtypeStruct((tok_here, width), jnp.bfloat16),
            jax.ShapeDtypeStruct((3, down_rows, ADAPTER_RANK), jnp.float32),
            jax.ShapeDtypeStruct((3, up_rows, columns), jnp.float32),
        ),
        in_specs=[smem_spec] * 2 + [any_spec] * 6,
        out_specs=(any_spec, vmem_spec, vmem_spec),
        scratch_shapes=[
            bf16(3, 3, length, columns),
            bf16(tok_here, model_width),
            bf16(groups, tok_here, group_cols),
            bf16(groups, tok_here, group_cols),
            bf16(group_cols, groups * tok_here),
            bf16(3, model_width, ADAPTER_RANK),
            bf16(3, ADAPTER_RANK, columns),
            bf16(outer, tok_here, rank_cols),
            bf16(outer, inner, tok_here, rank_cols),
            f32(3, 1, ADAPTER_RANK),
            f32(3, 1, ADAPTER_RANK),
            bf16(heads_here, length, HDIM),
            bf16(heads_here, length, HDIM),
            f32(length, HDIM),
            bf16(length, HDIM),
            bf16(length, HDIM),
            bf16(length, HDIM),
            bf16(HDIM, length),
            bf16(HDIM, length),
            bf16(length, HDIM),
            f32(length, HDIM),
            f32(length, HDIM),
            f32(length, rank_cols),
            bf16(length, rank_cols),
            bf16(outer, inner, tok_here, rank_cols),
            bf16(outer, tok_here, rank_cols),
            bf16(outer, tok_here, rank_cols),
            bf16(length, columns),
            bf16(up_groups, 3, up_rows, columns),
            bf16(2, dp_count // inner, inner, 3, up_rows, columns),
            bf16(tok_here, rank_cols),
            bf16(groups, tok_here, rank_cols),
            bf16(outer, down_rows, rank_cols),
            bf16(outer, down_rows, rank_cols),
            *sems(2, heads_here, 3, outer, inner),
            *sems(heads_here, 3),
            *sems(2, outer),
            *sems(inner),
            *sems(heads_here),
            *sems(heads_here, outer, inner),
            *sems(groups),
            *sems(2, dp_count // inner, inner),
            *sems(3, outer, inner),
            *sems(3, outer),
            *sems(3, pairs),
            *sems(3, pairs, dp_count),
            *sems(3, outer),
            *sems(inner),
            pltpu.SemaphoreType.DMA((7,)),
        ],
        compiler_params=pltpu.CompilerParams(
            collective_id=0, has_side_effects=True, vmem_limit_bytes=VMEM_LIMIT
        ),
        name="step",
    )(guide, time_index, *fields, hidden, down, up)


def emit_kernel(*refs):
    count = (len(refs) - 2) // 3
    held = refs[2 * count : 3 * count]
    load_sem, store_sem = refs[3 * count :]
    loads = [
        pltpu.make_async_copy(refs[item], held[item], load_sem.at[item]) for item in range(count)
    ]
    stores = [
        pltpu.make_async_copy(held[item], refs[count + item], store_sem.at[item])
        for item in range(count)
    ]
    for load in loads:
        load.start()
    for load, store in zip(loads, stores):
        load.wait()
        store.start()
    for store in stores:
        store.wait()


def emit(arrays):
    any_specs = (pl.BlockSpec(memory_space=pl.ANY),) * len(arrays)
    return pl.pallas_call(
        emit_kernel,
        out_shape=tuple(jax.ShapeDtypeStruct(array.shape, array.dtype) for array in arrays),
        in_specs=any_specs,
        out_specs=any_specs,
        scratch_shapes=[pltpu.VMEM(array.shape, array.dtype) for array in arrays]
        + [pltpu.SemaphoreType.DMA((len(arrays),))] * 2,
        compiler_params=pltpu.CompilerParams(vmem_limit_bytes=VMEM_LIMIT),
        name="emit",
    )(*arrays)


def body(
    teacher_query,
    teacher_key,
    teacher_value,
    hidden,
    adapter_down_weight,
    adapter_up_weight,
    guidance_index,
    timestep_index,
):
    seq_count = lax.axis_size("seq")
    dp_count = lax.axis_size("dp")
    outputs = run_step(
        (seq_count, inner_size(seq_count, dp_count), dp_count),
        guidance_index[:, 0],
        timestep_index[:, 0],
        (teacher_query[0, :, 0], teacher_key[0, :, 0], teacher_value[0, :, 0]),
        hidden[0, 0],
        adapter_down_weight,
        adapter_up_weight,
    )
    student_tokens, grad_down, grad_up = emit(outputs)
    return (student_tokens[None, None], grad_down, grad_up)


def solution(mesh):
    placed = (
        P("cfg", None, "dp", "seq", None),
        P("cfg", None, "dp", "seq", None),
        P("cfg", None, "dp", "seq", None),
        P("cfg", "dp", "seq", None),
        P(),
        P(),
        P(None, "dp"),
        P(None, "dp"),
    )
    return jax.shard_map(
        body,
        mesh=mesh,
        in_specs=placed,
        out_specs=(
            P("cfg", "dp", "seq", None),
            P(None, ("cfg", "seq", "dp"), None),
            P(None, ("cfg", "dp"), "seq"),
        ),
        check_vma=False,
    )
```

```python
import functools
import math

import jax
import jax.numpy as jnp
from jax import lax
from jax.experimental import pallas as pl
from jax.experimental.pallas import tpu as pltpu
from jax.sharding import PartitionSpec as P

HDIM = 128
ADAPTER_RANK = 128
TSTEPS = 1000
FACTOR = HDIM ** (-0.5)
FACTOR_BASE2 = FACTOR * math.log2(math.e)
VMEM_LIMIT = 63 * 1024 * 1024
BLOCK = 512
BLOCK_AREA = BLOCK * 1024
KEPT_BYTES = 16 * 1024 * 1024
MESH = pl.DeviceIdType.MESH

NT = (((1,), (1,)), ((), ()))
TN = (((0,), (0,)), ((), ()))


def dot_f32(left, right):
    return jnp.dot(left, right, preferred_element_type=jnp.float32)


def dot_nt(left, right):
    return lax.dot_general(left, right, NT, preferred_element_type=jnp.float32)


def dot_tn(left, right):
    return lax.dot_general(left, right, TN, preferred_element_type=jnp.float32)


def inner_size(count, dp_count):
    return max(
        size
        for size in range(1, count + 1)
        if count % size == 0 and dp_count % size == 0 and size * size <= count
    )


def aligned(index, size):
    return pl.ds(pl.multiple_of(index * size, size), size)


def probs_by_key(key_head, query_block):
    scores = dot_nt(key_head, query_block)
    highest = jnp.max(scores, axis=0, keepdims=True)
    raised = jnp.exp2((scores - highest) * FACTOR_BASE2)
    return raised * (1.0 / jnp.sum(raised, axis=0, keepdims=True))


def step_kernel(
    sizes,
    out_scale,
    guide_ref,
    time_ref,
    query_ref,
    key_ref,
    value_ref,
    hidden_ref,
    down_ref,
    up_ref,
    tokens_ref,
    grad_down_ref,
    grad_up_ref,
    heads,
    hidden_own,
    hidden_cols,
    hidden_all,
    hidden_t,
    down_own,
    up_own,
    rank_line,
    ranks,
    facts,
    work_facts,
    weighted,
    weighted_in,
    target,
    s_query,
    s_key,
    s_value,
    key_t,
    value_t,
    grad_query,
    grad_key,
    grad_value,
    teacher_w,
    student_w,
    student_p,
    back_sum,
    back,
    near_in,
    far_out,
    far_in,
    student,
    up_parts,
    up_in,
    low,
    low_all,
    down_out,
    down_in,
    field_send,
    field_recv,
    pass_send,
    pass_recv,
    rank_send,
    rank_recv,
    fan_send,
    fan_recv,
    swap_send,
    swap_recv,
    out_send,
    out_recv,
    cols_send,
    cols_recv,
    up_send,
    up_recv,
    near_send,
    near_recv,
    far_send,
    far_recv,
    low_send,
    low_recv,
    share_send,
    share_recv,
    down_send,
    down_recv,
    facts_send,
    facts_recv,
    local_sem,
):
    count, inner, dp_count = sizes
    outer = count // inner
    pairs = 2 * inner
    groups = pairs * dp_count
    up_groups = 2 * dp_count
    fields = (query_ref, key_ref, value_ref)
    tok_here = query_ref.shape[1]
    length = tok_here * count
    columns = student.shape[1]
    heads_here = columns // HDIM
    step_rows = min(BLOCK, BLOCK_AREA // length, length)
    blocks = length // step_rows

    me = lax.axis_index("seq")
    cfg = lax.axis_index("cfg")
    dp = lax.axis_index("dp")
    other = 1 - cfg
    far = me // inner
    near = lax.rem(me, inner)
    part = lax.rem(dp, inner)
    bundle = dp // inner
    bundles = dp_count // inner
    diagonal = near == part
    off_diagonal = near != part
    pair = cfg * inner + near
    group = dp * pairs + pair
    work_block = far * inner + part
    own_rows = aligned(me, tok_here)
    grid_steps = [(far_step, near_step) for far_step in range(outer) for near_step in range(inner)]
    up_steps = [
        (cfg_step, bundle_step, near_step)
        for cfg_step in range(2)
        for bundle_step in range(bundles)
        for near_step in range(inner)
    ]
    order = (other, cfg)

    def head_columns(head):
        return slice(head * HDIM, (head + 1) * HDIM)

    def when_remote(steps, action):
        if any(steps):
            action()
        else:
            pl.when(off_diagonal)(action)

    def low_slot(pair_index, dp_index):
        return (
            dp_index // inner * inner + lax.rem(pair_index, inner)
        ) * pairs + pair_index // inner * inner + lax.rem(dp_index, inner)

    def device_of(pair_index):
        return {"cfg": pair_index // inner, "seq": far * inner + lax.rem(pair_index, inner)}

    def group_device(step):
        peer = lax.rem(group + step, groups)
        return {**device_of(lax.rem(peer, pairs)), "dp": peer // pairs}

    def remote(src, dst, send, recv, device):
        return pltpu.make_async_remote_copy(
            src_ref=src,
            dst_ref=dst,
            send_sem=send,
            recv_sem=recv,
            device_id=device,
            device_id_type=MESH,
        )

    loads = [
        pltpu.make_async_copy(hidden_ref, hidden_own, local_sem.at[0]),
        pltpu.make_async_copy(down_ref, down_own, local_sem.at[1]),
        pltpu.make_async_copy(
            up_ref.at[:, :, aligned(work_block, columns)], up_own, local_sem.at[2]
        ),
    ]
    own_loads = [
        pltpu.make_async_copy(
            fields[member].at[:, :, aligned(me, columns)],
            heads.at[member, 0:2, own_rows, :],
            local_sem.at[3 + member],
        )
        for member in range(3)
    ]
    for load in loads:
        load.start()

    @pl.when(diagonal)
    def _():
        for load in own_loads:
            load.start()

    barrier = pltpu.get_barrier_semaphore()
    for step in range(1, count * inner):
        peer_near = lax.rem(near + step // inner % inner, inner)
        peer_part = lax.rem(part + step % inner, inner)
        pl.semaphore_signal(
            barrier,
            inc=1,
            device_id={
                "seq": lax.rem(far + step // (inner * inner), outer) * inner + peer_near,
                "dp": bundle * inner + peer_part,
            },
            device_id_type=MESH,
        )
    for step in range(1, groups):
        pl.semaphore_signal(barrier, inc=1, device_id=group_device(step), device_id_type=MESH)

    def field_copy(phase, head, member, steps):
        peer_far = lax.rem(far + steps[0], outer)
        peer_part = lax.rem(near + steps[1], inner)
        half = order[phase]
        start = pl.multiple_of((peer_far * inner + peer_part) * columns, columns) + head * HDIM
        return remote(
            fields[member].at[half, :, pl.ds(start, HDIM)],
            heads.at[member, half, own_rows, head_columns(head)],
            field_send.at[phase, head, member, *steps],
            field_recv.at[phase, head, member, *steps],
            {"seq": peer_far * inner + part, "dp": bundle * inner + peer_part},
        )

    def each_field(phase, head, member, action):
        for steps in grid_steps:
            when_remote(steps, getattr(field_copy(phase, head, member, steps), action))

    def pass_copy(head, member):
        return remote(
            heads.at[member, 1, :, head_columns(head)],
            heads.at[member, 2, :, head_columns(head)],
            pass_send.at[head, member],
            pass_recv.at[head, member],
            {"cfg": other},
        )

    def rank_copy(way, hop):
        toward, back_by = (1, outer - hop) if way == 0 else (outer - 1, hop)
        block = rank_line.at[lax.rem(far + back_by, outer)]
        return remote(
            block,
            block,
            rank_send.at[way, hop],
            rank_recv.at[way, hop],
            {"seq": lax.rem(far + toward, outer) * inner + near},
        )

    def ranks_leave(way, hop):
        if way == 0:
            return jnp.logical_and(far >= hop, far < outer - 1)
        return jnp.logical_and(far < outer - hop, far > 0)

    def ranks_come(way, hop):
        return far > hop if way == 0 else far < outer - 1 - hop

    def rank_step(hop, action, test):
        for way in range(2):

            @pl.when(test(way, hop))
            def _():
                getattr(rank_copy(way, hop), action)()

    def fan_copy(step):
        peer_part = lax.rem(near + step, inner)
        return remote(
            rank_line,
            ranks.at[:, near],
            fan_send.at[step],
            fan_recv.at[step],
            {"seq": far * inner + part, "dp": bundle * inner + peer_part},
        )

    def facts_copy(step):
        return remote(
            facts,
            work_facts,
            facts_send.at[step],
            facts_recv.at[0],
            {"dp": bundle * inner + lax.rem(part + step, inner)},
        )

    def swap_copy(head):
        return remote(
            weighted.at[head],
            weighted_in.at[head],
            swap_send.at[head],
            swap_recv.at[head],
            {"cfg": other},
        )

    def out_copy(head, steps):
        peer = lax.rem(far + steps[0], outer) * inner + lax.rem(part + steps[1], inner)
        start = pl.multiple_of(work_block * columns, columns) + head * HDIM
        return remote(
            student.at[aligned(peer, tok_here), head_columns(head)],
            tokens_ref.at[:, pl.ds(start, HDIM)],
            out_send.at[head, *steps],
            out_recv.at[head, *steps],
            {"seq": peer, "dp": bundle * inner + near},
        )

    def each_out(head, action):
        for steps in grid_steps:
            when_remote(steps, getattr(out_copy(head, steps), action))

    def cols_copy(step):
        return remote(
            hidden_cols.at[lax.rem(group + step, groups)],
            hidden_all.at[group],
            cols_send.at[step],
            cols_recv.at[step],
            group_device(step),
        )

    def up_copy(steps):
        peer_cfg = lax.rem(cfg + steps[0], 2)
        peer_dp = lax.rem(bundle + steps[1], bundles) * inner + lax.rem(near + steps[2], inner)
        return remote(
            up_parts.at[peer_cfg * dp_count + peer_dp],
            up_in.at[steps],
            up_send.at[steps],
            up_recv.at[steps],
            {"cfg": peer_cfg, "seq": work_block, "dp": peer_dp},
        )

    def each_up(action):
        for steps in up_steps:
            when_remote(steps, getattr(up_copy(steps), action))

    def near_copy(member, far_step, step):
        peer = lax.rem(part + step, inner)
        row = lax.rem(far + far_step, outer)
        return remote(
            back.at[aligned(row * inner + peer, tok_here), head_columns(member)],
            near_in.at[far_step, step, :, head_columns(member)],
            near_send.at[member, far_step, step],
            near_recv.at[member, far_step, step],
            {"dp": bundle * inner + peer},
        )

    def far_copy(member, step):
        return remote(
            far_out.at[step, :, head_columns(member)],
            far_in.at[step, :, head_columns(member)],
            far_send.at[member, step],
            far_recv.at[member, step],
            {"seq": lax.rem(far + step, outer) * inner + near},
        )

    def low_copy(member, step):
        return remote(
            low.at[:, head_columns(member)],
            low_all.at[low_slot(pair, dp), :, head_columns(member)],
            low_send.at[member, step],
            low_recv.at[member, step],
            device_of(lax.rem(pair + step, pairs)),
        )

    def share_copy(member, pair_step, step):
        source = lax.rem(pair - pair_step + pairs, pairs)
        lanes = head_columns(member)
        slot = low_all.at[low_slot(source, dp), :, lanes]
        return remote(
            low.at[:, lanes] if pair_step == 0 else slot,
            slot,
            share_send.at[member, pair_step, step],
            share_recv.at[member, pair_step, step],
            {"dp": lax.rem(dp + step, dp_count)},
        )

    def down_copy(member, step):
        peer = lax.rem(far + step, outer)
        return remote(
            down_out.at[peer, :, head_columns(member)],
            down_in.at[step, :, head_columns(member)],
            down_send.at[member, step],
            down_recv.at[member, step],
            {"seq": peer * inner + near},
        )

    def guide_scale(half):
        return 1.0 + 0.5 * guide_ref[half].astype(jnp.float32)

    rank_index = (lax.broadcasted_iota(jnp.int32, (1, ADAPTER_RANK), 1) + 1).astype(jnp.float32)
    time_frac = (time_ref[cfg].astype(jnp.float32) + 0.5) / TSTEPS
    modulation = 1.0 + 0.5 * jnp.cos(
        math.pi * rank_index * time_frac + 0.25 * rank_index * guide_scale(cfg)
    )

    facts[0] = modulation
    for half in range(2):
        facts[1 + half] = jnp.full((1, ADAPTER_RANK), guide_scale(half), jnp.float32)

    def weighting(half):
        scale = work_facts[1 + half]
        return jnp.where(cfg == 0, scale, 1.0 - scale)

    phases = [(phase, head) for phase in range(2) for head in range(heads_here)]
    sends = [(phase, head, member) for phase, head in phases for member in (1, 0, 2)]
    pl.semaphore_wait(barrier, count * inner + groups - 2)
    each_field(*sends[0], "start")

    @pl.when(diagonal)
    def _():
        work_facts[...] = facts[...]
        for step in range(1, inner):
            facts_copy(step).start()

    loads[0].wait()
    loads[1].wait()
    for member in range(3):
        projected = dot_f32(hidden_own[...], down_own[member]) * modulation
        rank_line[far, :, head_columns(member)] = projected.astype(jnp.bfloat16)
    for hop in range(outer - 1):
        rank_step(hop, "start", ranks_leave)
        each_field(*sends[1 + hop], "start")
        rank_step(hop, "wait_recv", ranks_come)
    for step in range(inner):
        when_remote((step,), fan_copy(step).start)
    for turn in sends[outer:]:
        each_field(*turn, "start")

    @pl.when(diagonal)
    def _():
        ranks[:, near] = rank_line[...]

    @pl.when(off_diagonal)
    def _():
        facts_copy(inner - 1).wait_recv()

    rows_here = hidden_cols.shape[2] // outer
    for block in range(outer * groups):
        target_dp = block % dp_count
        target_near = block // dp_count % inner
        target_far = block // dp_count // inner % outer
        target_pair = block // (dp_count * count) * inner + target_near
        hidden_cols[
            target_dp * pairs + target_pair, :, target_far * rows_here : (target_far + 1) * rows_here
        ] = hidden_own[:, block * rows_here : (block + 1) * rows_here]
    hidden_all[group] = hidden_cols[group]
    for step in range(1, groups):
        cols_copy(step).start()
    loads[2].wait()

    @pl.when(diagonal)
    def _():
        for load in own_loads:
            load.wait()

    far_order = sorted(range(outer), key=lambda step: (step == 0, abs(2 * step - outer)))

    def run_blocks(one_block):
        unroll = 2 if blocks % 2 == 0 else 1

        def some(step, _):
            for offset in range(unroll):
                one_block(step * unroll + offset)
            return 0

        lax.fori_loop(0, blocks // unroll, some, 0)

    def block_rows(step):
        return aligned(step, step_rows)

    def teacher_weights(half, lanes):
        def one_block(step):
            probability = probs_by_key(
                heads[1, half, :, lanes], heads[0, half, block_rows(step), lanes]
            )
            teacher_w[step] = probability.astype(jnp.bfloat16)

        run_blocks(one_block)

    def student_weights(step):
        if student_w is None:
            return student_p[step].astype(jnp.bfloat16)
        return student_w[step]

    def arrived(phase, head, member):
        each_field(phase, head, member, "wait_recv")
        if phase == 0:
            pl.when(cfg == 0)(pass_copy(head, member).start)

    def project(head, member, projected):
        lanes = head_columns(head)
        pl.when(cfg == 1)(pass_copy(head, member).wait_recv)
        low_rank = ranks[:, :, :, head_columns(member)].reshape(length, ADAPTER_RANK)
        frozen = heads[member, 2 * cfg, :, lanes].astype(jnp.float32)
        projected[...] = (frozen + dot_f32(low_rank, up_own[member, :, lanes])).astype(
            jnp.bfloat16
        )

    for head in range(heads_here):
        lanes = head_columns(head)
        arrived(0, head, 1)
        arrived(0, head, 0)
        teacher_weights(other, lanes)
        arrived(0, head, 2)
        value_t[...] = heads[2, other, :, lanes].T

        def one_block(step):
            attended = dot_f32(value_t[...], teacher_w[step]).T.astype(jnp.bfloat16)
            weighted[head, block_rows(step), :] = (
                weighting(other) * attended.astype(jnp.float32)
            ).astype(jnp.bfloat16)

        run_blocks(one_block)
        swap_copy(head).start()

    for step in range(inner):
        when_remote((step,), fan_copy(step).wait_recv)

    for head in range(heads_here):
        lanes = head_columns(head)
        arrived(1, head, 1)
        project(head, 1, s_key)
        key_t[...] = s_key[...].T
        arrived(1, head, 0)
        project(head, 0, s_query)
        teacher_weights(cfg, lanes)

        def one_block(step):
            probability = probs_by_key(s_key[...], s_query[block_rows(step), :])
            student_p[step] = probability
            if student_w is not None:
                student_w[step] = probability.astype(jnp.bfloat16)

        run_blocks(one_block)
        grad_key[...] = jnp.zeros_like(grad_key)
        grad_value[...] = jnp.zeros_like(grad_value)
        arrived(1, head, 2)
        project(head, 2, s_value)
        value_t[...] = s_value[...].T

        def one_block(step):
            attended = dot_f32(value_t[...], student_weights(step)).T
            student[block_rows(step), lanes] = attended.astype(jnp.bfloat16)

        run_blocks(one_block)
        each_out(head, "start")
        value_t[...] = heads[2, cfg, :, lanes].T

        def one_block(step):
            attended = dot_f32(value_t[...], teacher_w[step]).T.astype(jnp.bfloat16)
            target[block_rows(step), :] = weighting(cfg) * attended.astype(jnp.float32)

        run_blocks(one_block)
        swap_copy(head).wait_recv()

        def one_block(step):
            rows = block_rows(step)
            probability = student_p[step]
            aim = target[rows, :] + weighted_in[head, rows, :].astype(jnp.float32)
            error = student[rows, lanes].astype(jnp.float32) - aim
            upstream = (error * out_scale).astype(jnp.bfloat16)
            grad_value[...] += dot_f32(student_weights(step), upstream)
            prob_grad = dot_nt(s_value[...], upstream)
            center = jnp.sum(probability * prob_grad, axis=0, keepdims=True)
            score_grad = (probability * (prob_grad - center)).astype(jnp.bfloat16)
            grad_key[...] += dot_f32(score_grad, s_query[rows, :])
            grad_query[rows, :] = (dot_f32(key_t[...], score_grad).T * FACTOR).astype(
                jnp.bfloat16
            )

        run_blocks(one_block)

        gradients = (
            grad_query[...],
            (grad_key[...] * FACTOR).astype(jnp.bfloat16),
            grad_value[...].astype(jnp.bfloat16),
        )
        for member, gradient in enumerate(gradients):
            piece = dot_nt(gradient, up_own[member, :, lanes])
            if head > 0:
                piece = piece + back_sum[:, head_columns(member)]
            if head < heads_here - 1:
                back_sum[:, head_columns(member)] = piece
            else:
                back[:, head_columns(member)] = piece.astype(jnp.bfloat16)
                for far_step in far_order:
                    for step in range(1, inner):
                        near_copy(member, far_step, step).start()
        for member, gradient in enumerate(gradients):
            low_rank = ranks[:, :, :, head_columns(member)].reshape(length, ADAPTER_RANK)
            piece = dot_tn(low_rank, gradient).astype(jnp.bfloat16)
            up_parts[:, member, :, lanes] = piece.reshape(up_groups, -1, HDIM)

    each_up("start")
    own_store = pltpu.make_async_copy(
        student.at[own_rows, :], tokens_ref.at[:, aligned(me, columns)], local_sem.at[6]
    )

    @pl.when(diagonal)
    def _():
        own_store.start()
        up_in[0, 0, 0] = up_parts[cfg * dp_count + dp]

    down_rows = hidden_t.shape[0] // outer

    def gather_columns():
        for step in range(1, groups):
            cols_copy(step).wait_recv()
        hidden_t[...] = hidden_all[...].reshape(groups * tok_here, -1).T

    def reduce_near(member):
        lanes = head_columns(member)
        for far_step in far_order:
            row = lax.rem(far + far_step, outer)
            total = back[aligned(row * inner + part, tok_here), lanes].astype(jnp.float32)
            for step in range(1, inner):
                near_copy(member, far_step, step).wait_recv()
                total = total + near_in[far_step, step, :, lanes].astype(jnp.float32)
            if far_step > 0:
                far_out[far_step, :, lanes] = total.astype(jnp.bfloat16)
                far_copy(member, far_step).start()
        return total

    def reduce_far(member, total):
        lanes = head_columns(member)
        for step in range(1, outer):
            far_copy(member, step).wait_recv()
            total = total + far_in[step, :, lanes].astype(jnp.float32)
        low_grad = (total * work_facts[0]).astype(jnp.bfloat16)
        low[:, lanes] = low_grad
        low_all[low_slot(pair, dp), :, lanes] = low_grad
        for step in range(1, pairs):
            low_copy(member, step).start()
        for step in range(1, dp_count):
            share_copy(member, 0, step).start()

    def spread(member):
        for pair_step in range(1, pairs):
            low_copy(member, pair_step).wait_recv()
            for step in range(1, dp_count):
                share_copy(member, pair_step, step).start()

    def contract(member):
        lanes = head_columns(member)
        for pair_step in range(pairs):
            for step in range(1, dp_count):
                share_copy(member, pair_step, step).wait_recv()
        gathered_low = low_all[:, :, lanes].reshape(groups * tok_here, ADAPTER_RANK)
        partial = dot_f32(hidden_t[...], gathered_low).astype(jnp.bfloat16)
        for peer in range(outer):
            down_out[peer, :, lanes] = partial[peer * down_rows : (peer + 1) * down_rows, :]
        for step in range(1, outer):
            down_copy(member, step).start()

    totals = {}
    for turn in range(6):
        if turn < 3:
            totals[turn] = reduce_near(turn)
        if 1 <= turn < 4:
            reduce_far(turn - 1, totals[turn - 1])
        if turn == 1:
            gather_columns()
        if 2 <= turn < 5:
            spread(turn - 2)
        if turn >= 3:
            contract(turn - 3)

    each_up("wait_recv")
    up_total = up_in[up_steps[0]].astype(jnp.float32)
    for steps in up_steps[1:]:
        up_total = up_total + up_in[steps].astype(jnp.float32)
    grad_up_ref[...] = up_total

    for member in range(3):
        lanes = head_columns(member)
        down_total = down_out[far, :, lanes].astype(jnp.float32)
        for step in range(1, outer):
            down_copy(member, step).wait_recv()
            down_total = down_total + down_in[step, :, lanes].astype(jnp.float32)
        grad_down_ref[member] = down_total

    @pl.when(diagonal)
    def _():
        own_store.wait()
        for step in range(1, inner):
            facts_copy(step).wait_send()

    for turn in sends:
        each_field(*turn, "wait_send")
    for head in range(heads_here):
        swap_copy(head).wait_send()

        @pl.when(cfg == 0)
        def _():
            for member in range(3):
                pass_copy(head, member).wait_send()

        each_out(head, "wait")
    for hop in range(outer - 1):
        rank_step(hop, "wait_send", ranks_leave)
    for step in range(inner):
        when_remote((step,), fan_copy(step).wait_send)
    for step in range(1, groups):
        cols_copy(step).wait_send()
    each_up("wait_send")
    for member in range(3):
        for pair_step in range(pairs):
            if pair_step > 0:
                low_copy(member, pair_step).wait_send()
            for step in range(1, dp_count):
                share_copy(member, pair_step, step).wait_send()
        for far_step in range(outer):
            if far_step > 0:
                far_copy(member, far_step).wait_send()
                down_copy(member, far_step).wait_send()
            for step in range(1, inner):
                near_copy(member, far_step, step).wait_send()


def with_gaps(kernel, scratch, skipped):
    def filled(*refs):
        held = iter(refs[skipped:])
        kernel(*refs[:skipped], *[None if item is None else next(held) for item in scratch])

    return filled


def run_step(sizes, guide, time_index, fields, hidden, down, up):
    count, inner, dp_count = sizes
    outer = count // inner
    pairs = 2 * inner
    groups = pairs * dp_count
    up_groups = 2 * dp_count
    tok_here, width = fields[0].shape[1:]
    model_width = hidden.shape[1]
    length, columns = tok_here * count, width // count
    heads_here = columns // HDIM
    step_rows = min(BLOCK, BLOCK_AREA // length, length)
    rank_cols = 3 * ADAPTER_RANK
    group_cols = model_width // groups
    down_rows = group_cols // outer
    up_rows = ADAPTER_RANK // up_groups
    any_spec = pl.BlockSpec(memory_space=pl.ANY)
    vmem_spec = pl.BlockSpec(memory_space=pltpu.VMEM)
    smem_spec = pl.BlockSpec(memory_space=pltpu.SMEM)

    def bf16(*shape):
        return pltpu.VMEM(shape, jnp.bfloat16)

    def f32(*shape):
        return pltpu.VMEM(shape, jnp.float32)

    def sems(*shape):
        return [pltpu.SemaphoreType.DMA(shape)] * 2

    total_rows = 2 * dp_count * length
    keep_weights = 8 * length * length <= KEPT_BYTES
    scratch = [
        bf16(3, 3, length, columns),
        bf16(tok_here, model_width),
        bf16(groups, tok_here, group_cols),
        bf16(groups, tok_here, group_cols),
        bf16(group_cols, groups * tok_here),
        bf16(3, model_width, ADAPTER_RANK),
        bf16(3, ADAPTER_RANK, columns),
        bf16(outer, tok_here, rank_cols),
        bf16(outer, inner, tok_here, rank_cols),
        f32(3, 1, ADAPTER_RANK),
        f32(3, 1, ADAPTER_RANK),
        bf16(heads_here, length, HDIM),
        bf16(heads_here, length, HDIM),
        f32(length, HDIM),
        bf16(length, HDIM),
        bf16(length, HDIM),
        bf16(length, HDIM),
        bf16(HDIM, length),
        bf16(HDIM, length),
        bf16(length, HDIM),
        f32(length, HDIM),
        f32(length, HDIM),
        bf16(length // step_rows, length, step_rows),
        bf16(length // step_rows, length, step_rows) if keep_weights else None,
        f32(length // step_rows, length, step_rows),
        f32(length, rank_cols) if heads_here > 1 else None,
        bf16(length, rank_cols),
        bf16(outer, inner, tok_here, rank_cols),
        bf16(outer, tok_here, rank_cols),
        bf16(outer, tok_here, rank_cols),
        bf16(length, columns),
        bf16(up_groups, 3, up_rows, columns),
        bf16(2, dp_count // inner, inner, 3, up_rows, columns),
        bf16(tok_here, rank_cols),
        bf16(groups, tok_here, rank_cols),
        bf16(outer, down_rows, rank_cols),
        bf16(outer, down_rows, rank_cols),
        *sems(2, heads_here, 3, outer, inner),
        *sems(heads_here, 3),
        *sems(2, outer),
        *sems(inner),
        *sems(heads_here),
        *sems(heads_here, outer, inner),
        *sems(groups),
        *sems(2, dp_count // inner, inner),
        *sems(3, outer, inner),
        *sems(3, outer),
        *sems(3, pairs),
        *sems(3, pairs, dp_count),
        *sems(3, outer),
        *sems(inner),
        pltpu.SemaphoreType.DMA((7,)),
    ]
    return pl.pallas_call(
        with_gaps(functools.partial(step_kernel, sizes, 1.0 / math.sqrt(total_rows)), scratch, 11),
        out_shape=(
            jax.ShapeDtypeStruct((tok_here, width), jnp.bfloat16),
            jax.ShapeDtypeStruct((3, down_rows, ADAPTER_RANK), jnp.float32),
            jax.ShapeDtypeStruct((3, up_rows, columns), jnp.float32),
        ),
        in_specs=[smem_spec] * 2 + [any_spec] * 6,
        out_specs=(any_spec, vmem_spec, vmem_spec),
        scratch_shapes=[item for item in scratch if item is not None],
        compiler_params=pltpu.CompilerParams(
            collective_id=0, has_side_effects=True, vmem_limit_bytes=VMEM_LIMIT
        ),
        name="step",
    )(guide, time_index, *fields, hidden, down, up)


def emit_kernel(*refs):
    count = (len(refs) - 2) // 3
    held = refs[2 * count : 3 * count]
    load_sem, store_sem = refs[3 * count :]
    loads = [
        pltpu.make_async_copy(refs[item], held[item], load_sem.at[item]) for item in range(count)
    ]
    stores = [
        pltpu.make_async_copy(held[item], refs[count + item], store_sem.at[item])
        for item in range(count)
    ]
    for load in loads:
        load.start()
    for load, store in zip(loads, stores):
        load.wait()
        store.start()
    for store in stores:
        store.wait()


def emit(arrays):
    any_specs = (pl.BlockSpec(memory_space=pl.ANY),) * len(arrays)
    return pl.pallas_call(
        emit_kernel,
        out_shape=tuple(jax.ShapeDtypeStruct(array.shape, array.dtype) for array in arrays),
        in_specs=any_specs,
        out_specs=any_specs,
        scratch_shapes=[pltpu.VMEM(array.shape, array.dtype) for array in arrays]
        + [pltpu.SemaphoreType.DMA((len(arrays),))] * 2,
        compiler_params=pltpu.CompilerParams(vmem_limit_bytes=VMEM_LIMIT),
        name="emit",
    )(*arrays)


def body(
    teacher_query,
    teacher_key,
    teacher_value,
    hidden,
    adapter_down_weight,
    adapter_up_weight,
    guidance_index,
    timestep_index,
):
    seq_count = lax.axis_size("seq")
    dp_count = lax.axis_size("dp")
    outputs = run_step(
        (seq_count, inner_size(seq_count, dp_count), dp_count),
        guidance_index[:, 0],
        timestep_index[:, 0],
        (teacher_query[0, :, 0], teacher_key[0, :, 0], teacher_value[0, :, 0]),
        hidden[0, 0],
        adapter_down_weight,
        adapter_up_weight,
    )
    student_tokens, grad_down, grad_up = emit(outputs)
    return (student_tokens[None, None], grad_down, grad_up)


def solution(mesh):
    placed = (
        P("cfg", None, "dp", "seq", None),
        P("cfg", None, "dp", "seq", None),
        P("cfg", None, "dp", "seq", None),
        P("cfg", "dp", "seq", None),
        P(),
        P(),
        P(None, "dp"),
        P(None, "dp"),
    )
    return jax.shard_map(
        body,
        mesh=mesh,
        in_specs=placed,
        out_specs=(
            P("cfg", "dp", "seq", None),
            P(None, ("cfg", "seq", "dp"), None),
            P(None, ("cfg", "dp"), "seq"),
        ),
        check_vma=False,
    )
```

```python
import functools
import math

import jax
import jax.numpy as jnp
from jax import lax
from jax.experimental import pallas as pl
from jax.experimental.pallas import tpu as pltpu
from jax.sharding import PartitionSpec as P

HDIM = 128
ADAPTER_RANK = 128
TSTEPS = 1000
FACTOR = HDIM ** (-0.5)
FACTOR_BASE2 = FACTOR * math.log2(math.e)
VMEM_LIMIT = 63 * 1024 * 1024
BLOCK = 512
BLOCK_AREA = BLOCK * 1024
KEPT_BYTES = 16 * 1024 * 1024
MESH = pl.DeviceIdType.MESH

NT = (((1,), (1,)), ((), ()))
TN = (((0,), (0,)), ((), ()))


def dot_f32(left, right):
    return jnp.dot(left, right, preferred_element_type=jnp.float32)


def dot_nt(left, right):
    return lax.dot_general(left, right, NT, preferred_element_type=jnp.float32)


def dot_tn(left, right):
    return lax.dot_general(left, right, TN, preferred_element_type=jnp.float32)


def inner_size(count, dp_count):
    return max(
        size
        for size in range(1, count + 1)
        if count % size == 0 and dp_count % size == 0 and size * size <= count
    )


def aligned(index, size):
    return pl.ds(pl.multiple_of(index * size, size), size)


def probs_by_key(key_head, query_block):
    scores = dot_nt(key_head, query_block)
    highest = jnp.max(scores, axis=0, keepdims=True)
    raised = jnp.exp2((scores - highest) * FACTOR_BASE2)
    return raised * (1.0 / jnp.sum(raised, axis=0, keepdims=True))


def step_kernel(
    sizes,
    out_scale,
    guide_ref,
    time_ref,
    query_ref,
    key_ref,
    value_ref,
    hidden_ref,
    down_ref,
    up_ref,
    tokens_ref,
    grad_down_ref,
    grad_up_ref,
    heads,
    hidden_own,
    hidden_cols,
    hidden_all,
    hidden_t,
    down_own,
    up_own,
    rank_line,
    ranks,
    facts,
    work_facts,
    weighted,
    weighted_in,
    target,
    s_query,
    s_key,
    s_value,
    key_t,
    value_t,
    upstream,
    grad_query,
    grad_key,
    grad_value,
    teacher_w,
    student_w,
    student_p,
    back_sum,
    back,
    near_in,
    far_out,
    far_in,
    student,
    up_parts,
    up_in,
    low,
    low_all,
    down_out,
    down_in,
    field_send,
    field_recv,
    pass_send,
    pass_recv,
    rank_send,
    rank_recv,
    fan_send,
    fan_recv,
    swap_send,
    swap_recv,
    out_send,
    out_recv,
    cols_send,
    cols_recv,
    up_send,
    up_recv,
    near_send,
    near_recv,
    far_send,
    far_recv,
    low_send,
    low_recv,
    share_send,
    share_recv,
    down_send,
    down_recv,
    facts_send,
    facts_recv,
    local_sem,
):
    count, inner, dp_count = sizes
    outer = count // inner
    pairs = 2 * inner
    groups = pairs * dp_count
    up_groups = 2 * dp_count
    fields = (query_ref, key_ref, value_ref)
    tok_here = query_ref.shape[1]
    length = tok_here * count
    columns = student.shape[1]
    heads_here = columns // HDIM
    step_rows = min(BLOCK, BLOCK_AREA // length, length)
    blocks = length // step_rows

    me = lax.axis_index("seq")
    cfg = lax.axis_index("cfg")
    dp = lax.axis_index("dp")
    other = 1 - cfg
    far = me // inner
    near = lax.rem(me, inner)
    part = lax.rem(dp, inner)
    bundle = dp // inner
    bundles = dp_count // inner
    diagonal = near == part
    off_diagonal = near != part
    pair = cfg * inner + near
    group = dp * pairs + pair
    work_block = far * inner + part
    own_rows = aligned(me, tok_here)
    grid_steps = [(far_step, near_step) for far_step in range(outer) for near_step in range(inner)]
    up_steps = [
        (cfg_step, bundle_step, near_step)
        for cfg_step in range(2)
        for bundle_step in range(bundles)
        for near_step in range(inner)
    ]
    order = (other, cfg)

    def head_columns(head):
        return slice(head * HDIM, (head + 1) * HDIM)

    def when_remote(steps, action):
        if any(steps):
            action()
        else:
            pl.when(off_diagonal)(action)

    def low_slot(pair_index, dp_index):
        return (
            dp_index // inner * inner + lax.rem(pair_index, inner)
        ) * pairs + pair_index // inner * inner + lax.rem(dp_index, inner)

    def device_of(pair_index):
        return {"cfg": pair_index // inner, "seq": far * inner + lax.rem(pair_index, inner)}

    def group_device(step):
        peer = lax.rem(group + step, groups)
        return {**device_of(lax.rem(peer, pairs)), "dp": peer // pairs}

    def remote(src, dst, send, recv, device):
        return pltpu.make_async_remote_copy(
            src_ref=src,
            dst_ref=dst,
            send_sem=send,
            recv_sem=recv,
            device_id=device,
            device_id_type=MESH,
        )

    loads = [
        pltpu.make_async_copy(hidden_ref, hidden_own, local_sem.at[0]),
        pltpu.make_async_copy(down_ref, down_own, local_sem.at[1]),
        pltpu.make_async_copy(
            up_ref.at[:, :, aligned(work_block, columns)], up_own, local_sem.at[2]
        ),
    ]
    own_loads = [
        pltpu.make_async_copy(
            fields[member].at[:, :, aligned(me, columns)],
            heads.at[member, 0:2, own_rows, :],
            local_sem.at[3 + member],
        )
        for member in range(3)
    ]
    for load in loads:
        load.start()

    @pl.when(diagonal)
    def _():
        for load in own_loads:
            load.start()

    barrier = pltpu.get_barrier_semaphore()
    for step in range(1, count * inner):
        peer_near = lax.rem(near + step // inner % inner, inner)
        peer_part = lax.rem(part + step % inner, inner)
        pl.semaphore_signal(
            barrier,
            inc=1,
            device_id={
                "seq": lax.rem(far + step // (inner * inner), outer) * inner + peer_near,
                "dp": bundle * inner + peer_part,
            },
            device_id_type=MESH,
        )
    for step in range(1, groups):
        pl.semaphore_signal(barrier, inc=1, device_id=group_device(step), device_id_type=MESH)

    def field_copy(phase, head, member, steps):
        peer_far = lax.rem(far + steps[0], outer)
        peer_part = lax.rem(near + steps[1], inner)
        half = order[phase]
        start = pl.multiple_of((peer_far * inner + peer_part) * columns, columns) + head * HDIM
        return remote(
            fields[member].at[half, :, pl.ds(start, HDIM)],
            heads.at[member, half, own_rows, head_columns(head)],
            field_send.at[phase, head, member, *steps],
            field_recv.at[phase, head, member, *steps],
            {"seq": peer_far * inner + part, "dp": bundle * inner + peer_part},
        )

    def each_field(phase, head, member, action):
        for steps in grid_steps:
            when_remote(steps, getattr(field_copy(phase, head, member, steps), action))

    def pass_copy(head, member):
        return remote(
            heads.at[member, 1, :, head_columns(head)],
            heads.at[member, 2, :, head_columns(head)],
            pass_send.at[head, member],
            pass_recv.at[head, member],
            {"cfg": other},
        )

    def rank_copy(way, hop):
        toward, back_by = (1, outer - hop) if way == 0 else (outer - 1, hop)
        block = rank_line.at[lax.rem(far + back_by, outer)]
        return remote(
            block,
            block,
            rank_send.at[way, hop],
            rank_recv.at[way, hop],
            {"seq": lax.rem(far + toward, outer) * inner + near},
        )

    def ranks_leave(way, hop):
        if way == 0:
            return jnp.logical_and(far >= hop, far < outer - 1)
        return jnp.logical_and(far < outer - hop, far > 0)

    def ranks_come(way, hop):
        return far > hop if way == 0 else far < outer - 1 - hop

    def rank_step(hop, action, test):
        for way in range(2):

            @pl.when(test(way, hop))
            def _():
                getattr(rank_copy(way, hop), action)()

    def fan_copy(step):
        peer_part = lax.rem(near + step, inner)
        return remote(
            rank_line,
            ranks.at[:, near],
            fan_send.at[step],
            fan_recv.at[step],
            {"seq": far * inner + part, "dp": bundle * inner + peer_part},
        )

    def facts_copy(step):
        return remote(
            facts,
            work_facts,
            facts_send.at[step],
            facts_recv.at[0],
            {"dp": bundle * inner + lax.rem(part + step, inner)},
        )

    def swap_copy(head):
        return remote(
            weighted.at[head],
            weighted_in.at[head],
            swap_send.at[head],
            swap_recv.at[head],
            {"cfg": other},
        )

    def out_copy(head, steps):
        peer = lax.rem(far + steps[0], outer) * inner + lax.rem(part + steps[1], inner)
        start = pl.multiple_of(work_block * columns, columns) + head * HDIM
        return remote(
            student.at[aligned(peer, tok_here), head_columns(head)],
            tokens_ref.at[:, pl.ds(start, HDIM)],
            out_send.at[head, *steps],
            out_recv.at[head, *steps],
            {"seq": peer, "dp": bundle * inner + near},
        )

    def each_out(head, action):
        for steps in grid_steps:
            when_remote(steps, getattr(out_copy(head, steps), action))

    def cols_copy(step):
        return remote(
            hidden_cols.at[lax.rem(group + step, groups)],
            hidden_all.at[group],
            cols_send.at[step],
            cols_recv.at[step],
            group_device(step),
        )

    def up_copy(steps):
        peer_cfg = lax.rem(cfg + steps[0], 2)
        peer_dp = lax.rem(bundle + steps[1], bundles) * inner + lax.rem(near + steps[2], inner)
        return remote(
            up_parts.at[peer_cfg * dp_count + peer_dp],
            up_in.at[steps],
            up_send.at[steps],
            up_recv.at[steps],
            {"cfg": peer_cfg, "seq": work_block, "dp": peer_dp},
        )

    def each_up(action):
        for steps in up_steps:
            when_remote(steps, getattr(up_copy(steps), action))

    def near_copy(member, far_step, step):
        peer = lax.rem(part + step, inner)
        row = lax.rem(far + far_step, outer)
        return remote(
            back.at[aligned(row * inner + peer, tok_here), head_columns(member)],
            near_in.at[far_step, step, :, head_columns(member)],
            near_send.at[member, far_step, step],
            near_recv.at[member, far_step, step],
            {"dp": bundle * inner + peer},
        )

    def far_copy(member, step):
        return remote(
            far_out.at[step, :, head_columns(member)],
            far_in.at[step, :, head_columns(member)],
            far_send.at[member, step],
            far_recv.at[member, step],
            {"seq": lax.rem(far + step, outer) * inner + near},
        )

    def low_copy(member, step):
        return remote(
            low.at[:, head_columns(member)],
            low_all.at[low_slot(pair, dp), :, head_columns(member)],
            low_send.at[member, step],
            low_recv.at[member, step],
            device_of(lax.rem(pair + step, pairs)),
        )

    def share_copy(member, pair_step, step):
        source = lax.rem(pair - pair_step + pairs, pairs)
        lanes = head_columns(member)
        slot = low_all.at[low_slot(source, dp), :, lanes]
        return remote(
            low.at[:, lanes] if pair_step == 0 else slot,
            slot,
            share_send.at[member, pair_step, step],
            share_recv.at[member, pair_step, step],
            {"dp": lax.rem(dp + step, dp_count)},
        )

    def down_copy(member, step):
        peer = lax.rem(far + step, outer)
        return remote(
            down_out.at[peer, :, head_columns(member)],
            down_in.at[step, :, head_columns(member)],
            down_send.at[member, step],
            down_recv.at[member, step],
            {"seq": peer * inner + near},
        )

    def guide_scale(half):
        return 1.0 + 0.5 * guide_ref[half].astype(jnp.float32)

    rank_index = (lax.broadcasted_iota(jnp.int32, (1, ADAPTER_RANK), 1) + 1).astype(jnp.float32)
    time_frac = (time_ref[cfg].astype(jnp.float32) + 0.5) / TSTEPS
    modulation = 1.0 + 0.5 * jnp.cos(
        math.pi * rank_index * time_frac + 0.25 * rank_index * guide_scale(cfg)
    )

    facts[0] = modulation
    for half in range(2):
        facts[1 + half] = jnp.full((1, ADAPTER_RANK), guide_scale(half), jnp.float32)

    def weighting(half):
        scale = work_facts[1 + half]
        return jnp.where(cfg == 0, scale, 1.0 - scale)

    phases = [(phase, head) for phase in range(2) for head in range(heads_here)]
    sends = [(phase, head, member) for phase, head in phases for member in (1, 0, 2)]
    pl.semaphore_wait(barrier, count * inner + groups - 2)
    each_field(*sends[0], "start")

    @pl.when(diagonal)
    def _():
        work_facts[...] = facts[...]
        for step in range(1, inner):
            facts_copy(step).start()

    loads[0].wait()
    loads[1].wait()
    for member in range(3):
        projected = dot_f32(hidden_own[...], down_own[member]) * modulation
        rank_line[far, :, head_columns(member)] = projected.astype(jnp.bfloat16)
    for hop in range(outer - 1):
        rank_step(hop, "start", ranks_leave)
        each_field(*sends[1 + hop], "start")
        rank_step(hop, "wait_recv", ranks_come)
    for step in range(inner):
        when_remote((step,), fan_copy(step).start)
    for turn in sends[outer:]:
        each_field(*turn, "start")

    @pl.when(diagonal)
    def _():
        ranks[:, near] = rank_line[...]

    @pl.when(off_diagonal)
    def _():
        facts_copy(inner - 1).wait_recv()

    rows_here = hidden_cols.shape[2] // outer
    for block in range(outer * groups):
        target_dp = block % dp_count
        target_near = block // dp_count % inner
        target_far = block // dp_count // inner % outer
        target_pair = block // (dp_count * count) * inner + target_near
        hidden_cols[
            target_dp * pairs + target_pair, :, target_far * rows_here : (target_far + 1) * rows_here
        ] = hidden_own[:, block * rows_here : (block + 1) * rows_here]
    hidden_all[group] = hidden_cols[group]
    for step in range(1, groups):
        cols_copy(step).start()
    loads[2].wait()

    @pl.when(diagonal)
    def _():
        for load in own_loads:
            load.wait()

    far_order = sorted(range(outer), key=lambda step: (step == 0, abs(2 * step - outer)))

    def run_blocks(one_block):
        unroll = 2 if blocks % 2 == 0 else 1

        def some(step, _):
            for offset in range(unroll):
                one_block(step * unroll + offset)
            return 0

        lax.fori_loop(0, blocks // unroll, some, 0)

    def block_rows(step):
        return aligned(step, step_rows)

    def teacher_weights(half, lanes):
        def one_block(step):
            probability = probs_by_key(
                heads[1, half, :, lanes], heads[0, half, block_rows(step), lanes]
            )
            teacher_w[step] = probability.astype(jnp.bfloat16)

        run_blocks(one_block)

    def student_weights(step):
        if student_w is None:
            return student_p[step].astype(jnp.bfloat16)
        return student_w[step]

    def arrived(phase, head, member):
        each_field(phase, head, member, "wait_recv")
        if phase == 0:
            pl.when(cfg == 0)(pass_copy(head, member).start)

    def project(head, member, projected):
        lanes = head_columns(head)
        pl.when(cfg == 1)(pass_copy(head, member).wait_recv)
        low_rank = ranks[:, :, :, head_columns(member)].reshape(length, ADAPTER_RANK)
        frozen = heads[member, 2 * cfg, :, lanes].astype(jnp.float32)
        projected[...] = (frozen + dot_f32(low_rank, up_own[member, :, lanes])).astype(
            jnp.bfloat16
        )

    for head in range(heads_here):
        lanes = head_columns(head)
        arrived(0, head, 1)
        arrived(0, head, 0)
        teacher_weights(other, lanes)
        arrived(0, head, 2)
        value_t[...] = heads[2, other, :, lanes].T

        def one_block(step):
            attended = dot_f32(value_t[...], teacher_w[step]).T.astype(jnp.bfloat16)
            weighted[head, block_rows(step), :] = (
                weighting(other) * attended.astype(jnp.float32)
            ).astype(jnp.bfloat16)

        run_blocks(one_block)
        swap_copy(head).start()

    for step in range(inner):
        when_remote((step,), fan_copy(step).wait_recv)

    def reduce_near(member):
        lanes = head_columns(member)
        for far_step in far_order:
            row = lax.rem(far + far_step, outer)
            total = back[aligned(row * inner + part, tok_here), lanes].astype(jnp.float32)
            for step in range(1, inner):
                near_copy(member, far_step, step).wait_recv()
                total = total + near_in[far_step, step, :, lanes].astype(jnp.float32)
            if far_step > 0:
                far_out[far_step, :, lanes] = total.astype(jnp.bfloat16)
                far_copy(member, far_step).start()
        return total

    def push_back(head, member, gradient):
        lanes = head_columns(member)
        piece = dot_nt(gradient, up_own[member, :, head_columns(head)])
        if head > 0:
            piece = piece + back_sum[:, lanes]
        if head < heads_here - 1:
            back_sum[:, lanes] = piece
            return
        back[:, lanes] = piece.astype(jnp.bfloat16)
        for far_step in far_order:
            for step in range(1, inner):
                near_copy(member, far_step, step).start()

    totals = {}
    for head in range(heads_here):
        lanes = head_columns(head)
        arrived(1, head, 1)
        project(head, 1, s_key)
        key_t[...] = s_key[...].T
        arrived(1, head, 0)
        project(head, 0, s_query)
        teacher_weights(cfg, lanes)

        def one_block(step):
            probability = probs_by_key(s_key[...], s_query[block_rows(step), :])
            student_p[step] = probability
            if student_w is not None:
                student_w[step] = probability.astype(jnp.bfloat16)

        run_blocks(one_block)
        grad_key[...] = jnp.zeros_like(grad_key)
        grad_value[...] = jnp.zeros_like(grad_value)
        arrived(1, head, 2)
        project(head, 2, s_value)
        value_t[...] = s_value[...].T

        def one_block(step):
            attended = dot_f32(value_t[...], student_weights(step)).T
            student[block_rows(step), lanes] = attended.astype(jnp.bfloat16)

        run_blocks(one_block)
        each_out(head, "start")
        value_t[...] = heads[2, cfg, :, lanes].T

        def one_block(step):
            attended = dot_f32(value_t[...], teacher_w[step]).T.astype(jnp.bfloat16)
            target[block_rows(step), :] = weighting(cfg) * attended.astype(jnp.float32)

        run_blocks(one_block)
        swap_copy(head).wait_recv()

        def one_block(step):
            rows = block_rows(step)
            aim = target[rows, :] + weighted_in[head, rows, :].astype(jnp.float32)
            error = student[rows, lanes].astype(jnp.float32) - aim
            upstream[rows, :] = (error * out_scale).astype(jnp.bfloat16)
            grad_value[...] += dot_f32(student_weights(step), upstream[rows, :])

        run_blocks(one_block)
        last = head == heads_here - 1
        gradients = {2: grad_value[...].astype(jnp.bfloat16)}
        push_back(head, 2, gradients[2])

        def one_block(step):
            rows = block_rows(step)
            probability = student_p[step]
            prob_grad = dot_nt(s_value[...], upstream[rows, :])
            center = jnp.sum(probability * prob_grad, axis=0, keepdims=True)
            score_grad = (probability * (prob_grad - center)).astype(jnp.bfloat16)
            grad_key[...] += dot_f32(score_grad, s_query[rows, :])
            grad_query[rows, :] = (dot_f32(key_t[...], score_grad).T * FACTOR).astype(
                jnp.bfloat16
            )

        run_blocks(one_block)
        if last:
            totals[2] = reduce_near(2)
        gradients[1] = (grad_key[...] * FACTOR).astype(jnp.bfloat16)
        push_back(head, 1, gradients[1])
        gradients[0] = grad_query[...]
        push_back(head, 0, gradients[0])
        if last:
            totals[1] = reduce_near(1)
            totals[0] = reduce_near(0)
        for member, gradient in gradients.items():
            low_rank = ranks[:, :, :, head_columns(member)].reshape(length, ADAPTER_RANK)
            piece = dot_tn(low_rank, gradient).astype(jnp.bfloat16)
            up_parts[:, member, :, lanes] = piece.reshape(up_groups, -1, HDIM)

    each_up("start")
    own_store = pltpu.make_async_copy(
        student.at[own_rows, :], tokens_ref.at[:, aligned(me, columns)], local_sem.at[6]
    )

    @pl.when(diagonal)
    def _():
        own_store.start()
        up_in[0, 0, 0] = up_parts[cfg * dp_count + dp]

    down_rows = hidden_t.shape[0] // outer

    def gather_columns():
        for step in range(1, groups):
            cols_copy(step).wait_recv()
        hidden_t[...] = hidden_all[...].reshape(groups * tok_here, -1).T

    def reduce_far(member, total):
        lanes = head_columns(member)
        for step in range(1, outer):
            far_copy(member, step).wait_recv()
            total = total + far_in[step, :, lanes].astype(jnp.float32)
        low_grad = (total * work_facts[0]).astype(jnp.bfloat16)
        low[:, lanes] = low_grad
        low_all[low_slot(pair, dp), :, lanes] = low_grad
        for step in range(1, pairs):
            low_copy(member, step).start()
        for step in range(1, dp_count):
            share_copy(member, 0, step).start()

    def spread(member):
        for pair_step in range(1, pairs):
            low_copy(member, pair_step).wait_recv()
            for step in range(1, dp_count):
                share_copy(member, pair_step, step).start()

    def contract(member):
        lanes = head_columns(member)
        for pair_step in range(pairs):
            for step in range(1, dp_count):
                share_copy(member, pair_step, step).wait_recv()
        gathered_low = low_all[:, :, lanes].reshape(groups * tok_here, ADAPTER_RANK)
        partial = dot_f32(hidden_t[...], gathered_low).astype(jnp.bfloat16)
        for peer in range(outer):
            down_out[peer, :, lanes] = partial[peer * down_rows : (peer + 1) * down_rows, :]
        for step in range(1, outer):
            down_copy(member, step).start()

    reduce_far(2, totals[2])
    gather_columns()
    reduce_far(1, totals[1])
    spread(2)
    contract(2)
    reduce_far(0, totals[0])
    spread(1)
    contract(1)
    spread(0)
    contract(0)

    each_up("wait_recv")
    up_total = up_in[up_steps[0]].astype(jnp.float32)
    for steps in up_steps[1:]:
        up_total = up_total + up_in[steps].astype(jnp.float32)
    grad_up_ref[...] = up_total

    for member in (2, 1, 0):
        lanes = head_columns(member)
        down_total = down_out[far, :, lanes].astype(jnp.float32)
        for step in range(1, outer):
            down_copy(member, step).wait_recv()
            down_total = down_total + down_in[step, :, lanes].astype(jnp.float32)
        grad_down_ref[member] = down_total

    @pl.when(diagonal)
    def _():
        own_store.wait()
        for step in range(1, inner):
            facts_copy(step).wait_send()

    for turn in sends:
        each_field(*turn, "wait_send")
    for head in range(heads_here):
        swap_copy(head).wait_send()

        @pl.when(cfg == 0)
        def _():
            for member in range(3):
                pass_copy(head, member).wait_send()

        each_out(head, "wait")
    for hop in range(outer - 1):
        rank_step(hop, "wait_send", ranks_leave)
    for step in range(inner):
        when_remote((step,), fan_copy(step).wait_send)
    for step in range(1, groups):
        cols_copy(step).wait_send()
    each_up("wait_send")
    for member in range(3):
        for pair_step in range(pairs):
            if pair_step > 0:
                low_copy(member, pair_step).wait_send()
            for step in range(1, dp_count):
                share_copy(member, pair_step, step).wait_send()
        for far_step in range(outer):
            if far_step > 0:
                far_copy(member, far_step).wait_send()
                down_copy(member, far_step).wait_send()
            for step in range(1, inner):
                near_copy(member, far_step, step).wait_send()


def with_gaps(kernel, scratch, skipped):
    def filled(*refs):
        held = iter(refs[skipped:])
        kernel(*refs[:skipped], *[None if item is None else next(held) for item in scratch])

    return filled


def run_step(sizes, guide, time_index, fields, hidden, down, up):
    count, inner, dp_count = sizes
    outer = count // inner
    pairs = 2 * inner
    groups = pairs * dp_count
    up_groups = 2 * dp_count
    tok_here, width = fields[0].shape[1:]
    model_width = hidden.shape[1]
    length, columns = tok_here * count, width // count
    heads_here = columns // HDIM
    step_rows = min(BLOCK, BLOCK_AREA // length, length)
    rank_cols = 3 * ADAPTER_RANK
    group_cols = model_width // groups
    down_rows = group_cols // outer
    up_rows = ADAPTER_RANK // up_groups
    any_spec = pl.BlockSpec(memory_space=pl.ANY)
    vmem_spec = pl.BlockSpec(memory_space=pltpu.VMEM)
    smem_spec = pl.BlockSpec(memory_space=pltpu.SMEM)

    def bf16(*shape):
        return pltpu.VMEM(shape, jnp.bfloat16)

    def f32(*shape):
        return pltpu.VMEM(shape, jnp.float32)

    def sems(*shape):
        return [pltpu.SemaphoreType.DMA(shape)] * 2

    total_rows = 2 * dp_count * length
    keep_weights = 8 * length * length <= KEPT_BYTES
    scratch = [
        bf16(3, 3, length, columns),
        bf16(tok_here, model_width),
        bf16(groups, tok_here, group_cols),
        bf16(groups, tok_here, group_cols),
        bf16(group_cols, groups * tok_here),
        bf16(3, model_width, ADAPTER_RANK),
        bf16(3, ADAPTER_RANK, columns),
        bf16(outer, tok_here, rank_cols),
        bf16(outer, inner, tok_here, rank_cols),
        f32(3, 1, ADAPTER_RANK),
        f32(3, 1, ADAPTER_RANK),
        bf16(heads_here, length, HDIM),
        bf16(heads_here, length, HDIM),
        f32(length, HDIM),
        bf16(length, HDIM),
        bf16(length, HDIM),
        bf16(length, HDIM),
        bf16(HDIM, length),
        bf16(HDIM, length),
        bf16(length, HDIM),
        bf16(length, HDIM),
        f32(length, HDIM),
        f32(length, HDIM),
        bf16(length // step_rows, length, step_rows),
        bf16(length // step_rows, length, step_rows) if keep_weights else None,
        f32(length // step_rows, length, step_rows),
        f32(length, rank_cols) if heads_here > 1 else None,
        bf16(length, rank_cols),
        bf16(outer, inner, tok_here, rank_cols),
        bf16(outer, tok_here, rank_cols),
        bf16(outer, tok_here, rank_cols),
        bf16(length, columns),
        bf16(up_groups, 3, up_rows, columns),
        bf16(2, dp_count // inner, inner, 3, up_rows, columns),
        bf16(tok_here, rank_cols),
        bf16(groups, tok_here, rank_cols),
        bf16(outer, down_rows, rank_cols),
        bf16(outer, down_rows, rank_cols),
        *sems(2, heads_here, 3, outer, inner),
        *sems(heads_here, 3),
        *sems(2, outer),
        *sems(inner),
        *sems(heads_here),
        *sems(heads_here, outer, inner),
        *sems(groups),
        *sems(2, dp_count // inner, inner),
        *sems(3, outer, inner),
        *sems(3, outer),
        *sems(3, pairs),
        *sems(3, pairs, dp_count),
        *sems(3, outer),
        *sems(inner),
        pltpu.SemaphoreType.DMA((7,)),
    ]
    return pl.pallas_call(
        with_gaps(functools.partial(step_kernel, sizes, 1.0 / math.sqrt(total_rows)), scratch, 11),
        out_shape=(
            jax.ShapeDtypeStruct((tok_here, width), jnp.bfloat16),
            jax.ShapeDtypeStruct((3, down_rows, ADAPTER_RANK), jnp.float32),
            jax.ShapeDtypeStruct((3, up_rows, columns), jnp.float32),
        ),
        in_specs=[smem_spec] * 2 + [any_spec] * 6,
        out_specs=(any_spec, vmem_spec, vmem_spec),
        scratch_shapes=[item for item in scratch if item is not None],
        compiler_params=pltpu.CompilerParams(
            collective_id=0, has_side_effects=True, vmem_limit_bytes=VMEM_LIMIT
        ),
        name="step",
    )(guide, time_index, *fields, hidden, down, up)


def emit_kernel(*refs):
    count = (len(refs) - 2) // 3
    held = refs[2 * count : 3 * count]
    load_sem, store_sem = refs[3 * count :]
    loads = [
        pltpu.make_async_copy(refs[item], held[item], load_sem.at[item]) for item in range(count)
    ]
    stores = [
        pltpu.make_async_copy(held[item], refs[count + item], store_sem.at[item])
        for item in range(count)
    ]
    for load in loads:
        load.start()
    for load, store in zip(loads, stores):
        load.wait()
        store.start()
    for store in stores:
        store.wait()


def emit(arrays):
    any_specs = (pl.BlockSpec(memory_space=pl.ANY),) * len(arrays)
    return pl.pallas_call(
        emit_kernel,
        out_shape=tuple(jax.ShapeDtypeStruct(array.shape, array.dtype) for array in arrays),
        in_specs=any_specs,
        out_specs=any_specs,
        scratch_shapes=[pltpu.VMEM(array.shape, array.dtype) for array in arrays]
        + [pltpu.SemaphoreType.DMA((len(arrays),))] * 2,
        compiler_params=pltpu.CompilerParams(vmem_limit_bytes=VMEM_LIMIT),
        name="emit",
    )(*arrays)


def body(
    teacher_query,
    teacher_key,
    teacher_value,
    hidden,
    adapter_down_weight,
    adapter_up_weight,
    guidance_index,
    timestep_index,
):
    seq_count = lax.axis_size("seq")
    dp_count = lax.axis_size("dp")
    outputs = run_step(
        (seq_count, inner_size(seq_count, dp_count), dp_count),
        guidance_index[:, 0],
        timestep_index[:, 0],
        (teacher_query[0, :, 0], teacher_key[0, :, 0], teacher_value[0, :, 0]),
        hidden[0, 0],
        adapter_down_weight,
        adapter_up_weight,
    )
    student_tokens, grad_down, grad_up = emit(outputs)
    return (student_tokens[None, None], grad_down, grad_up)


def solution(mesh):
    placed = (
        P("cfg", None, "dp", "seq", None),
        P("cfg", None, "dp", "seq", None),
        P("cfg", None, "dp", "seq", None),
        P("cfg", "dp", "seq", None),
        P(),
        P(),
        P(None, "dp"),
        P(None, "dp"),
    )
    return jax.shard_map(
        body,
        mesh=mesh,
        in_specs=placed,
        out_specs=(
            P("cfg", "dp", "seq", None),
            P(None, ("cfg", "seq", "dp"), None),
            P(None, ("cfg", "dp"), "seq"),
        ),
        check_vma=False,
    )
```

```python
import functools
import math

import jax
import jax.numpy as jnp
from jax import lax
from jax.experimental import pallas as pl
from jax.experimental.pallas import tpu as pltpu
from jax.sharding import PartitionSpec as P

HDIM = 128
ADAPTER_RANK = 128
TSTEPS = 1000
FACTOR = HDIM ** (-0.5)
FACTOR_BASE2 = FACTOR * math.log2(math.e)
VMEM_LIMIT = 63 * 1024 * 1024
BLOCK = 512
BLOCK_AREA = BLOCK * 1024
KEPT_BYTES = 16 * 1024 * 1024
MESH = pl.DeviceIdType.MESH

NT = (((1,), (1,)), ((), ()))
TN = (((0,), (0,)), ((), ()))


def dot_f32(left, right):
    return jnp.dot(left, right, preferred_element_type=jnp.float32)


def dot_nt(left, right):
    return lax.dot_general(left, right, NT, preferred_element_type=jnp.float32)


def dot_tn(left, right):
    return lax.dot_general(left, right, TN, preferred_element_type=jnp.float32)


def inner_size(count, dp_count):
    return max(
        size
        for size in range(1, count + 1)
        if count % size == 0 and dp_count % size == 0 and size * size <= count
    )


def aligned(index, size):
    return pl.ds(pl.multiple_of(index * size, size), size)


def probs_by_key(key_head, query_block):
    scores = dot_nt(key_head, query_block)
    highest = jnp.max(scores, axis=0, keepdims=True)
    raised = jnp.exp2((scores - highest) * FACTOR_BASE2)
    return raised * (1.0 / jnp.sum(raised, axis=0, keepdims=True))


def step_kernel(
    sizes,
    out_scale,
    guide_ref,
    time_ref,
    query_ref,
    key_ref,
    value_ref,
    hidden_ref,
    down_ref,
    up_ref,
    tokens_ref,
    grad_down_ref,
    grad_up_ref,
    heads,
    hidden_own,
    hidden_cols,
    hidden_all,
    hidden_t,
    down_own,
    up_own,
    rank_line,
    ranks,
    facts,
    work_facts,
    weighted,
    weighted_in,
    target,
    s_query,
    s_key,
    s_value,
    key_t,
    value_t,
    upstream,
    grad_query,
    grad_key,
    grad_value,
    teacher_w,
    student_w,
    student_p,
    back_sum,
    back,
    near_in,
    far_out,
    far_in,
    student,
    up_parts,
    up_in,
    low,
    low_all,
    down_out,
    down_in,
    field_send,
    field_recv,
    pass_send,
    pass_recv,
    rank_send,
    rank_recv,
    fan_send,
    fan_recv,
    swap_send,
    swap_recv,
    out_send,
    out_recv,
    cols_send,
    cols_recv,
    up_send,
    up_recv,
    near_send,
    near_recv,
    far_send,
    far_recv,
    low_send,
    low_recv,
    share_send,
    share_recv,
    down_send,
    down_recv,
    facts_send,
    facts_recv,
    local_sem,
):
    count, inner, dp_count = sizes
    outer = count // inner
    pairs = 2 * inner
    groups = pairs * dp_count
    up_groups = 2 * dp_count
    fields = (query_ref, key_ref, value_ref)
    tok_here = query_ref.shape[1]
    length = tok_here * count
    columns = student.shape[1]
    heads_here = columns // HDIM
    step_rows = min(BLOCK, BLOCK_AREA // length, length)
    blocks = length // step_rows

    me = lax.axis_index("seq")
    cfg = lax.axis_index("cfg")
    dp = lax.axis_index("dp")
    other = 1 - cfg
    far = me // inner
    near = lax.rem(me, inner)
    part = lax.rem(dp, inner)
    bundle = dp // inner
    bundles = dp_count // inner
    diagonal = near == part
    off_diagonal = near != part
    pair = cfg * inner + near
    group = dp * pairs + pair
    work_block = far * inner + part
    own_rows = aligned(me, tok_here)
    grid_steps = [(far_step, near_step) for far_step in range(outer) for near_step in range(inner)]
    up_steps = [
        (cfg_step, bundle_step, near_step)
        for cfg_step in range(2)
        for bundle_step in range(bundles)
        for near_step in range(inner)
    ]
    order = (other, cfg)

    def head_columns(head):
        return slice(head * HDIM, (head + 1) * HDIM)

    def when_remote(steps, action):
        if any(steps):
            action()
        else:
            pl.when(off_diagonal)(action)

    def low_slot(pair_index, dp_index):
        return (
            dp_index // inner * inner + lax.rem(pair_index, inner)
        ) * pairs + pair_index // inner * inner + lax.rem(dp_index, inner)

    def device_of(pair_index):
        return {"cfg": pair_index // inner, "seq": far * inner + lax.rem(pair_index, inner)}

    def group_device(step):
        peer = lax.rem(group + step, groups)
        return {**device_of(lax.rem(peer, pairs)), "dp": peer // pairs}

    def remote(src, dst, send, recv, device):
        return pltpu.make_async_remote_copy(
            src_ref=src,
            dst_ref=dst,
            send_sem=send,
            recv_sem=recv,
            device_id=device,
            device_id_type=MESH,
        )

    loads = [
        pltpu.make_async_copy(hidden_ref, hidden_own, local_sem.at[0]),
        pltpu.make_async_copy(down_ref, down_own, local_sem.at[1]),
        pltpu.make_async_copy(
            up_ref.at[:, :, aligned(work_block, columns)], up_own, local_sem.at[2]
        ),
    ]
    own_loads = [
        pltpu.make_async_copy(
            fields[member].at[:, :, aligned(me, columns)],
            heads.at[member, 0:2, own_rows, :],
            local_sem.at[3 + member],
        )
        for member in range(3)
    ]
    barrier = pltpu.get_barrier_semaphore()
    for step in range(1, count * inner):
        peer_near = lax.rem(near + step // inner % inner, inner)
        peer_part = lax.rem(part + step % inner, inner)
        pl.semaphore_signal(
            barrier,
            inc=1,
            device_id={
                "seq": lax.rem(far + step // (inner * inner), outer) * inner + peer_near,
                "dp": bundle * inner + peer_part,
            },
            device_id_type=MESH,
        )
    for step in range(1, groups):
        pl.semaphore_signal(barrier, inc=1, device_id=group_device(step), device_id_type=MESH)

    def field_copy(phase, head, member, steps):
        peer_far = lax.rem(far + steps[0], outer)
        peer_part = lax.rem(near + steps[1], inner)
        half = order[phase]
        start = pl.multiple_of((peer_far * inner + peer_part) * columns, columns) + head * HDIM
        return remote(
            fields[member].at[half, :, pl.ds(start, HDIM)],
            heads.at[member, half, own_rows, head_columns(head)],
            field_send.at[phase, head, member, *steps],
            field_recv.at[phase, head, member, *steps],
            {"seq": peer_far * inner + part, "dp": bundle * inner + peer_part},
        )

    def each_field(phase, head, member, action):
        for steps in grid_steps:
            when_remote(steps, getattr(field_copy(phase, head, member, steps), action))

    def pass_copy(head, member):
        return remote(
            heads.at[member, 1, :, head_columns(head)],
            heads.at[member, 2, :, head_columns(head)],
            pass_send.at[head, member],
            pass_recv.at[head, member],
            {"cfg": other},
        )

    def rank_copy(way, hop):
        toward, back_by = (1, outer - hop) if way == 0 else (outer - 1, hop)
        block = rank_line.at[lax.rem(far + back_by, outer)]
        return remote(
            block,
            block,
            rank_send.at[way, hop],
            rank_recv.at[way, hop],
            {"seq": lax.rem(far + toward, outer) * inner + near},
        )

    def ranks_leave(way, hop):
        if way == 0:
            return jnp.logical_and(far >= hop, far < outer - 1)
        return jnp.logical_and(far < outer - hop, far > 0)

    def ranks_come(way, hop):
        return far > hop if way == 0 else far < outer - 1 - hop

    def rank_step(hop, action, test):
        for way in range(2):

            @pl.when(test(way, hop))
            def _():
                getattr(rank_copy(way, hop), action)()

    def fan_copy(step):
        peer_part = lax.rem(near + step, inner)
        return remote(
            rank_line,
            ranks.at[:, near],
            fan_send.at[step],
            fan_recv.at[step],
            {"seq": far * inner + part, "dp": bundle * inner + peer_part},
        )

    def facts_copy(step):
        return remote(
            facts,
            work_facts,
            facts_send.at[step],
            facts_recv.at[0],
            {"dp": bundle * inner + lax.rem(part + step, inner)},
        )

    def swap_copy(head):
        return remote(
            weighted.at[head],
            weighted_in.at[head],
            swap_send.at[head],
            swap_recv.at[head],
            {"cfg": other},
        )

    def out_copy(head, steps):
        peer = lax.rem(far + steps[0], outer) * inner + lax.rem(part + steps[1], inner)
        start = pl.multiple_of(work_block * columns, columns) + head * HDIM
        return remote(
            student.at[aligned(peer, tok_here), head_columns(head)],
            tokens_ref.at[:, pl.ds(start, HDIM)],
            out_send.at[head, *steps],
            out_recv.at[head, *steps],
            {"seq": peer, "dp": bundle * inner + near},
        )

    def each_out(head, action):
        for steps in grid_steps:
            when_remote(steps, getattr(out_copy(head, steps), action))

    def cols_copy(step):
        return remote(
            hidden_cols.at[lax.rem(group + step, groups)],
            hidden_all.at[group],
            cols_send.at[step],
            cols_recv.at[step],
            group_device(step),
        )

    def up_copy(steps):
        peer_cfg = lax.rem(cfg + steps[0], 2)
        peer_dp = lax.rem(bundle + steps[1], bundles) * inner + lax.rem(near + steps[2], inner)
        return remote(
            up_parts.at[peer_cfg * dp_count + peer_dp],
            up_in.at[steps],
            up_send.at[steps],
            up_recv.at[steps],
            {"cfg": peer_cfg, "seq": work_block, "dp": peer_dp},
        )

    def each_up(action):
        for steps in up_steps:
            when_remote(steps, getattr(up_copy(steps), action))

    def near_copy(member, far_step, step):
        peer = lax.rem(part + step, inner)
        row = lax.rem(far + far_step, outer)
        return remote(
            back.at[aligned(row * inner + peer, tok_here), head_columns(member)],
            near_in.at[far_step, step, :, head_columns(member)],
            near_send.at[member, far_step, step],
            near_recv.at[member, far_step, step],
            {"dp": bundle * inner + peer},
        )

    def far_copy(member, step):
        return remote(
            far_out.at[step, :, head_columns(member)],
            far_in.at[step, :, head_columns(member)],
            far_send.at[member, step],
            far_recv.at[member, step],
            {"seq": lax.rem(far + step, outer) * inner + near},
        )

    def low_copy(member, step):
        return remote(
            low.at[:, head_columns(member)],
            low_all.at[low_slot(pair, dp), :, head_columns(member)],
            low_send.at[member, step],
            low_recv.at[member, step],
            device_of(lax.rem(pair + step, pairs)),
        )

    def share_copy(member, pair_step, step):
        source = lax.rem(pair - pair_step + pairs, pairs)
        lanes = head_columns(member)
        slot = low_all.at[low_slot(source, dp), :, lanes]
        return remote(
            low.at[:, lanes] if pair_step == 0 else slot,
            slot,
            share_send.at[member, pair_step, step],
            share_recv.at[member, pair_step, step],
            {"dp": lax.rem(dp + step, dp_count)},
        )

    def down_copy(member, step):
        peer = lax.rem(far + step, outer)
        return remote(
            down_out.at[peer, :, head_columns(member)],
            down_in.at[step, :, head_columns(member)],
            down_send.at[member, step],
            down_recv.at[member, step],
            {"seq": peer * inner + near},
        )

    def weighting(half):
        scale = work_facts[1 + half]
        return jnp.where(cfg == 0, scale, 1.0 - scale)

    phases = [(phase, head) for phase in range(2) for head in range(heads_here)]
    sends = [(phase, head, member) for phase, head in phases for member in (1, 0, 2)]
    early_sends, late_sends = sends[:-3], sends[-3:]
    loads[0].start()
    loads[1].start()
    pl.semaphore_wait(barrier, count * inner + groups - 2)
    each_field(*sends[0], "start")
    loads[2].start()

    @pl.when(diagonal)
    def _():
        for load in own_loads:
            load.start()

    def guide_scale(half):
        return 1.0 + 0.5 * guide_ref[half].astype(jnp.float32)

    rank_index = (lax.broadcasted_iota(jnp.int32, (1, ADAPTER_RANK), 1) + 1).astype(jnp.float32)
    time_frac = (time_ref[cfg].astype(jnp.float32) + 0.5) / TSTEPS
    modulation = 1.0 + 0.5 * jnp.cos(
        math.pi * rank_index * time_frac + 0.25 * rank_index * guide_scale(cfg)
    )

    facts[0] = modulation
    for half in range(2):
        facts[1 + half] = jnp.full((1, ADAPTER_RANK), guide_scale(half), jnp.float32)

    @pl.when(diagonal)
    def _():
        work_facts[...] = facts[...]
        for step in range(1, inner):
            facts_copy(step).start()

    loads[0].wait()
    loads[1].wait()
    for member in range(3):
        projected = dot_f32(hidden_own[...], down_own[member]) * modulation
        rank_line[far, :, head_columns(member)] = projected.astype(jnp.bfloat16)
    for hop in range(outer - 1):
        rank_step(hop, "start", ranks_leave)
        each_field(*sends[1 + hop], "start")
        rank_step(hop, "wait_recv", ranks_come)
    for step in range(inner):
        when_remote((step,), fan_copy(step).start)
    for turn in sends[outer:]:
        each_field(*turn, "start")

    @pl.when(diagonal)
    def _():
        ranks[:, near] = rank_line[...]

    @pl.when(off_diagonal)
    def _():
        facts_copy(inner - 1).wait_recv()

    rows_here = hidden_cols.shape[2] // outer
    for block in range(outer * groups):
        target_dp = block % dp_count
        target_near = block // dp_count % inner
        target_far = block // dp_count // inner % outer
        target_pair = block // (dp_count * count) * inner + target_near
        hidden_cols[
            target_dp * pairs + target_pair, :, target_far * rows_here : (target_far + 1) * rows_here
        ] = hidden_own[:, block * rows_here : (block + 1) * rows_here]
    hidden_all[group] = hidden_cols[group]
    for step in range(1, groups):
        cols_copy(step).start()
    loads[2].wait()

    @pl.when(diagonal)
    def _():
        for load in own_loads:
            load.wait()

    far_order = sorted(range(outer), key=lambda step: (step == 0, abs(2 * step - outer)))

    def run_blocks(one_block):
        unroll = 2 if blocks % 2 == 0 else 1

        def some(step, _):
            for offset in range(unroll):
                one_block(step * unroll + offset)
            return 0

        lax.fori_loop(0, blocks // unroll, some, 0)

    def block_rows(step):
        return aligned(step, step_rows)

    def teacher_weights(half, lanes):
        def one_block(step):
            probability = probs_by_key(
                heads[1, half, :, lanes], heads[0, half, block_rows(step), lanes]
            )
            teacher_w[step] = probability.astype(jnp.bfloat16)

        run_blocks(one_block)

    def student_weights(step):
        if student_w is None:
            return student_p[step].astype(jnp.bfloat16)
        return student_w[step]

    def arrived(phase, head, member):
        each_field(phase, head, member, "wait_recv")
        if phase == 0:
            pl.when(cfg == 0)(pass_copy(head, member).start)

    def project(head, member, projected):
        lanes = head_columns(head)
        pl.when(cfg == 1)(pass_copy(head, member).wait_recv)
        low_rank = ranks[:, :, :, head_columns(member)].reshape(length, ADAPTER_RANK)
        frozen = heads[member, 2 * cfg, :, lanes].astype(jnp.float32)
        projected[...] = (frozen + dot_f32(low_rank, up_own[member, :, lanes])).astype(
            jnp.bfloat16
        )

    for head in range(heads_here):
        lanes = head_columns(head)
        arrived(0, head, 1)
        arrived(0, head, 0)
        teacher_weights(other, lanes)
        arrived(0, head, 2)
        value_t[...] = heads[2, other, :, lanes].T

        def one_block(step):
            attended = dot_f32(value_t[...], teacher_w[step]).T.astype(jnp.bfloat16)
            weighted[head, block_rows(step), :] = (
                weighting(other) * attended.astype(jnp.float32)
            ).astype(jnp.bfloat16)

        run_blocks(one_block)
        swap_copy(head).start()

    for step in range(inner):
        when_remote((step,), fan_copy(step).wait_recv)

    def reduce_near(member):
        lanes = head_columns(member)
        for far_step in far_order:
            row = lax.rem(far + far_step, outer)
            total = back[aligned(row * inner + part, tok_here), lanes].astype(jnp.float32)
            for step in range(1, inner):
                near_copy(member, far_step, step).wait_recv()
                total = total + near_in[far_step, step, :, lanes].astype(jnp.float32)
            if far_step > 0:
                far_out[far_step, :, lanes] = total.astype(jnp.bfloat16)
                far_copy(member, far_step).start()
        return total

    def push_back(head, member, gradient):
        lanes = head_columns(member)
        piece = dot_nt(gradient, up_own[member, :, head_columns(head)])
        if head > 0:
            piece = piece + back_sum[:, lanes]
        if head < heads_here - 1:
            back_sum[:, lanes] = piece
            return
        back[:, lanes] = piece.astype(jnp.bfloat16)
        for far_step in far_order:
            for step in range(1, inner):
                near_copy(member, far_step, step).start()

    totals = {}
    for head in range(heads_here):
        lanes = head_columns(head)
        arrived(1, head, 1)
        project(head, 1, s_key)
        key_t[...] = s_key[...].T
        arrived(1, head, 0)
        project(head, 0, s_query)
        teacher_weights(cfg, lanes)

        def one_block(step):
            probability = probs_by_key(s_key[...], s_query[block_rows(step), :])
            student_p[step] = probability
            if student_w is not None:
                student_w[step] = probability.astype(jnp.bfloat16)

        run_blocks(one_block)
        grad_key[...] = jnp.zeros_like(grad_key)
        grad_value[...] = jnp.zeros_like(grad_value)
        if head == heads_here - 1:
            for turn in early_sends:
                each_field(*turn, "wait_send")
        arrived(1, head, 2)
        project(head, 2, s_value)
        value_t[...] = s_value[...].T

        def one_block(step):
            attended = dot_f32(value_t[...], student_weights(step)).T
            student[block_rows(step), lanes] = attended.astype(jnp.bfloat16)

        run_blocks(one_block)
        each_out(head, "start")
        value_t[...] = heads[2, cfg, :, lanes].T

        def one_block(step):
            attended = dot_f32(value_t[...], teacher_w[step]).T.astype(jnp.bfloat16)
            target[block_rows(step), :] = weighting(cfg) * attended.astype(jnp.float32)

        run_blocks(one_block)
        swap_copy(head).wait_recv()

        def one_block(step):
            rows = block_rows(step)
            aim = target[rows, :] + weighted_in[head, rows, :].astype(jnp.float32)
            error = student[rows, lanes].astype(jnp.float32) - aim
            upstream[rows, :] = (error * out_scale).astype(jnp.bfloat16)
            grad_value[...] += dot_f32(student_weights(step), upstream[rows, :])

        run_blocks(one_block)
        last = head == heads_here - 1
        gradients = {2: grad_value[...].astype(jnp.bfloat16)}
        push_back(head, 2, gradients[2])

        def one_block(step):
            rows = block_rows(step)
            probability = student_p[step]
            prob_grad = dot_nt(s_value[...], upstream[rows, :])
            center = jnp.sum(probability * prob_grad, axis=0, keepdims=True)
            score_grad = (probability * (prob_grad - center)).astype(jnp.bfloat16)
            grad_key[...] += dot_f32(score_grad, s_query[rows, :])
            grad_query[rows, :] = (dot_f32(key_t[...], score_grad).T * FACTOR).astype(
                jnp.bfloat16
            )

        run_blocks(one_block)
        if last:
            totals[2] = reduce_near(2)
        gradients[1] = (grad_key[...] * FACTOR).astype(jnp.bfloat16)
        push_back(head, 1, gradients[1])
        gradients[0] = grad_query[...]
        push_back(head, 0, gradients[0])
        if last:
            totals[1] = reduce_near(1)
            totals[0] = reduce_near(0)
        for member, gradient in gradients.items():
            low_rank = ranks[:, :, :, head_columns(member)].reshape(length, ADAPTER_RANK)
            piece = dot_tn(low_rank, gradient).astype(jnp.bfloat16)
            up_parts[:, member, :, lanes] = piece.reshape(up_groups, -1, HDIM)

    each_up("start")
    own_store = pltpu.make_async_copy(
        student.at[own_rows, :], tokens_ref.at[:, aligned(me, columns)], local_sem.at[6]
    )

    @pl.when(diagonal)
    def _():
        own_store.start()
        up_in[0, 0, 0] = up_parts[cfg * dp_count + dp]

    down_rows = hidden_t.shape[0] // outer

    def gather_columns():
        for step in range(1, groups):
            cols_copy(step).wait_recv()
        hidden_t[...] = hidden_all[...].reshape(groups * tok_here, -1).T

    def reduce_far(member, total):
        lanes = head_columns(member)
        for step in range(1, outer):
            far_copy(member, step).wait_recv()
            total = total + far_in[step, :, lanes].astype(jnp.float32)
        low_grad = (total * work_facts[0]).astype(jnp.bfloat16)
        low[:, lanes] = low_grad
        low_all[low_slot(pair, dp), :, lanes] = low_grad
        for step in range(1, pairs):
            low_copy(member, step).start()
        for step in range(1, dp_count):
            share_copy(member, 0, step).start()

    def spread(member):
        for pair_step in range(1, pairs):
            low_copy(member, pair_step).wait_recv()
            for step in range(1, dp_count):
                share_copy(member, pair_step, step).start()

    def contract(member):
        lanes = head_columns(member)
        for pair_step in range(pairs):
            for step in range(1, dp_count):
                share_copy(member, pair_step, step).wait_recv()
        gathered_low = low_all[:, :, lanes].reshape(groups * tok_here, ADAPTER_RANK)
        partial = dot_f32(hidden_t[...], gathered_low).astype(jnp.bfloat16)
        for peer in range(outer):
            down_out[peer, :, lanes] = partial[peer * down_rows : (peer + 1) * down_rows, :]
        for step in range(1, outer):
            down_copy(member, step).start()

    for turn in late_sends:
        each_field(*turn, "wait_send")
    for head in range(heads_here):
        swap_copy(head).wait_send()

        @pl.when(cfg == 0)
        def _():
            for member in range(3):
                pass_copy(head, member).wait_send()

        if head < heads_here - 1:
            each_out(head, "wait")
    for hop in range(outer - 1):
        rank_step(hop, "wait_send", ranks_leave)
    for step in range(inner):
        when_remote((step,), fan_copy(step).wait_send)

    reduce_far(2, totals[2])
    gather_columns()
    for step in range(1, groups):
        cols_copy(step).wait_send()
    for member in range(3):
        for far_step in range(outer):
            for step in range(1, inner):
                near_copy(member, far_step, step).wait_send()
    reduce_far(1, totals[1])
    spread(2)
    contract(2)
    reduce_far(0, totals[0])
    for member in range(3):
        for step in range(1, outer):
            far_copy(member, step).wait_send()
    spread(1)
    contract(1)
    spread(0)
    contract(0)

    each_up("wait_recv")
    up_total = up_in[up_steps[0]].astype(jnp.float32)
    for steps in up_steps[1:]:
        up_total = up_total + up_in[steps].astype(jnp.float32)
    grad_up_ref[...] = up_total

    for member in (2, 1, 0):
        lanes = head_columns(member)
        down_total = down_out[far, :, lanes].astype(jnp.float32)
        for step in range(1, outer):
            down_copy(member, step).wait_recv()
            down_total = down_total + down_in[step, :, lanes].astype(jnp.float32)
        grad_down_ref[member] = down_total

    @pl.when(diagonal)
    def _():
        own_store.wait()
        for step in range(1, inner):
            facts_copy(step).wait_send()

    each_out(heads_here - 1, "wait")
    each_up("wait_send")
    for member in range(3):
        for pair_step in range(pairs):
            if pair_step > 0:
                low_copy(member, pair_step).wait_send()
            for step in range(1, dp_count):
                share_copy(member, pair_step, step).wait_send()
        for step in range(1, outer):
            down_copy(member, step).wait_send()


def with_gaps(kernel, scratch, skipped):
    def filled(*refs):
        held = iter(refs[skipped:])
        kernel(*refs[:skipped], *[None if item is None else next(held) for item in scratch])

    return filled


def run_step(sizes, guide, time_index, fields, hidden, down, up):
    count, inner, dp_count = sizes
    outer = count // inner
    pairs = 2 * inner
    groups = pairs * dp_count
    up_groups = 2 * dp_count
    tok_here, width = fields[0].shape[1:]
    model_width = hidden.shape[1]
    length, columns = tok_here * count, width // count
    heads_here = columns // HDIM
    step_rows = min(BLOCK, BLOCK_AREA // length, length)
    rank_cols = 3 * ADAPTER_RANK
    group_cols = model_width // groups
    down_rows = group_cols // outer
    up_rows = ADAPTER_RANK // up_groups
    any_spec = pl.BlockSpec(memory_space=pl.ANY)
    vmem_spec = pl.BlockSpec(memory_space=pltpu.VMEM)
    smem_spec = pl.BlockSpec(memory_space=pltpu.SMEM)

    def bf16(*shape):
        return pltpu.VMEM(shape, jnp.bfloat16)

    def f32(*shape):
        return pltpu.VMEM(shape, jnp.float32)

    def sems(*shape):
        return [pltpu.SemaphoreType.DMA(shape)] * 2

    total_rows = 2 * dp_count * length
    keep_weights = 8 * length * length <= KEPT_BYTES
    scratch = [
        bf16(3, 3, length, columns),
        bf16(tok_here, model_width),
        bf16(groups, tok_here, group_cols),
        bf16(groups, tok_here, group_cols),
        bf16(group_cols, groups * tok_here),
        bf16(3, model_width, ADAPTER_RANK),
        bf16(3, ADAPTER_RANK, columns),
        bf16(outer, tok_here, rank_cols),
        bf16(outer, inner, tok_here, rank_cols),
        f32(3, 1, ADAPTER_RANK),
        f32(3, 1, ADAPTER_RANK),
        bf16(heads_here, length, HDIM),
        bf16(heads_here, length, HDIM),
        f32(length, HDIM),
        bf16(length, HDIM),
        bf16(length, HDIM),
        bf16(length, HDIM),
        bf16(HDIM, length),
        bf16(HDIM, length),
        bf16(length, HDIM),
        bf16(length, HDIM),
        f32(length, HDIM),
        f32(length, HDIM),
        bf16(length // step_rows, length, step_rows),
        bf16(length // step_rows, length, step_rows) if keep_weights else None,
        f32(length // step_rows, length, step_rows),
        f32(length, rank_cols) if heads_here > 1 else None,
        bf16(length, rank_cols),
        bf16(outer, inner, tok_here, rank_cols),
        bf16(outer, tok_here, rank_cols),
        bf16(outer, tok_here, rank_cols),
        bf16(length, columns),
        bf16(up_groups, 3, up_rows, columns),
        bf16(2, dp_count // inner, inner, 3, up_rows, columns),
        bf16(tok_here, rank_cols),
        bf16(groups, tok_here, rank_cols),
        bf16(outer, down_rows, rank_cols),
        bf16(outer, down_rows, rank_cols),
        *sems(2, heads_here, 3, outer, inner),
        *sems(heads_here, 3),
        *sems(2, outer),
        *sems(inner),
        *sems(heads_here),
        *sems(heads_here, outer, inner),
        *sems(groups),
        *sems(2, dp_count // inner, inner),
        *sems(3, outer, inner),
        *sems(3, outer),
        *sems(3, pairs),
        *sems(3, pairs, dp_count),
        *sems(3, outer),
        *sems(inner),
        pltpu.SemaphoreType.DMA((7,)),
    ]
    return pl.pallas_call(
        with_gaps(functools.partial(step_kernel, sizes, 1.0 / math.sqrt(total_rows)), scratch, 11),
        out_shape=(
            jax.ShapeDtypeStruct((tok_here, width), jnp.bfloat16),
            jax.ShapeDtypeStruct((3, down_rows, ADAPTER_RANK), jnp.float32),
            jax.ShapeDtypeStruct((3, up_rows, columns), jnp.float32),
        ),
        in_specs=[smem_spec] * 2 + [any_spec] * 6,
        out_specs=(any_spec, vmem_spec, vmem_spec),
        scratch_shapes=[item for item in scratch if item is not None],
        compiler_params=pltpu.CompilerParams(
            collective_id=0, has_side_effects=True, vmem_limit_bytes=VMEM_LIMIT
        ),
        name="step",
    )(guide, time_index, *fields, hidden, down, up)


def emit_kernel(*refs):
    count = (len(refs) - 2) // 3
    held = refs[2 * count : 3 * count]
    load_sem, store_sem = refs[3 * count :]
    loads = [
        pltpu.make_async_copy(refs[item], held[item], load_sem.at[item]) for item in range(count)
    ]
    stores = [
        pltpu.make_async_copy(held[item], refs[count + item], store_sem.at[item])
        for item in range(count)
    ]
    for load in loads:
        load.start()
    for load, store in zip(loads, stores):
        load.wait()
        store.start()
    for store in stores:
        store.wait()


def emit(arrays):
    any_specs = (pl.BlockSpec(memory_space=pl.ANY),) * len(arrays)
    return pl.pallas_call(
        emit_kernel,
        out_shape=tuple(jax.ShapeDtypeStruct(array.shape, array.dtype) for array in arrays),
        in_specs=any_specs,
        out_specs=any_specs,
        scratch_shapes=[pltpu.VMEM(array.shape, array.dtype) for array in arrays]
        + [pltpu.SemaphoreType.DMA((len(arrays),))] * 2,
        compiler_params=pltpu.CompilerParams(vmem_limit_bytes=VMEM_LIMIT),
        name="emit",
    )(*arrays)


def body(
    teacher_query,
    teacher_key,
    teacher_value,
    hidden,
    adapter_down_weight,
    adapter_up_weight,
    guidance_index,
    timestep_index,
):
    seq_count = lax.axis_size("seq")
    dp_count = lax.axis_size("dp")
    outputs = run_step(
        (seq_count, inner_size(seq_count, dp_count), dp_count),
        guidance_index[:, 0],
        timestep_index[:, 0],
        (teacher_query[0, :, 0], teacher_key[0, :, 0], teacher_value[0, :, 0]),
        hidden[0, 0],
        adapter_down_weight,
        adapter_up_weight,
    )
    student_tokens, grad_down, grad_up = emit(outputs)
    return (student_tokens[None, None], grad_down, grad_up)


def solution(mesh):
    placed = (
        P("cfg", None, "dp", "seq", None),
        P("cfg", None, "dp", "seq", None),
        P("cfg", None, "dp", "seq", None),
        P("cfg", "dp", "seq", None),
        P(),
        P(),
        P(None, "dp"),
        P(None, "dp"),
    )
    return jax.shard_map(
        body,
        mesh=mesh,
        in_specs=placed,
        out_specs=(
            P("cfg", "dp", "seq", None),
            P(None, ("cfg", "seq", "dp"), None),
            P(None, ("cfg", "dp"), "seq"),
        ),
        check_vma=False,
    )
```

```python
import functools
import math

import jax
import jax.numpy as jnp
from jax import lax
from jax.experimental import pallas as pl
from jax.experimental.pallas import tpu as pltpu
from jax.sharding import PartitionSpec as P

HDIM = 128
ADAPTER_RANK = 128
TSTEPS = 1000
FACTOR = HDIM ** (-0.5)
FACTOR_BASE2 = FACTOR * math.log2(math.e)
VMEM_LIMIT = 63 * 1024 * 1024
BLOCK = 512
BLOCK_AREA = BLOCK * 1024
KEPT_BYTES = 16 * 1024 * 1024
MESH = pl.DeviceIdType.MESH

NT = (((1,), (1,)), ((), ()))
TN = (((0,), (0,)), ((), ()))


def dot_f32(left, right):
    return jnp.dot(left, right, preferred_element_type=jnp.float32)


def dot_nt(left, right):
    return lax.dot_general(left, right, NT, preferred_element_type=jnp.float32)


def dot_tn(left, right):
    return lax.dot_general(left, right, TN, preferred_element_type=jnp.float32)


def inner_size(count, dp_count):
    return max(
        size
        for size in range(1, count + 1)
        if count % size == 0 and dp_count % size == 0 and size * size <= count
    )


def aligned(index, size):
    return pl.ds(pl.multiple_of(index * size, size), size)


def probs_by_key(key_head, query_block):
    scores = dot_nt(key_head, query_block)
    highest = jnp.max(scores, axis=0, keepdims=True)
    raised = jnp.exp2((scores - highest) * FACTOR_BASE2)
    return raised * (1.0 / jnp.sum(raised, axis=0, keepdims=True))


def step_kernel(
    sizes,
    out_scale,
    guide_ref,
    time_ref,
    query_ref,
    key_ref,
    value_ref,
    hidden_ref,
    down_ref,
    up_ref,
    tokens_ref,
    grad_down_ref,
    grad_up_ref,
    heads,
    hidden_own,
    hidden_cols,
    hidden_all,
    hidden_t,
    down_own,
    up_own,
    rank_line,
    ranks,
    facts,
    work_facts,
    weighted,
    weighted_in,
    target,
    s_query,
    s_key,
    s_value,
    key_t,
    value_t,
    upstream,
    grad_query,
    grad_key,
    grad_value,
    teacher_w,
    student_w,
    student_p,
    back_sum,
    back,
    near_in,
    far_out,
    far_in,
    student,
    up_parts,
    up_in,
    low,
    low_all,
    down_out,
    down_in,
    field_send,
    field_recv,
    pass_send,
    pass_recv,
    rank_send,
    rank_recv,
    fan_send,
    fan_recv,
    swap_send,
    swap_recv,
    out_send,
    out_recv,
    cols_send,
    cols_recv,
    up_send,
    up_recv,
    near_send,
    near_recv,
    far_send,
    far_recv,
    low_send,
    low_recv,
    share_send,
    share_recv,
    down_send,
    down_recv,
    facts_send,
    facts_recv,
    local_sem,
):
    count, inner, dp_count = sizes
    outer = count // inner
    pairs = 2 * inner
    groups = pairs * dp_count
    up_groups = 2 * dp_count
    fields = (query_ref, key_ref, value_ref)
    tok_here = query_ref.shape[1]
    length = tok_here * count
    columns = student.shape[1]
    heads_here = columns // HDIM
    step_rows = min(BLOCK, BLOCK_AREA // length, length)
    blocks = length // step_rows

    me = lax.axis_index("seq")
    cfg = lax.axis_index("cfg")
    dp = lax.axis_index("dp")
    other = 1 - cfg
    far = me // inner
    near = lax.rem(me, inner)
    part = lax.rem(dp, inner)
    bundle = dp // inner
    bundles = dp_count // inner
    diagonal = near == part
    off_diagonal = near != part
    pair = cfg * inner + near
    group = dp * pairs + pair
    work_block = far * inner + part
    own_rows = aligned(me, tok_here)
    far_order = sorted(range(outer), key=lambda step: (step == 0, abs(2 * step - outer)))
    grid_steps = [(far_step, near_step) for far_step in far_order for near_step in range(inner)]
    up_steps = [
        (cfg_step, bundle_step, near_step)
        for cfg_step in range(2)
        for bundle_step in range(bundles)
        for near_step in range(inner)
    ]
    order = (other, cfg)

    def head_columns(head):
        return slice(head * HDIM, (head + 1) * HDIM)

    def when_remote(steps, action):
        if any(steps):
            action()
        else:
            pl.when(off_diagonal)(action)

    def low_slot(pair_index, dp_index):
        return (
            dp_index // inner * inner + lax.rem(pair_index, inner)
        ) * pairs + pair_index // inner * inner + lax.rem(dp_index, inner)

    def device_of(pair_index):
        return {"cfg": pair_index // inner, "seq": far * inner + lax.rem(pair_index, inner)}

    def group_device(step):
        peer = lax.rem(group + step, groups)
        return {**device_of(lax.rem(peer, pairs)), "dp": peer // pairs}

    def remote(src, dst, send, recv, device):
        return pltpu.make_async_remote_copy(
            src_ref=src,
            dst_ref=dst,
            send_sem=send,
            recv_sem=recv,
            device_id=device,
            device_id_type=MESH,
        )

    loads = [
        pltpu.make_async_copy(hidden_ref, hidden_own, local_sem.at[0]),
        pltpu.make_async_copy(down_ref, down_own, local_sem.at[1]),
        pltpu.make_async_copy(
            up_ref.at[:, :, aligned(work_block, columns)], up_own, local_sem.at[2]
        ),
    ]
    own_loads = [
        pltpu.make_async_copy(
            fields[member].at[:, :, aligned(me, columns)],
            heads.at[member, 0:2, own_rows, :],
            local_sem.at[3 + member],
        )
        for member in range(3)
    ]
    barrier = pltpu.get_barrier_semaphore()
    for step in range(1, count * inner):
        peer_near = lax.rem(near + step // inner % inner, inner)
        peer_part = lax.rem(part + step % inner, inner)
        pl.semaphore_signal(
            barrier,
            inc=1,
            device_id={
                "seq": lax.rem(far + step // (inner * inner), outer) * inner + peer_near,
                "dp": bundle * inner + peer_part,
            },
            device_id_type=MESH,
        )
    for step in range(1, groups):
        pl.semaphore_signal(barrier, inc=1, device_id=group_device(step), device_id_type=MESH)

    def field_copy(phase, head, member, steps):
        peer_far = lax.rem(far + steps[0], outer)
        peer_part = lax.rem(near + steps[1], inner)
        half = order[phase]
        start = pl.multiple_of((peer_far * inner + peer_part) * columns, columns) + head * HDIM
        return remote(
            fields[member].at[half, :, pl.ds(start, HDIM)],
            heads.at[member, half, own_rows, head_columns(head)],
            field_send.at[phase, head, member, *steps],
            field_recv.at[phase, head, member, *steps],
            {"seq": peer_far * inner + part, "dp": bundle * inner + peer_part},
        )

    def each_field(phase, head, member, action):
        for steps in grid_steps:
            when_remote(steps, getattr(field_copy(phase, head, member, steps), action))

    def pass_copy(head, member):
        return remote(
            heads.at[member, 1, :, head_columns(head)],
            heads.at[member, 2, :, head_columns(head)],
            pass_send.at[head, member],
            pass_recv.at[head, member],
            {"cfg": other},
        )

    def rank_copy(way, hop):
        toward, back_by = (1, outer - hop) if way == 0 else (outer - 1, hop)
        block = rank_line.at[lax.rem(far + back_by, outer)]
        return remote(
            block,
            block,
            rank_send.at[way, hop],
            rank_recv.at[way, hop],
            {"seq": lax.rem(far + toward, outer) * inner + near},
        )

    def ranks_leave(way, hop):
        if way == 0:
            return jnp.logical_and(far >= hop, far < outer - 1)
        return jnp.logical_and(far < outer - hop, far > 0)

    def ranks_come(way, hop):
        return far > hop if way == 0 else far < outer - 1 - hop

    def rank_step(hop, action, test):
        for way in range(2):

            @pl.when(test(way, hop))
            def _():
                getattr(rank_copy(way, hop), action)()

    def fan_copy(step):
        peer_part = lax.rem(near + step, inner)
        return remote(
            rank_line,
            ranks.at[:, near],
            fan_send.at[step],
            fan_recv.at[step],
            {"seq": far * inner + part, "dp": bundle * inner + peer_part},
        )

    def facts_copy(step):
        return remote(
            facts,
            work_facts,
            facts_send.at[step],
            facts_recv.at[0],
            {"dp": bundle * inner + lax.rem(part + step, inner)},
        )

    def swap_copy(head):
        return remote(
            weighted.at[head],
            weighted_in.at[head],
            swap_send.at[head],
            swap_recv.at[head],
            {"cfg": other},
        )

    def out_copy(head, steps):
        peer = lax.rem(far + steps[0], outer) * inner + lax.rem(part + steps[1], inner)
        start = pl.multiple_of(work_block * columns, columns) + head * HDIM
        return remote(
            student.at[aligned(peer, tok_here), head_columns(head)],
            tokens_ref.at[:, pl.ds(start, HDIM)],
            out_send.at[head, *steps],
            out_recv.at[head, *steps],
            {"seq": peer, "dp": bundle * inner + near},
        )

    def each_out(head, action):
        for steps in grid_steps:
            when_remote(steps, getattr(out_copy(head, steps), action))

    def cols_copy(step):
        return remote(
            hidden_cols.at[lax.rem(group + step, groups)],
            hidden_all.at[group],
            cols_send.at[step],
            cols_recv.at[step],
            group_device(step),
        )

    def up_copy(steps):
        peer_cfg = lax.rem(cfg + steps[0], 2)
        peer_dp = lax.rem(bundle + steps[1], bundles) * inner + lax.rem(near + steps[2], inner)
        return remote(
            up_parts.at[peer_cfg * dp_count + peer_dp],
            up_in.at[steps],
            up_send.at[steps],
            up_recv.at[steps],
            {"cfg": peer_cfg, "seq": work_block, "dp": peer_dp},
        )

    def each_up(action):
        for steps in up_steps:
            when_remote(steps, getattr(up_copy(steps), action))

    def near_copy(member, far_step, step):
        peer = lax.rem(part + step, inner)
        row = lax.rem(far + far_step, outer)
        return remote(
            back.at[aligned(row * inner + peer, tok_here), head_columns(member)],
            near_in.at[far_step, step, :, head_columns(member)],
            near_send.at[member, far_step, step],
            near_recv.at[member, far_step, step],
            {"dp": bundle * inner + peer},
        )

    def far_copy(member, step):
        return remote(
            far_out.at[step, :, head_columns(member)],
            far_in.at[step, :, head_columns(member)],
            far_send.at[member, step],
            far_recv.at[member, step],
            {"seq": lax.rem(far + step, outer) * inner + near},
        )

    def low_copy(member, step):
        return remote(
            low.at[:, head_columns(member)],
            low_all.at[low_slot(pair, dp), :, head_columns(member)],
            low_send.at[member, step],
            low_recv.at[member, step],
            device_of(lax.rem(pair + step, pairs)),
        )

    def share_copy(member, pair_step, step):
        source = lax.rem(pair - pair_step + pairs, pairs)
        lanes = head_columns(member)
        slot = low_all.at[low_slot(source, dp), :, lanes]
        return remote(
            low.at[:, lanes] if pair_step == 0 else slot,
            slot,
            share_send.at[member, pair_step, step],
            share_recv.at[member, pair_step, step],
            {"dp": lax.rem(dp + step, dp_count)},
        )

    def down_copy(member, step):
        peer = lax.rem(far + step, outer)
        return remote(
            down_out.at[peer, :, head_columns(member)],
            down_in.at[step, :, head_columns(member)],
            down_send.at[member, step],
            down_recv.at[member, step],
            {"seq": peer * inner + near},
        )

    def weighting(half):
        scale = work_facts[1 + half]
        return jnp.where(cfg == 0, scale, 1.0 - scale)

    phases = [(phase, head) for phase in range(2) for head in range(heads_here)]
    sends = [(phase, head, member) for phase, head in phases for member in (1, 0, 2)]
    early_sends, late_sends = sends[:-3], sends[-3:]
    loads[0].start()
    loads[1].start()
    pl.semaphore_wait(barrier, count * inner + groups - 2)
    each_field(*sends[0], "start")
    loads[2].start()

    @pl.when(diagonal)
    def _():
        for load in own_loads:
            load.start()

    def guide_scale(half):
        return 1.0 + 0.5 * guide_ref[half].astype(jnp.float32)

    rank_index = (lax.broadcasted_iota(jnp.int32, (1, ADAPTER_RANK), 1) + 1).astype(jnp.float32)
    time_frac = (time_ref[cfg].astype(jnp.float32) + 0.5) / TSTEPS
    modulation = 1.0 + 0.5 * jnp.cos(
        math.pi * rank_index * time_frac + 0.25 * rank_index * guide_scale(cfg)
    )

    facts[0] = modulation
    for half in range(2):
        facts[1 + half] = jnp.full((1, ADAPTER_RANK), guide_scale(half), jnp.float32)

    @pl.when(diagonal)
    def _():
        work_facts[...] = facts[...]
        for step in range(1, inner):
            facts_copy(step).start()

    loads[0].wait()
    loads[1].wait()
    for member in range(3):
        projected = dot_f32(hidden_own[...], down_own[member]) * modulation
        rank_line[far, :, head_columns(member)] = projected.astype(jnp.bfloat16)
    for hop in range(outer - 1):
        rank_step(hop, "start", ranks_leave)
        each_field(*sends[1 + hop], "start")
        rank_step(hop, "wait_recv", ranks_come)
    for step in range(inner):
        when_remote((step,), fan_copy(step).start)
    for turn in sends[outer:]:
        each_field(*turn, "start")

    @pl.when(diagonal)
    def _():
        ranks[:, near] = rank_line[...]

    @pl.when(off_diagonal)
    def _():
        facts_copy(inner - 1).wait_recv()

    rows_here = hidden_cols.shape[2] // outer
    for block in range(outer * groups):
        target_dp = block % dp_count
        target_near = block // dp_count % inner
        target_far = block // dp_count // inner % outer
        target_pair = block // (dp_count * count) * inner + target_near
        hidden_cols[
            target_dp * pairs + target_pair, :, target_far * rows_here : (target_far + 1) * rows_here
        ] = hidden_own[:, block * rows_here : (block + 1) * rows_here]
    hidden_all[group] = hidden_cols[group]
    for step in range(1, groups):
        cols_copy(step).start()
    loads[2].wait()

    @pl.when(diagonal)
    def _():
        for load in own_loads:
            load.wait()


    def run_blocks(one_block):
        unroll = 2 if blocks % 2 == 0 else 1

        def some(step, _):
            for offset in range(unroll):
                one_block(step * unroll + offset)
            return 0

        lax.fori_loop(0, blocks // unroll, some, 0)

    def block_rows(step):
        return aligned(step, step_rows)

    def teacher_weights(half, lanes):
        def one_block(step):
            probability = probs_by_key(
                heads[1, half, :, lanes], heads[0, half, block_rows(step), lanes]
            )
            teacher_w[step] = probability.astype(jnp.bfloat16)

        run_blocks(one_block)

    def student_weights(step):
        if student_w is None:
            return student_p[step].astype(jnp.bfloat16)
        return student_w[step]

    def arrived(phase, head, member):
        each_field(phase, head, member, "wait_recv")
        if phase == 0:
            pl.when(cfg == 0)(pass_copy(head, member).start)

    def project(head, member, projected):
        lanes = head_columns(head)
        pl.when(cfg == 1)(pass_copy(head, member).wait_recv)
        low_rank = ranks[:, :, :, head_columns(member)].reshape(length, ADAPTER_RANK)
        frozen = heads[member, 2 * cfg, :, lanes].astype(jnp.float32)
        projected[...] = (frozen + dot_f32(low_rank, up_own[member, :, lanes])).astype(
            jnp.bfloat16
        )

    for head in range(heads_here):
        lanes = head_columns(head)
        arrived(0, head, 1)
        arrived(0, head, 0)
        teacher_weights(other, lanes)
        arrived(0, head, 2)
        value_t[...] = heads[2, other, :, lanes].T

        def one_block(step):
            attended = dot_f32(value_t[...], teacher_w[step]).T.astype(jnp.bfloat16)
            weighted[head, block_rows(step), :] = (
                weighting(other) * attended.astype(jnp.float32)
            ).astype(jnp.bfloat16)

        run_blocks(one_block)
        swap_copy(head).start()

    for step in range(inner):
        when_remote((step,), fan_copy(step).wait_recv)

    def reduce_near(member):
        lanes = head_columns(member)
        for far_step in far_order:
            row = lax.rem(far + far_step, outer)
            total = back[aligned(row * inner + part, tok_here), lanes].astype(jnp.float32)
            for step in range(1, inner):
                near_copy(member, far_step, step).wait_recv()
                total = total + near_in[far_step, step, :, lanes].astype(jnp.float32)
            if far_step > 0:
                far_out[far_step, :, lanes] = total.astype(jnp.bfloat16)
                far_copy(member, far_step).start()
        return total

    def push_back(head, member, gradient):
        lanes = head_columns(member)
        piece = dot_nt(gradient, up_own[member, :, head_columns(head)])
        if head > 0:
            piece = piece + back_sum[:, lanes]
        if head < heads_here - 1:
            back_sum[:, lanes] = piece
            return
        back[:, lanes] = piece.astype(jnp.bfloat16)
        for far_step in far_order:
            for step in range(1, inner):
                near_copy(member, far_step, step).start()

    totals = {}
    for head in range(heads_here):
        lanes = head_columns(head)
        arrived(1, head, 1)
        project(head, 1, s_key)
        key_t[...] = s_key[...].T
        arrived(1, head, 0)
        project(head, 0, s_query)
        teacher_weights(cfg, lanes)

        def one_block(step):
            probability = probs_by_key(s_key[...], s_query[block_rows(step), :])
            student_p[step] = probability
            if student_w is not None:
                student_w[step] = probability.astype(jnp.bfloat16)

        run_blocks(one_block)
        grad_key[...] = jnp.zeros_like(grad_key)
        grad_value[...] = jnp.zeros_like(grad_value)
        if head == heads_here - 1:
            for turn in early_sends:
                each_field(*turn, "wait_send")
        arrived(1, head, 2)
        project(head, 2, s_value)
        value_t[...] = s_value[...].T

        def one_block(step):
            attended = dot_f32(value_t[...], student_weights(step)).T
            student[block_rows(step), lanes] = attended.astype(jnp.bfloat16)

        run_blocks(one_block)
        each_out(head, "start")
        value_t[...] = heads[2, cfg, :, lanes].T

        def one_block(step):
            attended = dot_f32(value_t[...], teacher_w[step]).T.astype(jnp.bfloat16)
            target[block_rows(step), :] = weighting(cfg) * attended.astype(jnp.float32)

        run_blocks(one_block)
        swap_copy(head).wait_recv()

        def one_block(step):
            rows = block_rows(step)
            aim = target[rows, :] + weighted_in[head, rows, :].astype(jnp.float32)
            error = student[rows, lanes].astype(jnp.float32) - aim
            upstream[rows, :] = (error * out_scale).astype(jnp.bfloat16)
            grad_value[...] += dot_f32(student_weights(step), upstream[rows, :])

        run_blocks(one_block)
        last = head == heads_here - 1
        gradients = {2: grad_value[...].astype(jnp.bfloat16)}
        push_back(head, 2, gradients[2])

        def one_block(step):
            rows = block_rows(step)
            probability = student_p[step]
            prob_grad = dot_nt(s_value[...], upstream[rows, :])
            center = jnp.sum(probability * prob_grad, axis=0, keepdims=True)
            score_grad = (probability * (prob_grad - center)).astype(jnp.bfloat16)
            grad_key[...] += dot_f32(score_grad, s_query[rows, :])
            grad_query[rows, :] = (dot_f32(key_t[...], score_grad).T * FACTOR).astype(
                jnp.bfloat16
            )

        run_blocks(one_block)
        if last:
            totals[2] = reduce_near(2)
        gradients[1] = (grad_key[...] * FACTOR).astype(jnp.bfloat16)
        push_back(head, 1, gradients[1])
        gradients[0] = grad_query[...]
        push_back(head, 0, gradients[0])
        if last:
            totals[1] = reduce_near(1)
            totals[0] = reduce_near(0)
        for member, gradient in gradients.items():
            low_rank = ranks[:, :, :, head_columns(member)].reshape(length, ADAPTER_RANK)
            piece = dot_tn(low_rank, gradient).astype(jnp.bfloat16)
            up_parts[:, member, :, lanes] = piece.reshape(up_groups, -1, HDIM)

    own_store = pltpu.make_async_copy(
        student.at[own_rows, :], tokens_ref.at[:, aligned(me, columns)], local_sem.at[6]
    )

    @pl.when(diagonal)
    def _():
        own_store.start()
        up_in[0, 0, 0] = up_parts[cfg * dp_count + dp]

    down_rows = hidden_t.shape[0] // outer

    def gather_columns():
        for step in range(1, groups):
            cols_copy(step).wait_recv()
        hidden_t[...] = hidden_all[...].reshape(groups * tok_here, -1).T

    def reduce_far(member, total):
        lanes = head_columns(member)
        for step in range(1, outer):
            far_copy(member, step).wait_recv()
            total = total + far_in[step, :, lanes].astype(jnp.float32)
        low_grad = (total * work_facts[0]).astype(jnp.bfloat16)
        low[:, lanes] = low_grad
        low_all[low_slot(pair, dp), :, lanes] = low_grad
        for step in range(1, pairs):
            low_copy(member, step).start()
        for step in range(1, dp_count):
            share_copy(member, 0, step).start()

    def spread(member):
        for pair_step in range(1, pairs):
            low_copy(member, pair_step).wait_recv()
            for step in range(1, dp_count):
                share_copy(member, pair_step, step).start()

    def contract(member):
        lanes = head_columns(member)
        for pair_step in range(pairs):
            for step in range(1, dp_count):
                share_copy(member, pair_step, step).wait_recv()
        gathered_low = low_all[:, :, lanes].reshape(groups * tok_here, ADAPTER_RANK)
        partial = dot_f32(hidden_t[...], gathered_low).astype(jnp.bfloat16)
        for peer in range(outer):
            down_out[peer, :, lanes] = partial[peer * down_rows : (peer + 1) * down_rows, :]
        for step in range(1, outer):
            down_copy(member, step).start()

    for turn in late_sends:
        each_field(*turn, "wait_send")
    for head in range(heads_here):
        swap_copy(head).wait_send()

        @pl.when(cfg == 0)
        def _():
            for member in range(3):
                pass_copy(head, member).wait_send()

        if head < heads_here - 1:
            each_out(head, "wait")
    for hop in range(outer - 1):
        rank_step(hop, "wait_send", ranks_leave)
    for step in range(inner):
        when_remote((step,), fan_copy(step).wait_send)

    reduce_far(2, totals[2])
    gather_columns()
    for step in range(1, groups):
        cols_copy(step).wait_send()
    for member in range(3):
        for far_step in range(outer):
            for step in range(1, inner):
                near_copy(member, far_step, step).wait_send()
    reduce_far(1, totals[1])
    each_up("start")
    spread(2)
    contract(2)
    reduce_far(0, totals[0])
    for member in range(3):
        for step in range(1, outer):
            far_copy(member, step).wait_send()
    spread(1)
    contract(1)
    spread(0)
    contract(0)

    each_up("wait_recv")
    up_total = up_in[up_steps[0]].astype(jnp.float32)
    for steps in up_steps[1:]:
        up_total = up_total + up_in[steps].astype(jnp.float32)
    grad_up_ref[...] = up_total

    for member in (2, 1, 0):
        lanes = head_columns(member)
        down_total = down_out[far, :, lanes].astype(jnp.float32)
        for step in range(1, outer):
            down_copy(member, step).wait_recv()
            down_total = down_total + down_in[step, :, lanes].astype(jnp.float32)
        grad_down_ref[member] = down_total

    @pl.when(diagonal)
    def _():
        own_store.wait()
        for step in range(1, inner):
            facts_copy(step).wait_send()

    each_out(heads_here - 1, "wait")
    each_up("wait_send")
    for member in range(3):
        for pair_step in range(pairs):
            if pair_step > 0:
                low_copy(member, pair_step).wait_send()
            for step in range(1, dp_count):
                share_copy(member, pair_step, step).wait_send()
        for step in range(1, outer):
            down_copy(member, step).wait_send()


def with_gaps(kernel, scratch, skipped):
    def filled(*refs):
        held = iter(refs[skipped:])
        kernel(*refs[:skipped], *[None if item is None else next(held) for item in scratch])

    return filled


def run_step(sizes, guide, time_index, fields, hidden, down, up):
    count, inner, dp_count = sizes
    outer = count // inner
    pairs = 2 * inner
    groups = pairs * dp_count
    up_groups = 2 * dp_count
    tok_here, width = fields[0].shape[1:]
    model_width = hidden.shape[1]
    length, columns = tok_here * count, width // count
    heads_here = columns // HDIM
    step_rows = min(BLOCK, BLOCK_AREA // length, length)
    rank_cols = 3 * ADAPTER_RANK
    group_cols = model_width // groups
    down_rows = group_cols // outer
    up_rows = ADAPTER_RANK // up_groups
    any_spec = pl.BlockSpec(memory_space=pl.ANY)
    vmem_spec = pl.BlockSpec(memory_space=pltpu.VMEM)
    smem_spec = pl.BlockSpec(memory_space=pltpu.SMEM)

    def bf16(*shape):
        return pltpu.VMEM(shape, jnp.bfloat16)

    def f32(*shape):
        return pltpu.VMEM(shape, jnp.float32)

    def sems(*shape):
        return [pltpu.SemaphoreType.DMA(shape)] * 2

    total_rows = 2 * dp_count * length
    keep_weights = 8 * length * length <= KEPT_BYTES
    scratch = [
        bf16(3, 3, length, columns),
        bf16(tok_here, model_width),
        bf16(groups, tok_here, group_cols),
        bf16(groups, tok_here, group_cols),
        bf16(group_cols, groups * tok_here),
        bf16(3, model_width, ADAPTER_RANK),
        bf16(3, ADAPTER_RANK, columns),
        bf16(outer, tok_here, rank_cols),
        bf16(outer, inner, tok_here, rank_cols),
        f32(3, 1, ADAPTER_RANK),
        f32(3, 1, ADAPTER_RANK),
        bf16(heads_here, length, HDIM),
        bf16(heads_here, length, HDIM),
        f32(length, HDIM),
        bf16(length, HDIM),
        bf16(length, HDIM),
        bf16(length, HDIM),
        bf16(HDIM, length),
        bf16(HDIM, length),
        bf16(length, HDIM),
        bf16(length, HDIM),
        f32(length, HDIM),
        f32(length, HDIM),
        bf16(length // step_rows, length, step_rows),
        bf16(length // step_rows, length, step_rows) if keep_weights else None,
        f32(length // step_rows, length, step_rows),
        f32(length, rank_cols) if heads_here > 1 else None,
        bf16(length, rank_cols),
        bf16(outer, inner, tok_here, rank_cols),
        bf16(outer, tok_here, rank_cols),
        bf16(outer, tok_here, rank_cols),
        bf16(length, columns),
        bf16(up_groups, 3, up_rows, columns),
        bf16(2, dp_count // inner, inner, 3, up_rows, columns),
        bf16(tok_here, rank_cols),
        bf16(groups, tok_here, rank_cols),
        bf16(outer, down_rows, rank_cols),
        bf16(outer, down_rows, rank_cols),
        *sems(2, heads_here, 3, outer, inner),
        *sems(heads_here, 3),
        *sems(2, outer),
        *sems(inner),
        *sems(heads_here),
        *sems(heads_here, outer, inner),
        *sems(groups),
        *sems(2, dp_count // inner, inner),
        *sems(3, outer, inner),
        *sems(3, outer),
        *sems(3, pairs),
        *sems(3, pairs, dp_count),
        *sems(3, outer),
        *sems(inner),
        pltpu.SemaphoreType.DMA((7,)),
    ]
    return pl.pallas_call(
        with_gaps(functools.partial(step_kernel, sizes, 1.0 / math.sqrt(total_rows)), scratch, 11),
        out_shape=(
            jax.ShapeDtypeStruct((tok_here, width), jnp.bfloat16),
            jax.ShapeDtypeStruct((3, down_rows, ADAPTER_RANK), jnp.float32),
            jax.ShapeDtypeStruct((3, up_rows, columns), jnp.float32),
        ),
        in_specs=[smem_spec] * 2 + [any_spec] * 6,
        out_specs=(any_spec, vmem_spec, vmem_spec),
        scratch_shapes=[item for item in scratch if item is not None],
        compiler_params=pltpu.CompilerParams(
            collective_id=0, has_side_effects=True, vmem_limit_bytes=VMEM_LIMIT
        ),
        name="step",
    )(guide, time_index, *fields, hidden, down, up)


def emit_kernel(*refs):
    count = (len(refs) - 2) // 3
    held = refs[2 * count : 3 * count]
    load_sem, store_sem = refs[3 * count :]
    loads = [
        pltpu.make_async_copy(refs[item], held[item], load_sem.at[item]) for item in range(count)
    ]
    stores = [
        pltpu.make_async_copy(held[item], refs[count + item], store_sem.at[item])
        for item in range(count)
    ]
    for load in loads:
        load.start()
    for load, store in zip(loads, stores):
        load.wait()
        store.start()
    for store in stores:
        store.wait()


def emit(arrays):
    any_specs = (pl.BlockSpec(memory_space=pl.ANY),) * len(arrays)
    return pl.pallas_call(
        emit_kernel,
        out_shape=tuple(jax.ShapeDtypeStruct(array.shape, array.dtype) for array in arrays),
        in_specs=any_specs,
        out_specs=any_specs,
        scratch_shapes=[pltpu.VMEM(array.shape, array.dtype) for array in arrays]
        + [pltpu.SemaphoreType.DMA((len(arrays),))] * 2,
        compiler_params=pltpu.CompilerParams(vmem_limit_bytes=VMEM_LIMIT),
        name="emit",
    )(*arrays)


def body(
    teacher_query,
    teacher_key,
    teacher_value,
    hidden,
    adapter_down_weight,
    adapter_up_weight,
    guidance_index,
    timestep_index,
):
    seq_count = lax.axis_size("seq")
    dp_count = lax.axis_size("dp")
    outputs = run_step(
        (seq_count, inner_size(seq_count, dp_count), dp_count),
        guidance_index[:, 0],
        timestep_index[:, 0],
        (teacher_query[0, :, 0], teacher_key[0, :, 0], teacher_value[0, :, 0]),
        hidden[0, 0],
        adapter_down_weight,
        adapter_up_weight,
    )
    student_tokens, grad_down, grad_up = emit(outputs)
    return (student_tokens[None, None], grad_down, grad_up)


def solution(mesh):
    placed = (
        P("cfg", None, "dp", "seq", None),
        P("cfg", None, "dp", "seq", None),
        P("cfg", None, "dp", "seq", None),
        P("cfg", "dp", "seq", None),
        P(),
        P(),
        P(None, "dp"),
        P(None, "dp"),
    )
    return jax.shard_map(
        body,
        mesh=mesh,
        in_specs=placed,
        out_specs=(
            P("cfg", "dp", "seq", None),
            P(None, ("cfg", "seq", "dp"), None),
            P(None, ("cfg", "dp"), "seq"),
        ),
        check_vma=False,
    )
```
